32 devices in a mesh: rep: 16 (over z, x, core), tp: 2 (over y).
Axes of the slice: x: 2, y: 2, z: 4, core: 2. Of those that a mesh axis runs over, the one named last changes fastest.
Arguments:
- tokens: bfloat16 [16, 256, 3072], P('rep', 'tp'), may hold values from -100 to 100
- norm_gain: float32 [16, 3072], P('rep'), may hold values from 0.5 to 1.5
- w_query: bfloat16 [16, 3072, 2048], P('rep', None, 'tp'), may hold values from -1 to 1
- key_weight: bfloat16 [16, 3072, 1024], P('rep', None, 'tp'), may hold values from -1 to 1
- value_weight: bfloat16 [16, 3072, 1024], P('rep', None, 'tp'), may hold values from -0.109375 to 0.109375
- attention_gradient: bfloat16 [16, 256, 2048], P('rep', None, 'tp'), may hold values from -6 to 6
- global_fragment: float32 [128, 3072], P('tp'), may hold values from -6 to 6
- momentum: float32 [128, 3072], P('tp'), may hold values from -3 to 3
- local_fragment: bfloat16 [16, 128, 3072], P('rep', 'tp'), may hold values from -6 to 6
Outputs:
- grad_query_w: bfloat16 [16, 3072, 2048], P('rep', None, 'tp')
- grad_key_w: bfloat16 [16, 3072, 1024], P('rep', None, 'tp')
- grad_value_w: bfloat16 [16, 3072, 1024], P('rep', None, 'tp')
- grad_gain: float32 [16, 3072], P('rep')
- grad_tokens: bfloat16 [16, 256, 3072], P('rep', 'tp')
- new_global: float32 [128, 3072], P('tp')
- new_momentum: float32 [128, 3072], P('tp')
The draws below stay inside these ranges and needn't reach their ends.
All inputs are finite; a program needn't handle non-finite values.
Results may differ from the reference program's by a relative error of at most 0.019.
The reference program's roundings to bfloat16 on the way count: a program that leaves them out, or rounds other values in their place, can miss the bound.
Values may be sent and summed in bfloat16 or wider, within the bound.
A program may use at most 128 MiB of HBM per device.

```python
import math
import jax
import jax.numpy as jnp
from jax import lax

MODEL_WIDTH = 3072
QUERY_HEADS = 16
KEY_VALUE_HEADS = 8
HEAD_SIZE = 128
SEQ = 256
FRAG = 128
N_REP = 16
N_TP = 2


def draw_tokens(key, part):
    col_scale = jnp.exp(jax.random.uniform(jax.random.fold_in(key, 12), (1, 1, MODEL_WIDTH), jnp.float32, math.log(0.5), math.log(2.0)))
    row_scale = jnp.exp(jax.random.uniform(jax.random.fold_in(key, 11), (N_REP, SEQ, 1), jnp.float32, 0.0, math.log(10.0)))
    jitter = jax.random.normal(jax.random.fold_in(key, 13), (N_REP, SEQ, MODEL_WIDTH), jnp.float32)
    result = jitter * col_scale * row_scale
    return jnp.clip(result, -100.0, 100.0).astype(jnp.bfloat16)


def draw_w_query(key, part):
    return (jax.random.normal(jax.random.fold_in(key, 21), (N_REP, MODEL_WIDTH, QUERY_HEADS * HEAD_SIZE), jnp.float32) * MODEL_WIDTH ** (-0.5)).astype(jnp.bfloat16)


def draw_key_weight(key, part):
    return (jax.random.normal(jax.random.fold_in(key, 31), (N_REP, MODEL_WIDTH, KEY_VALUE_HEADS * HEAD_SIZE), jnp.float32) * MODEL_WIDTH ** (-0.5)).astype(jnp.bfloat16)


def levels(own_key, shape, pieces, low, largest):
    level, own = 1.0, jax.random.fold_in(own_key, 6)
    for dim, parts in pieces:
        heights = jnp.exp(jax.random.uniform(jax.random.fold_in(own, dim), (parts,), jnp.float32, low / len(pieces), largest / len(pieces)))
        level = level * jnp.repeat(heights, shape[dim] // parts).reshape([-1 if axis == dim else 1 for axis in range(len(shape))])
    return level


def centred(own_key, shape, spread, reach, cuts=(), kind=jnp.bfloat16):
    array = jax.random.normal(own_key, shape, jnp.float32) * spread
    if len(cuts) > 0:
        array = levels(own_key, shape, cuts, -0.22, 0.18) * array
    return jnp.clip(array, min=-reach, max=reach).astype(kind)


def setup_inputs(seed: int = 0) -> dict:
    seeds = jax.random.split(jax.random.key(seed), 10)
    return {
        "tokens": draw_tokens(jax.random.fold_in(seeds[9], 71), 0),
        "norm_gain": jnp.clip(1.0 + 0.1 * jax.random.normal(seeds[1], (N_REP, MODEL_WIDTH), jnp.float32), 0.5, 1.5),
        "w_query": draw_w_query(jax.random.fold_in(seeds[9], 71), 0),
        "key_weight": draw_key_weight(jax.random.fold_in(seeds[9], 71), 0),
        "value_weight": centred(seeds[4], (N_REP, MODEL_WIDTH, KEY_VALUE_HEADS * HEAD_SIZE), MODEL_WIDTH ** -0.5, 0.109375, ((0, 16), (2, 2))),
        "attention_gradient": centred(seeds[5], (N_REP, SEQ, QUERY_HEADS * HEAD_SIZE), 1.0, 6.0, ((0, 16), (2, 2))),
        "global_fragment": centred(seeds[6], (FRAG, MODEL_WIDTH), 1.0, 6.0, ((0, 2),), jnp.float32),
        "momentum": centred(seeds[7], (FRAG, MODEL_WIDTH), 0.5, 3.0, ((0, 2),), jnp.float32),
        "local_fragment": centred(seeds[8], (N_REP, FRAG, MODEL_WIDTH), 1.0, 6.0, ((0, 16), (1, 2))),
    }


epsilon = 1e-05
rope_base = 500000.0
outer_rate = 0.7
outer_momentum = 0.9

def rope_tables(sequence_length, width):
    middle = width // 2
    frequency = rope_base ** (-2.0 * jnp.arange(middle, dtype=jnp.float32) / width)
    angles = jnp.arange(sequence_length, dtype=jnp.float32)[:, None] * frequency[None, :]
    angles = jnp.concatenate([angles, angles], axis=1)
    return (jnp.cos(angles)[:, None, :], jnp.sin(angles)[:, None, :])

def rotate(vectors, cosine_table, sine_table):
    middle = vectors.shape[-1] // 2
    turned = jnp.concatenate([-vectors[..., middle:], vectors[..., :middle]], axis=-1)
    return vectors * cosine_table + turned * sine_table

def reverse_rotation(gradient, cosine_table, sine_table):
    middle = gradient.shape[-1] // 2
    shifted = gradient * sine_table
    turned = jnp.concatenate([shifted[..., middle:], -shifted[..., :middle]], axis=-1)
    return gradient * cosine_table + turned

def attention_reverse(query_rows, rotated_keys, values_bfloat, grad_out, block_of_rows):
    sequence_length = query_rows.shape[0]
    score_scale = query_rows.shape[-1] ** (-0.5)
    keys_wide = rotated_keys.astype(jnp.float32)
    values_wide = values_bfloat.astype(jnp.float32)

    def one_block(running, block_index):
        acc_key, acc_value = running
        offset = block_index * block_of_rows
        query_block = lax.dynamic_slice_in_dim(query_rows, offset, block_of_rows, 0).astype(jnp.float32)
        grad_block = lax.dynamic_slice_in_dim(grad_out, offset, block_of_rows, 0).astype(jnp.float32)
        scores = jnp.einsum('qgrd,kgd->grqk', query_block, keys_wide) * score_scale
        row_pos = offset + jnp.arange(block_of_rows)
        col_pos = jnp.arange(sequence_length)
        allowed = col_pos[None, :] <= row_pos[:, None]
        scores = jnp.where(allowed, scores, -jnp.inf)
        highest = lax.optimization_barrier(jnp.max(scores, axis=-1, keepdims=True))
        powers = jnp.exp(scores - highest)
        probability = powers / lax.optimization_barrier(jnp.sum(powers, axis=-1, keepdims=True))
        prob_low = lax.optimization_barrier(probability.astype(jnp.bfloat16)).astype(jnp.float32)
        acc_value = acc_value + jnp.einsum('grqk,qgrd->kgd', prob_low, grad_block)
        grad_prob = jnp.einsum('qgrd,kgd->grqk', grad_block, values_wide)
        grad_score = probability * (grad_prob - lax.optimization_barrier(jnp.sum(grad_prob * probability, axis=-1, keepdims=True))) * score_scale
        score_low = lax.optimization_barrier(grad_score.astype(jnp.bfloat16)).astype(jnp.float32)
        grad_query = jnp.einsum('grqk,kgd->qgrd', score_low, keys_wide)
        acc_key = acc_key + jnp.einsum('grqk,qgrd->kgd', score_low, query_block)
        return ((acc_key, acc_value), grad_query)
    initial = jnp.zeros(rotated_keys.shape, jnp.float32)
    (acc_key, acc_value), grad_blocks = lax.scan(one_block, (initial, initial), jnp.arange(sequence_length // block_of_rows))
    grad_query = grad_blocks.reshape(query_rows.shape)
    return (grad_query, acc_key, acc_value)

def replica_grads(items):
    tokens, norm_gains, w_query, key_weight, value_weight, attention_gradient = items
    sequence_length = tokens.shape[0]
    widened_rows = tokens.astype(jnp.float32)
    inverse_norm = lax.rsqrt(lax.optimization_barrier(jnp.mean(widened_rows * widened_rows, axis=-1, keepdims=True)) + epsilon)
    normalized_input = widened_rows * inverse_norm
    normalized = (normalized_input * norm_gains[None, :]).astype(jnp.bfloat16)
    cosine_table, sine_table = rope_tables(sequence_length, HEAD_SIZE)
    query_rows = jnp.dot(normalized, w_query, preferred_element_type=jnp.float32).reshape(sequence_length, QUERY_HEADS, HEAD_SIZE)
    query_rows = rotate(query_rows, cosine_table, sine_table).astype(jnp.bfloat16)
    rotated_keys = jnp.dot(normalized, key_weight, preferred_element_type=jnp.float32).reshape(sequence_length, KEY_VALUE_HEADS, HEAD_SIZE)
    rotated_keys = rotate(rotated_keys, cosine_table, sine_table).astype(jnp.bfloat16)
    values_bfloat = jnp.dot(normalized, value_weight, preferred_element_type=jnp.float32).astype(jnp.bfloat16).reshape(sequence_length, KEY_VALUE_HEADS, HEAD_SIZE)
    replica_group = QUERY_HEADS // KEY_VALUE_HEADS
    block_of_rows = min(512, sequence_length)
    query_input_gradient, key_input_gradient, value_input_gradient = attention_reverse(query_rows.reshape(sequence_length, KEY_VALUE_HEADS, replica_group, HEAD_SIZE), rotated_keys, values_bfloat, attention_gradient.reshape(sequence_length, KEY_VALUE_HEADS, replica_group, HEAD_SIZE), block_of_rows)
    dquery = reverse_rotation(query_input_gradient.reshape(sequence_length, QUERY_HEADS, HEAD_SIZE), cosine_table, sine_table).astype(jnp.bfloat16).reshape(sequence_length, QUERY_HEADS * HEAD_SIZE)
    key_gradient = reverse_rotation(key_input_gradient, cosine_table, sine_table).astype(jnp.bfloat16).reshape(sequence_length, KEY_VALUE_HEADS * HEAD_SIZE)
    value_gradient = value_input_gradient.astype(jnp.bfloat16).reshape(sequence_length, KEY_VALUE_HEADS * HEAD_SIZE)
    contract = (((0,), (0,)), ((), ()))
    grad_wq = lax.dot_general(normalized, dquery, contract, preferred_element_type=jnp.float32).astype(jnp.bfloat16)
    grad_wk = lax.dot_general(normalized, key_gradient, contract, preferred_element_type=jnp.float32).astype(jnp.bfloat16)
    grad_wv = lax.dot_general(normalized, value_gradient, contract, preferred_element_type=jnp.float32).astype(jnp.bfloat16)
    query_cols = QUERY_HEADS * HEAD_SIZE // N_TP
    key_value_columns = KEY_VALUE_HEADS * HEAD_SIZE // N_TP
    back = (((1,), (1,)), ((), ()))
    summed_rows = jnp.zeros((sequence_length, MODEL_WIDTH), jnp.float32)
    for shard_index in range(N_TP):
        qa, qb_end = (shard_index * query_cols, (shard_index + 1) * query_cols)
        ka, kb_end = (shard_index * key_value_columns, (shard_index + 1) * key_value_columns)
        partial_value = lax.dot_general(dquery[:, qa:qb_end], w_query[:, qa:qb_end], back, preferred_element_type=jnp.float32)
        partial_value = partial_value + lax.dot_general(key_gradient[:, ka:kb_end], key_weight[:, ka:kb_end], back, preferred_element_type=jnp.float32)
        partial_value = partial_value + lax.dot_general(value_gradient[:, ka:kb_end], value_weight[:, ka:kb_end], back, preferred_element_type=jnp.float32)
        summed_rows = summed_rows + lax.optimization_barrier(partial_value.astype(jnp.bfloat16)).astype(jnp.float32)
    gains_gradient = lax.optimization_barrier(jnp.sum(summed_rows * normalized_input, axis=0))
    scaled_rows = summed_rows * norm_gains[None, :]
    gradient_rows = inverse_norm * (scaled_rows - normalized_input * lax.optimization_barrier(jnp.mean(scaled_rows * normalized_input, axis=-1, keepdims=True)))
    return (grad_wq, grad_wk, grad_wv, gains_gradient, gradient_rows.astype(jnp.bfloat16))

def reference(tokens, norm_gain, w_query, key_weight, value_weight, attention_gradient, global_fragment, momentum, local_fragment):
    grad_wq, grad_wk, grad_wv, gains_gradient, gradient_rows = lax.map(replica_grads, (tokens, norm_gain, w_query, key_weight, value_weight, attention_gradient))
    delta = global_fragment[None, :, :] - local_fragment.astype(jnp.float32)
    mean_delta = lax.optimization_barrier(jnp.sum(delta, axis=0)) / N_REP
    new_momentum = outer_momentum * momentum + mean_delta
    new_global = global_fragment - outer_rate * (mean_delta + outer_momentum * new_momentum)
    return (grad_wq, grad_wk, grad_wv, gains_gradient, gradient_rows, new_global, new_momentum)
```

```python
import functools

import jax
import jax.numpy as jnp
import numpy as np
from jax import lax
from jax.experimental import pallas as pl
from jax.experimental.pallas import tpu as pltpu
from jax.sharding import PartitionSpec as P

MESH = pl.DeviceIdType.MESH

HEAD_SIZE = 128


epsilon = 1e-05
rope_base = 500000.0
outer_rate = 0.7
outer_momentum = 0.9
LOG2_E = 1.4426950408889634


def rope_tables(sequence_length, width):
    middle = width // 2
    frequency = rope_base ** (-2.0 * jnp.arange(middle, dtype=jnp.float32) / width)
    angles = jnp.arange(sequence_length, dtype=jnp.float32)[:, None] * frequency[None, :]
    angles = jnp.concatenate([angles, angles], axis=1)
    return (jnp.cos(angles)[:, None, :], jnp.sin(angles)[:, None, :])


def rotate(vectors, cosine_table, sine_table):
    middle = vectors.shape[-1] // 2
    turned = jnp.concatenate([-vectors[..., middle:], vectors[..., :middle]], axis=-1)
    return vectors * cosine_table + turned * sine_table


def reverse_rotation(gradient, cosine_table, sine_table):
    middle = gradient.shape[-1] // 2
    shifted = gradient * sine_table
    turned = jnp.concatenate([shifted[..., middle:], -shifted[..., :middle]], axis=-1)
    return gradient * cosine_table + turned


def attention_reverse(query_rows, rotated_keys, values_bfloat, grad_out, block_of_rows):
    sequence_length = query_rows.shape[0]
    score_scale = query_rows.shape[-1] ** (-0.5)

    def one_block(running, block_index):
        acc_key, acc_value = running
        offset = block_index * block_of_rows
        query_block = lax.dynamic_slice_in_dim(query_rows, offset, block_of_rows, 0)
        grad_block = lax.dynamic_slice_in_dim(grad_out, offset, block_of_rows, 0)
        scores = (
            jnp.einsum(
                "qgrd,kgd->grqk", query_block, rotated_keys, preferred_element_type=jnp.float32
            )
            * score_scale
        )
        row_pos = offset + jnp.arange(block_of_rows)
        col_pos = jnp.arange(sequence_length)
        allowed = col_pos[None, :] <= row_pos[:, None]
        scores = jnp.where(allowed, scores, -jnp.inf)
        highest = jnp.max(scores, axis=-1, keepdims=True)
        powers = jnp.exp(scores - highest)
        probability = powers / jnp.sum(powers, axis=-1, keepdims=True)
        prob_low = probability.astype(jnp.bfloat16)
        acc_value = acc_value + jnp.einsum(
            "grqk,qgrd->kgd", prob_low, grad_block, preferred_element_type=jnp.float32
        )
        grad_prob = jnp.einsum(
            "qgrd,kgd->grqk", grad_block, values_bfloat, preferred_element_type=jnp.float32
        )
        grad_score = (
            probability
            * (grad_prob - jnp.sum(grad_prob * probability, axis=-1, keepdims=True))
            * score_scale
        )
        score_low = grad_score.astype(jnp.bfloat16)
        grad_query = jnp.einsum(
            "grqk,kgd->qgrd", score_low, rotated_keys, preferred_element_type=jnp.float32
        )
        acc_key = acc_key + jnp.einsum(
            "grqk,qgrd->kgd", score_low, query_block, preferred_element_type=jnp.float32
        )
        return ((acc_key, acc_value), grad_query)

    initial = jnp.zeros(rotated_keys.shape, jnp.float32)
    (acc_key, acc_value), grad_blocks = lax.scan(
        one_block, (initial, initial), jnp.arange(sequence_length // block_of_rows)
    )
    return (grad_blocks.reshape(query_rows.shape), acc_key, acc_value)


def body(
    tokens,
    norm_gain,
    w_query,
    key_weight,
    value_weight,
    attention_gradient,
    global_fragment,
    momentum,
    local_fragment,
):
    local_rows = tokens[0]
    norm_gains = norm_gain[0]
    weight_q = w_query[0]
    weight_k = key_weight[0]
    weight_v = value_weight[0]
    widened_rows = local_rows.astype(jnp.float32)
    inverse_norm = lax.rsqrt(
        jnp.mean(widened_rows * widened_rows, axis=-1, keepdims=True) + epsilon
    )
    normalized_input = widened_rows * inverse_norm
    normalized_local = (normalized_input * norm_gains[None, :]).astype(jnp.bfloat16)
    normalized = lax.all_gather(normalized_local, "tp", axis=0, tiled=True)
    sequence_length = normalized.shape[0]
    heads_q = weight_q.shape[1] // HEAD_SIZE
    heads_kv = weight_k.shape[1] // HEAD_SIZE
    cosine_table, sine_table = rope_tables(sequence_length, HEAD_SIZE)
    query_rows = jnp.dot(normalized, weight_q, preferred_element_type=jnp.float32).reshape(
        sequence_length, heads_q, HEAD_SIZE
    )
    query_rows = rotate(query_rows, cosine_table, sine_table).astype(jnp.bfloat16)
    rotated_keys = jnp.dot(normalized, weight_k, preferred_element_type=jnp.float32).reshape(
        sequence_length, heads_kv, HEAD_SIZE
    )
    rotated_keys = rotate(rotated_keys, cosine_table, sine_table).astype(jnp.bfloat16)
    values_bfloat = (
        jnp.dot(normalized, weight_v, preferred_element_type=jnp.float32)
        .astype(jnp.bfloat16)
        .reshape(sequence_length, heads_kv, HEAD_SIZE)
    )
    replica_group = heads_q // heads_kv
    block_of_rows = min(512, sequence_length)
    query_input_gradient, key_input_gradient, value_input_gradient = attention_reverse(
        query_rows.reshape(sequence_length, heads_kv, replica_group, HEAD_SIZE),
        rotated_keys,
        values_bfloat,
        attention_gradient[0].reshape(sequence_length, heads_kv, replica_group, HEAD_SIZE),
        block_of_rows,
    )
    dquery = (
        reverse_rotation(
            query_input_gradient.reshape(sequence_length, heads_q, HEAD_SIZE),
            cosine_table,
            sine_table,
        )
        .astype(jnp.bfloat16)
        .reshape(sequence_length, heads_q * HEAD_SIZE)
    )
    key_gradient = (
        reverse_rotation(key_input_gradient, cosine_table, sine_table)
        .astype(jnp.bfloat16)
        .reshape(sequence_length, heads_kv * HEAD_SIZE)
    )
    value_gradient = value_input_gradient.astype(jnp.bfloat16).reshape(
        sequence_length, heads_kv * HEAD_SIZE
    )
    contract = (((0,), (0,)), ((), ()))
    grad_wq = lax.dot_general(
        normalized, dquery, contract, preferred_element_type=jnp.float32
    ).astype(jnp.bfloat16)
    grad_wk = lax.dot_general(
        normalized, key_gradient, contract, preferred_element_type=jnp.float32
    ).astype(jnp.bfloat16)
    grad_wv = lax.dot_general(
        normalized, value_gradient, contract, preferred_element_type=jnp.float32
    ).astype(jnp.bfloat16)
    back = (((1,), (1,)), ((), ()))
    partial_value = lax.dot_general(dquery, weight_q, back, preferred_element_type=jnp.float32)
    partial_value = partial_value + lax.dot_general(
        key_gradient, weight_k, back, preferred_element_type=jnp.float32
    )
    summed_rows = lax.psum_scatter(
        (
            partial_value
            + lax.dot_general(value_gradient, weight_v, back, preferred_element_type=jnp.float32)
        ).astype(jnp.bfloat16),
        "tp",
        scatter_dimension=0,
        tiled=True,
    ).astype(jnp.float32)
    gains_gradient = lax.psum(jnp.sum(summed_rows * normalized_input, axis=0), "tp")
    scaled_rows = summed_rows * norm_gains[None, :]
    gradient_rows = (
        inverse_norm
        * (
            scaled_rows
            - normalized_input * jnp.mean(scaled_rows * normalized_input, axis=-1, keepdims=True)
        )
    ).astype(jnp.bfloat16)
    delta = global_fragment - local_fragment[0].astype(jnp.float32)
    replicas = lax.axis_size("rep")
    mean_delta = lax.psum(delta, "rep") / replicas
    new_momentum = outer_momentum * momentum + mean_delta
    new_global = global_fragment - outer_rate * (mean_delta + outer_momentum * new_momentum)
    return (
        grad_wq[None],
        grad_wk[None],
        grad_wv[None],
        gains_gradient[None],
        gradient_rows[None],
        new_global,
        new_momentum,
    )

NT = (((1,), (1,)), ((), ()))
TN = (((0,), (0,)), ((), ()))


def dot(a, b, dims=(((1,), (0,)), ((), ()))):
    return lax.dot_general(a, b, dims, preferred_element_type=jnp.float32)


def ds(index, size):
    return pl.ds(pl.multiple_of(index * size, size), size)


def host_tables(sequence_length, width):
    middle = width // 2
    frequency = rope_base ** (-2.0 * np.arange(middle) / width)
    angles = np.arange(sequence_length)[:, None] * frequency[None, :]
    cosine, sine = np.cos(angles), np.sin(angles)
    return (
        jnp.asarray(np.concatenate([cosine, cosine], axis=1), jnp.float32),
        jnp.asarray(np.concatenate([-sine, sine], axis=1), jnp.float32),
    )


def front_kernel(
    n_rep,
    chunks,
    tile,
    tokens_hbm,
    gain_hbm,
    wq_hbm,
    wk_hbm,
    wv_hbm,
    go_hbm,
    cos_hbm,
    sin_hbm,
    local_hbm,
    x_ref,
    nm_ref,
    d_ref,
    here_ref,
    far_hbm,
    gain_part_ref,
    mean_ref,
    gain_ref,
    go_ref,
    cos_ref,
    sin_ref,
    w_ref,
    acc_ref,
    q_ref,
    k_ref,
    v_ref,
    far_ref,
    pieces_ref,
    own_mean_ref,
    in_sems,
    w_sems,
    far_sems,
    ag_send,
    ag_recv,
    fr_send,
    fr_recv,
    fg_send,
    fg_recv,
    own_sem,
    go_sem,
):
    me = lax.axis_index("tp")
    peer = 1 - me
    rep = lax.axis_index("rep")
    side = lax.rem(rep, 2)
    rows, width = x_ref.shape
    qw, kw = wq_hbm.shape[1], wk_hbm.shape[1]
    total = qw + 2 * kw
    cw = width // chunks
    piece_rows, piece_cols = own_mean_ref.shape
    col_blocks = width // piece_cols
    barrier = pltpu.get_barrier_semaphore()
    pl.semaphore_signal(barrier, inc=1, device_id={"tp": peer}, device_id_type=MESH)

    def greet(j, _):
        pl.semaphore_signal(
            barrier, inc=1, device_id={"rep": lax.rem(rep + j, n_rep)}, device_id_type=MESH
        )
        return 0

    lax.fori_loop(1, n_rep, greet, 0)
    first_copies = [
        pltpu.make_async_copy(tokens_hbm, x_ref, in_sems.at[0]),
        pltpu.make_async_copy(gain_hbm, gain_ref, in_sems.at[1]),
    ]
    late_copies = [
        pltpu.make_async_copy(cos_hbm, cos_ref, in_sems.at[2]),
        pltpu.make_async_copy(sin_hbm, sin_ref, in_sems.at[3]),
        pltpu.make_async_copy(go_hbm, go_ref, in_sems.at[4]),
    ]
    weight_copies = []
    for source, offset in ((wq_hbm, 0), (wk_hbm, qw), (wv_hbm, qw + kw)):
        for t in range(source.shape[1] // tile):
            weight_copies.append(
                pltpu.make_async_copy(
                    source.at[:, pl.ds(t * tile, tile)],
                    w_ref.at[:, pl.ds(offset + t * tile, tile)],
                    w_sems.at[len(weight_copies)],
                )
            )

    def piece(owner):
        return (
            ds(owner // col_blocks, piece_rows),
            ds(lax.rem(owner, col_blocks), piece_cols),
        )

    own_piece = pltpu.make_async_copy(local_hbm.at[piece(rep)], pieces_ref.at[0], own_sem)
    for copy in first_copies + weight_copies[:1] + late_copies[:2] + weight_copies[1:]:
        copy.start()
    own_piece.start()
    late_copies[2].start()
    for copy in first_copies:
        copy.wait()

    step = 16

    def norm_rows(i, _):
        x = x_ref[ds(i, step), :].astype(jnp.float32)
        inverse = lax.rsqrt(jnp.mean(x * x, axis=-1, keepdims=True) + epsilon)
        nm_ref[pl.ds(pl.multiple_of(me * rows + i * step, step), step), :] = (
            x * inverse * gain_ref[...]
        ).astype(jnp.bfloat16)
        return 0

    lax.fori_loop(0, rows // step, norm_rows, 0)
    pl.semaphore_wait(barrier, n_rep)

    def gather_copy(c):
        part = nm_ref.at[ds(me, rows), ds(c, cw)]
        return pltpu.make_async_remote_copy(
            src_ref=part,
            dst_ref=part,
            send_sem=ag_send.at[c],
            recv_sem=ag_recv.at[c],
            device_id={"tp": peer},
            device_id_type=MESH,
        )

    def scatter_copy(j):
        target = lax.rem(rep + j, n_rep)
        return pltpu.make_async_remote_copy(
            src_ref=local_hbm.at[piece(target)],
            dst_ref=pieces_ref.at[j],
            send_sem=fr_send.at[j],
            recv_sem=fr_recv.at[j],
            device_id={"rep": target},
            device_id_type=MESH,
        )

    def spread_copy(j, owner):
        return pltpu.make_async_remote_copy(
            src_ref=own_mean_ref,
            dst_ref=mean_ref.at[piece(owner)],
            send_sem=fg_send.at[j],
            recv_sem=fg_recv.at[j],
            device_id={"rep": lax.rem(rep + j, n_rep)},
            device_id_type=MESH,
        )

    def start_all(make, low, high):
        def one(j, _):
            make(j).start()
            return 0

        lax.fori_loop(low, high, one, 0)

    def wait_recv_all(make, low, high):
        def one(j, _):
            make(j).wait_recv()
            return 0

        lax.fori_loop(low, high, one, 0)

    def wait_send_all(make, low, high):
        def one(j, _):
            make(j).wait_send()
            return 0

        lax.fori_loop(low, high, one, 0)

    @pl.when(side == 0)
    def _():
        start_all(gather_copy, 0, chunks)

    start_all(scatter_copy, 1, n_rep)

    for t, copy in enumerate(weight_copies):
        copy.wait()
        acc_ref[ds(me, rows), pl.ds(t * tile, tile)] = dot(
            nm_ref[ds(me, rows), :], w_ref[:, pl.ds(t * tile, tile)]
        )
    acc_ref[ds(peer, rows), :] = jnp.zeros((rows, total), jnp.float32)
    for copy in late_copies:
        copy.wait()

    heads_q, heads_kv = qw // HEAD_SIZE, kw // HEAD_SIZE

    def rope_rows(which):
        block = ds(which, rows)
        cosine, sine = cos_ref[block, :], sin_ref[block, :]

        def rope_head(source, target, index):
            vector = acc_ref[block, pl.ds(source * HEAD_SIZE, HEAD_SIZE)]
            target[block, pl.ds(index * HEAD_SIZE, HEAD_SIZE)] = (
                vector * cosine + pltpu.roll(vector, HEAD_SIZE // 2, 1) * sine
            ).astype(jnp.bfloat16)

        for h in range(heads_q):
            rope_head(h, q_ref, h)
        for h in range(heads_kv):
            rope_head(heads_q + h, k_ref, h)
        v_ref[block, :] = acc_ref[block, pl.ds(qw + kw, kw)].astype(jnp.bfloat16)

    rope_rows(me)

    def average_pieces():
        own_piece.wait()
        wait_recv_all(scatter_copy, 1, n_rep)
        summed = pieces_ref[0].astype(jnp.float32)
        for j in range(1, n_rep):
            summed = summed + pieces_ref[j].astype(jnp.float32)
        summed = (summed * (1.0 / n_rep)).astype(jnp.bfloat16)
        own_mean_ref[...] = summed
        mean_ref[piece(rep)] = summed
        start_all(lambda j: spread_copy(j, rep), 1, n_rep)

    @pl.when(side == 1)
    def _():
        pl.semaphore_wait(go_sem, 1)
        start_all(gather_copy, 0, chunks)
        average_pieces()

    def arrived(c, _):
        pltpu.make_async_remote_copy(
            src_ref=nm_ref.at[ds(peer, rows), ds(c, cw)],
            dst_ref=nm_ref.at[ds(peer, rows), ds(c, cw)],
            send_sem=ag_send.at[c],
            recv_sem=ag_recv.at[c],
            device_id={"tp": peer},
            device_id_type=MESH,
        ).wait_recv()

        @pl.when((side == 0) & (c == chunks - 2))
        def _():
            pl.semaphore_signal(
                go_sem, inc=1, device_id={"rep": lax.rem(rep + 1, n_rep)}, device_id_type=MESH
            )

        part = nm_ref[ds(peer, rows), ds(c, cw)]

        def one(t, _):
            acc_ref[ds(peer, rows), ds(t, tile)] += dot(part, w_ref[ds(c, cw), ds(t, tile)])
            return 0

        lax.fori_loop(0, total // tile, one, 0)
        return 0

    lax.fori_loop(0, chunks, arrived, 0)
    rope_rows(peer)

    group = heads_q // heads_kv
    scale = HEAD_SIZE ** (-0.5)
    key_pos = lax.broadcasted_iota(jnp.int32, (rows, rows), 0)
    query_pos = lax.broadcasted_iota(jnp.int32, (rows, rows), 1)
    bias = jnp.where(key_pos <= query_pos, 0.0, -jnp.inf).astype(jnp.float32)
    bias = jnp.concatenate([bias] * group, axis=1)

    def reverse(gradient, block):
        c = cos_ref[block * rows : (block + 1) * rows]
        s = sin_ref[block * rows : (block + 1) * rows]
        return (gradient * c - pltpu.roll(gradient, HEAD_SIZE // 2, 1) * s).astype(jnp.bfloat16)

    def kv_head(g, _):
        @pl.when((side == 0) & (g == 1))
        def _():
            average_pieces()

        grad_k = [None, None]
        grad_v = [None, None]
        kv = ds(g, HEAD_SIZE)
        for b in range(2):
            keys = (b + 1) * rows
            block = pl.ds(b * rows, rows)
            heads = [ds(g * group + r, HEAD_SIZE) for r in range(group)]
            query = jnp.concatenate([q_ref[block, head] for head in heads], axis=0)
            out_grad = jnp.concatenate([go_ref[block, head] for head in heads], axis=0)
            key = k_ref[pl.ds(0, keys), kv]
            value = v_ref[pl.ds(0, keys), kv]
            scores = dot(key, query, NT)
            grad_prob = dot(value, out_grad, NT)
            if b == 0:
                scores = scores + bias
            else:
                scores = jnp.concatenate([scores[:rows], scores[rows:] + bias], axis=0)
            highest = jnp.max(scores, axis=0, keepdims=True)
            powers = jnp.exp2((scores - highest) * (scale * LOG2_E))
            prob = powers * (1.0 / jnp.sum(powers, axis=0, keepdims=True))
            inner = jnp.sum(grad_prob * prob, axis=0, keepdims=True)
            score_low = (prob * (grad_prob - inner) * scale).astype(jnp.bfloat16)
            grad_q = dot(score_low, key, TN)
            for r, head in enumerate(heads):
                d_ref[block, head] = reverse(grad_q[r * rows : (r + 1) * rows], b)
            part_v = dot(prob.astype(jnp.bfloat16), out_grad)
            part_k = dot(score_low, query)
            for j in range(b + 1):
                pv = part_v[j * rows : (j + 1) * rows]
                pk = part_k[j * rows : (j + 1) * rows]
                grad_v[j] = pv if grad_v[j] is None else grad_v[j] + pv
                grad_k[j] = pk if grad_k[j] is None else grad_k[j] + pk
        for j in range(2):
            block = pl.ds(j * rows, rows)
            d_ref[block, ds(heads_q + g, HEAD_SIZE)] = reverse(grad_k[j], j)
            d_ref[block, ds(heads_q + heads_kv + g, HEAD_SIZE)] = grad_v[j].astype(jnp.bfloat16)
        return 0

    lax.fori_loop(0, heads_kv, kv_head, 0)

    def far_copy(t):
        return pltpu.make_async_copy(
            far_ref.at[:, ds(t, tile)], far_hbm.at[:, ds(t, tile)], far_sems.at[t]
        )

    def back(t, _):
        both = jnp.concatenate([d_ref[ds(peer, rows), :], d_ref[ds(me, rows), :]], axis=0)
        part = dot(both, w_ref[ds(t, tile), :], NT).astype(jnp.bfloat16)
        cols = ds(t, tile)
        far_ref[:, cols] = part[:rows]
        here_ref[:, cols] = part[rows:]
        wide = part.astype(jnp.float32)
        products = wide[:rows] * nm_ref[ds(peer, rows), cols].astype(jnp.float32)
        products += wide[rows:] * nm_ref[ds(me, rows), cols].astype(jnp.float32)
        gain_part_ref[:, cols] = jnp.sum(products, axis=0, keepdims=True) / gain_ref[:, cols]
        far_copy(t).start()
        return 0

    tiles = width // tile
    lax.fori_loop(0, tiles, back, 0)

    wait_recv_all(lambda j: spread_copy(j, lax.rem(rep + n_rep - j, n_rep)), 1, n_rep)
    wait_send_all(gather_copy, 0, chunks)
    wait_send_all(scatter_copy, 1, n_rep)
    wait_send_all(lambda j: spread_copy(j, rep), 1, n_rep)
    for t in range(tiles):
        far_copy(t).wait()


def weights_kernel(nm_ref, d_ref, mean_ref, global_ref, momentum_ref, gq_ref, gk_ref, gv_ref, ng_ref, nmom_ref):
    i = pl.program_id(0)
    wide = gq_ref.shape[0]
    qw, kw = gq_ref.shape[1], gk_ref.shape[1]
    grad = dot(nm_ref[:, ds(i, wide)], d_ref[...], TN).astype(jnp.bfloat16)
    gq_ref[...] = grad[:, :qw]
    gk_ref[...] = grad[:, qw : qw + kw]
    gv_ref[...] = grad[:, qw + kw :]
    held = global_ref[...]
    mean_delta = held - mean_ref[:, ds(i, wide)].astype(jnp.float32)
    new_momentum = outer_momentum * momentum_ref[...] + mean_delta
    nmom_ref[...] = new_momentum
    ng_ref[...] = held - outer_rate * (mean_delta + outer_momentum * new_momentum)


def rows_kernel(x_ref, here_ref, gain_ref, landed_ref, gain_a_ref, gain_b_ref, out_ref, gain_out_ref):
    i = pl.program_id(0)
    count = landed_ref.shape[0]

    @pl.when(i == 0)
    def _():
        gain_out_ref[...] = gain_a_ref[...] + gain_b_ref[...]

    step = 16

    def some(j, _):
        block = pl.ds(pl.multiple_of(i * count + j * step, step), step)
        part = ds(j, step)
        x = x_ref[block, :].astype(jnp.float32)
        inverse = lax.rsqrt(jnp.mean(x * x, axis=-1, keepdims=True) + epsilon)
        xhat = x * inverse
        scaled = (
            here_ref[block, :].astype(jnp.float32) + landed_ref[part, :].astype(jnp.float32)
        ) * gain_ref[...]
        out_ref[part, :] = (
            inverse * (scaled - xhat * jnp.mean(scaled * xhat, axis=-1, keepdims=True))
        ).astype(jnp.bfloat16)
        return 0

    lax.fori_loop(0, count // step, some, 0)


def pair_body(
    n_rep,
    tokens,
    norm_gain,
    w_query,
    key_weight,
    value_weight,
    attention_gradient,
    global_fragment,
    momentum,
    local_fragment,
):
    rows, width = tokens.shape[1:]
    sequence = 2 * rows
    weight_q, weight_k, weight_v = w_query[0], key_weight[0], value_weight[0]
    qw, kw = weight_q.shape[1], weight_k.shape[1]
    total = qw + 2 * kw
    frag_rows = local_fragment.shape[1]
    piece_rows = 16
    piece_cols = width * frag_rows // piece_rows // n_rep
    chunks = 6
    tile = 512
    bf16, f32 = jnp.bfloat16, jnp.float32
    cosine, sine = host_tables(sequence, HEAD_SIZE)
    vmem = pl.BlockSpec(memory_space=pltpu.VMEM)
    hbm = pl.BlockSpec(memory_space=pltpu.HBM)
    x, normed, d, here, far, gain_partial, mean_local = pl.pallas_call(
        functools.partial(front_kernel, n_rep, chunks, tile),
        out_shape=(
            jax.ShapeDtypeStruct((rows, width), bf16),
            jax.ShapeDtypeStruct((sequence, width), bf16),
            jax.ShapeDtypeStruct((sequence, total), bf16),
            jax.ShapeDtypeStruct((rows, width), bf16),
            jax.ShapeDtypeStruct((rows, width), bf16),
            jax.ShapeDtypeStruct((1, width), f32),
            jax.ShapeDtypeStruct((frag_rows, width), bf16),
        ),
        in_specs=[hbm] * 9,
        out_specs=(vmem, vmem, vmem, vmem, hbm, vmem, vmem),
        scratch_shapes=[
            pltpu.VMEM((1, width), f32),
            pltpu.VMEM((sequence, qw), bf16),
            pltpu.VMEM((sequence, HEAD_SIZE), f32),
            pltpu.VMEM((sequence, HEAD_SIZE), f32),
            pltpu.VMEM((width, total), bf16),
            pltpu.VMEM((sequence, total), f32),
            pltpu.VMEM((sequence, qw), bf16),
            pltpu.VMEM((sequence, kw), bf16),
            pltpu.VMEM((sequence, kw), bf16),
            pltpu.VMEM((rows, width), bf16),
            pltpu.VMEM((n_rep, piece_rows, piece_cols), bf16),
            pltpu.VMEM((piece_rows, piece_cols), bf16),
            pltpu.SemaphoreType.DMA((5,)),
            pltpu.SemaphoreType.DMA((total // tile,)),
            pltpu.SemaphoreType.DMA((width // tile,)),
            pltpu.SemaphoreType.DMA((chunks,)),
            pltpu.SemaphoreType.DMA((chunks,)),
            pltpu.SemaphoreType.DMA((n_rep,)),
            pltpu.SemaphoreType.DMA((n_rep,)),
            pltpu.SemaphoreType.DMA((n_rep,)),
            pltpu.SemaphoreType.DMA((n_rep,)),
            pltpu.SemaphoreType.DMA,
            pltpu.SemaphoreType.REGULAR,
        ],
        compiler_params=pltpu.CompilerParams(
            collective_id=0, has_side_effects=True, vmem_limit_bytes=48 * 1024 * 1024
        ),
    )(
        tokens[0],
        norm_gain,
        weight_q,
        weight_k,
        weight_v,
        attention_gradient[0],
        cosine,
        sine,
        local_fragment[0],
    )
    swap = [(0, 1), (1, 0)]
    landed = lax.ppermute(far, "tp", swap)
    gain_landed = lax.ppermute(gain_partial, "tp", swap)
    wide = 256
    columns = lambda size: pl.BlockSpec((size, wide), lambda i: (0, i))
    grad_wq, grad_wk, grad_wv, new_global, new_momentum = pl.pallas_call(
        weights_kernel,
        grid=(width // wide,),
        out_shape=(
            jax.ShapeDtypeStruct((width, qw), bf16),
            jax.ShapeDtypeStruct((width, kw), bf16),
            jax.ShapeDtypeStruct((width, kw), bf16),
            jax.ShapeDtypeStruct((frag_rows, width), f32),
            jax.ShapeDtypeStruct((frag_rows, width), f32),
        ),
        in_specs=[vmem, vmem, vmem, columns(frag_rows), columns(frag_rows)],
        out_specs=(
            pl.BlockSpec((wide, qw), lambda i: (i, 0)),
            pl.BlockSpec((wide, kw), lambda i: (i, 0)),
            pl.BlockSpec((wide, kw), lambda i: (i, 0)),
            columns(frag_rows),
            columns(frag_rows),
        ),
        compiler_params=pltpu.CompilerParams(vmem_limit_bytes=16 * 1024 * 1024),
        cost_estimate=pl.CostEstimate(
            flops=2 * sequence * width * total, bytes_accessed=3 * width * total, transcendentals=0
        ),
    )(normed, d, mean_local, global_fragment, momentum)
    count = 32
    block = pl.BlockSpec((count, width), lambda i: (i, 0))
    gradient_rows, gains_gradient = pl.pallas_call(
        rows_kernel,
        grid=(rows // count,),
        out_shape=(
            jax.ShapeDtypeStruct((rows, width), bf16),
            jax.ShapeDtypeStruct((1, width), f32),
        ),
        in_specs=[vmem, vmem, vmem, block, vmem, vmem],
        out_specs=(block, pl.BlockSpec((1, width), lambda i: (0, 0))),
        compiler_params=pltpu.CompilerParams(vmem_limit_bytes=8 * 1024 * 1024),
        cost_estimate=pl.CostEstimate(
            flops=12 * rows * width, bytes_accessed=4 * rows * width, transcendentals=0
        ),
    )(x, here, norm_gain, landed, gain_partial, gain_landed)
    return (
        grad_wq[None],
        grad_wk[None],
        grad_wv[None],
        gains_gradient,
        gradient_rows[None],
        new_global,
        new_momentum,
    )


def solution(mesh):
    placed = (
        P("rep", "tp", None),
        P("rep", None),
        P("rep", None, "tp"),
        P("rep", None, "tp"),
        P("rep", None, "tp"),
        P("rep", None, "tp"),
        P("tp", None),
        P("tp", None),
        P("rep", "tp", None),
    )
    paired = mesh.shape["tp"] == 2 and mesh.shape["rep"] % 2 == 0
    chosen = functools.partial(pair_body, mesh.shape["rep"]) if paired else body
    return jax.shard_map(
        chosen,
        mesh=mesh,
        in_specs=placed,
        out_specs=(
            P("rep", None, "tp"),
            P("rep", None, "tp"),
            P("rep", None, "tp"),
            P("rep", None),
            P("rep", "tp", None),
            P("tp", None),
            P("tp", None),
        ),
        check_vma=False,
    )
```

```python
import functools

import jax
import jax.numpy as jnp
import numpy as np
from jax import lax
from jax.experimental import pallas as pl
from jax.experimental.pallas import tpu as pltpu
from jax.sharding import PartitionSpec as P

MESH = pl.DeviceIdType.MESH

HEAD_SIZE = 128


epsilon = 1e-05
rope_base = 500000.0
outer_rate = 0.7
outer_momentum = 0.9
LOG2_E = 1.4426950408889634


def rope_tables(sequence_length, width):
    middle = width // 2
    frequency = rope_base ** (-2.0 * jnp.arange(middle, dtype=jnp.float32) / width)
    angles = jnp.arange(sequence_length, dtype=jnp.float32)[:, None] * frequency[None, :]
    angles = jnp.concatenate([angles, angles], axis=1)
    return (jnp.cos(angles)[:, None, :], jnp.sin(angles)[:, None, :])


def rotate(vectors, cosine_table, sine_table):
    middle = vectors.shape[-1] // 2
    turned = jnp.concatenate([-vectors[..., middle:], vectors[..., :middle]], axis=-1)
    return vectors * cosine_table + turned * sine_table


def reverse_rotation(gradient, cosine_table, sine_table):
    middle = gradient.shape[-1] // 2
    shifted = gradient * sine_table
    turned = jnp.concatenate([shifted[..., middle:], -shifted[..., :middle]], axis=-1)
    return gradient * cosine_table + turned


def attention_reverse(query_rows, rotated_keys, values_bfloat, grad_out, block_of_rows):
    sequence_length = query_rows.shape[0]
    score_scale = query_rows.shape[-1] ** (-0.5)

    def one_block(running, block_index):
        acc_key, acc_value = running
        offset = block_index * block_of_rows
        query_block = lax.dynamic_slice_in_dim(query_rows, offset, block_of_rows, 0)
        grad_block = lax.dynamic_slice_in_dim(grad_out, offset, block_of_rows, 0)
        scores = (
            jnp.einsum(
                "qgrd,kgd->grqk", query_block, rotated_keys, preferred_element_type=jnp.float32
            )
            * score_scale
        )
        row_pos = offset + jnp.arange(block_of_rows)
        col_pos = jnp.arange(sequence_length)
        allowed = col_pos[None, :] <= row_pos[:, None]
        scores = jnp.where(allowed, scores, -jnp.inf)
        highest = jnp.max(scores, axis=-1, keepdims=True)
        powers = jnp.exp(scores - highest)
        probability = powers / jnp.sum(powers, axis=-1, keepdims=True)
        prob_low = probability.astype(jnp.bfloat16)
        acc_value = acc_value + jnp.einsum(
            "grqk,qgrd->kgd", prob_low, grad_block, preferred_element_type=jnp.float32
        )
        grad_prob = jnp.einsum(
            "qgrd,kgd->grqk", grad_block, values_bfloat, preferred_element_type=jnp.float32
        )
        grad_score = (
            probability
            * (grad_prob - jnp.sum(grad_prob * probability, axis=-1, keepdims=True))
            * score_scale
        )
        score_low = grad_score.astype(jnp.bfloat16)
        grad_query = jnp.einsum(
            "grqk,kgd->qgrd", score_low, rotated_keys, preferred_element_type=jnp.float32
        )
        acc_key = acc_key + jnp.einsum(
            "grqk,qgrd->kgd", score_low, query_block, preferred_element_type=jnp.float32
        )
        return ((acc_key, acc_value), grad_query)

    initial = jnp.zeros(rotated_keys.shape, jnp.float32)
    (acc_key, acc_value), grad_blocks = lax.scan(
        one_block, (initial, initial), jnp.arange(sequence_length // block_of_rows)
    )
    return (grad_blocks.reshape(query_rows.shape), acc_key, acc_value)


def body(
    tokens,
    norm_gain,
    w_query,
    key_weight,
    value_weight,
    attention_gradient,
    global_fragment,
    momentum,
    local_fragment,
):
    local_rows = tokens[0]
    norm_gains = norm_gain[0]
    weight_q = w_query[0]
    weight_k = key_weight[0]
    weight_v = value_weight[0]
    widened_rows = local_rows.astype(jnp.float32)
    inverse_norm = lax.rsqrt(
        jnp.mean(widened_rows * widened_rows, axis=-1, keepdims=True) + epsilon
    )
    normalized_input = widened_rows * inverse_norm
    normalized_local = (normalized_input * norm_gains[None, :]).astype(jnp.bfloat16)
    normalized = lax.all_gather(normalized_local, "tp", axis=0, tiled=True)
    sequence_length = normalized.shape[0]
    heads_q = weight_q.shape[1] // HEAD_SIZE
    heads_kv = weight_k.shape[1] // HEAD_SIZE
    cosine_table, sine_table = rope_tables(sequence_length, HEAD_SIZE)
    query_rows = jnp.dot(normalized, weight_q, preferred_element_type=jnp.float32).reshape(
        sequence_length, heads_q, HEAD_SIZE
    )
    query_rows = rotate(query_rows, cosine_table, sine_table).astype(jnp.bfloat16)
    rotated_keys = jnp.dot(normalized, weight_k, preferred_element_type=jnp.float32).reshape(
        sequence_length, heads_kv, HEAD_SIZE
    )
    rotated_keys = rotate(rotated_keys, cosine_table, sine_table).astype(jnp.bfloat16)
    values_bfloat = (
        jnp.dot(normalized, weight_v, preferred_element_type=jnp.float32)
        .astype(jnp.bfloat16)
        .reshape(sequence_length, heads_kv, HEAD_SIZE)
    )
    replica_group = heads_q // heads_kv
    block_of_rows = min(512, sequence_length)
    query_input_gradient, key_input_gradient, value_input_gradient = attention_reverse(
        query_rows.reshape(sequence_length, heads_kv, replica_group, HEAD_SIZE),
        rotated_keys,
        values_bfloat,
        attention_gradient[0].reshape(sequence_length, heads_kv, replica_group, HEAD_SIZE),
        block_of_rows,
    )
    dquery = (
        reverse_rotation(
            query_input_gradient.reshape(sequence_length, heads_q, HEAD_SIZE),
            cosine_table,
            sine_table,
        )
        .astype(jnp.bfloat16)
        .reshape(sequence_length, heads_q * HEAD_SIZE)
    )
    key_gradient = (
        reverse_rotation(key_input_gradient, cosine_table, sine_table)
        .astype(jnp.bfloat16)
        .reshape(sequence_length, heads_kv * HEAD_SIZE)
    )
    value_gradient = value_input_gradient.astype(jnp.bfloat16).reshape(
        sequence_length, heads_kv * HEAD_SIZE
    )
    contract = (((0,), (0,)), ((), ()))
    grad_wq = lax.dot_general(
        normalized, dquery, contract, preferred_element_type=jnp.float32
    ).astype(jnp.bfloat16)
    grad_wk = lax.dot_general(
        normalized, key_gradient, contract, preferred_element_type=jnp.float32
    ).astype(jnp.bfloat16)
    grad_wv = lax.dot_general(
        normalized, value_gradient, contract, preferred_element_type=jnp.float32
    ).astype(jnp.bfloat16)
    back = (((1,), (1,)), ((), ()))
    partial_value = lax.dot_general(dquery, weight_q, back, preferred_element_type=jnp.float32)
    partial_value = partial_value + lax.dot_general(
        key_gradient, weight_k, back, preferred_element_type=jnp.float32
    )
    summed_rows = lax.psum_scatter(
        (
            partial_value
            + lax.dot_general(value_gradient, weight_v, back, preferred_element_type=jnp.float32)
        ).astype(jnp.bfloat16),
        "tp",
        scatter_dimension=0,
        tiled=True,
    ).astype(jnp.float32)
    gains_gradient = lax.psum(jnp.sum(summed_rows * normalized_input, axis=0), "tp")
    scaled_rows = summed_rows * norm_gains[None, :]
    gradient_rows = (
        inverse_norm
        * (
            scaled_rows
            - normalized_input * jnp.mean(scaled_rows * normalized_input, axis=-1, keepdims=True)
        )
    ).astype(jnp.bfloat16)
    delta = global_fragment - local_fragment[0].astype(jnp.float32)
    replicas = lax.axis_size("rep")
    mean_delta = lax.psum(delta, "rep") / replicas
    new_momentum = outer_momentum * momentum + mean_delta
    new_global = global_fragment - outer_rate * (mean_delta + outer_momentum * new_momentum)
    return (
        grad_wq[None],
        grad_wk[None],
        grad_wv[None],
        gains_gradient[None],
        gradient_rows[None],
        new_global,
        new_momentum,
    )

NT = (((1,), (1,)), ((), ()))
TN = (((0,), (0,)), ((), ()))


def dot(a, b, dims=(((1,), (0,)), ((), ()))):
    return lax.dot_general(a, b, dims, preferred_element_type=jnp.float32)


def ds(index, size):
    return pl.ds(pl.multiple_of(index * size, size), size)


def host_tables(sequence_length, width):
    middle = width // 2
    frequency = rope_base ** (-2.0 * np.arange(middle) / width)
    angles = np.arange(sequence_length)[:, None] * frequency[None, :]
    cosine, sine = np.cos(angles), np.sin(angles)
    return (
        jnp.asarray(np.concatenate([cosine, cosine], axis=1), jnp.float32),
        jnp.asarray(np.concatenate([-sine, sine], axis=1), jnp.float32),
    )


def front_kernel(
    n_rep,
    chunks,
    tile,
    tokens_hbm,
    gain_hbm,
    wq_hbm,
    wk_hbm,
    wv_hbm,
    go_hbm,
    cos_hbm,
    sin_hbm,
    local_hbm,
    x_ref,
    nm_ref,
    d_ref,
    here_ref,
    far_ref,
    gain_part_ref,
    mean_ref,
    gain_ref,
    go_ref,
    cos_ref,
    sin_ref,
    w_ref,
    acc_ref,
    q_ref,
    k_ref,
    v_ref,
    pieces_ref,
    own_mean_ref,
    in_sems,
    w_sems,
    ag_send,
    ag_recv,
    fr_send,
    fr_recv,
    fg_send,
    fg_recv,
    own_sem,
    go_sem,
):
    me = lax.axis_index("tp")
    peer = 1 - me
    rep = lax.axis_index("rep")
    side = lax.rem(rep, 2)
    rows, width = x_ref.shape
    qw, kw = wq_hbm.shape[1], wk_hbm.shape[1]
    total = qw + 2 * kw
    cw = width // chunks
    piece_rows, piece_cols = own_mean_ref.shape
    col_blocks = width // piece_cols
    barrier = pltpu.get_barrier_semaphore()
    pl.semaphore_signal(barrier, inc=1, device_id={"tp": peer}, device_id_type=MESH)

    def greet(j, _):
        pl.semaphore_signal(
            barrier, inc=1, device_id={"rep": lax.rem(rep + j, n_rep)}, device_id_type=MESH
        )
        return 0

    lax.fori_loop(1, n_rep, greet, 0)
    first_copies = [
        pltpu.make_async_copy(tokens_hbm, x_ref, in_sems.at[0]),
        pltpu.make_async_copy(gain_hbm, gain_ref, in_sems.at[1]),
    ]
    late_copies = [
        pltpu.make_async_copy(cos_hbm, cos_ref, in_sems.at[2]),
        pltpu.make_async_copy(sin_hbm, sin_ref, in_sems.at[3]),
        pltpu.make_async_copy(go_hbm, go_ref, in_sems.at[4]),
    ]
    weight_copies = []
    for source, offset in ((wq_hbm, 0), (wk_hbm, qw), (wv_hbm, qw + kw)):
        for t in range(source.shape[1] // tile):
            weight_copies.append(
                pltpu.make_async_copy(
                    source.at[:, pl.ds(t * tile, tile)],
                    w_ref.at[:, pl.ds(offset + t * tile, tile)],
                    w_sems.at[len(weight_copies)],
                )
            )

    def piece(owner):
        return (
            ds(owner // col_blocks, piece_rows),
            ds(lax.rem(owner, col_blocks), piece_cols),
        )

    own_piece = pltpu.make_async_copy(local_hbm.at[piece(rep)], pieces_ref.at[0], own_sem)
    for copy in first_copies + weight_copies[:1] + late_copies[:2] + weight_copies[1:]:
        copy.start()
    own_piece.start()
    late_copies[2].start()
    for copy in first_copies:
        copy.wait()

    step = 16

    def norm_rows(i, _):
        x = x_ref[ds(i, step), :].astype(jnp.float32)
        inverse = lax.rsqrt(jnp.mean(x * x, axis=-1, keepdims=True) + epsilon)
        nm_ref[pl.ds(pl.multiple_of(me * rows + i * step, step), step), :] = (
            x * inverse * gain_ref[...]
        ).astype(jnp.bfloat16)
        return 0

    lax.fori_loop(0, rows // step, norm_rows, 0)
    pl.semaphore_wait(barrier, n_rep)

    def gather_copy(c):
        part = nm_ref.at[ds(me, rows), ds(c, cw)]
        return pltpu.make_async_remote_copy(
            src_ref=part,
            dst_ref=part,
            send_sem=ag_send.at[c],
            recv_sem=ag_recv.at[c],
            device_id={"tp": peer},
            device_id_type=MESH,
        )

    def scatter_copy(j):
        target = lax.rem(rep + j, n_rep)
        return pltpu.make_async_remote_copy(
            src_ref=local_hbm.at[piece(target)],
            dst_ref=pieces_ref.at[j],
            send_sem=fr_send.at[j],
            recv_sem=fr_recv.at[j],
            device_id={"rep": target},
            device_id_type=MESH,
        )

    def spread_copy(j, owner):
        return pltpu.make_async_remote_copy(
            src_ref=own_mean_ref,
            dst_ref=mean_ref.at[piece(owner)],
            send_sem=fg_send.at[j],
            recv_sem=fg_recv.at[j],
            device_id={"rep": lax.rem(rep + j, n_rep)},
            device_id_type=MESH,
        )

    def start_all(make, low, high):
        def one(j, _):
            make(j).start()
            return 0

        lax.fori_loop(low, high, one, 0)

    def wait_recv_all(make, low, high):
        def one(j, _):
            make(j).wait_recv()
            return 0

        lax.fori_loop(low, high, one, 0)

    def wait_send_all(make, low, high):
        def one(j, _):
            make(j).wait_send()
            return 0

        lax.fori_loop(low, high, one, 0)

    @pl.when(side == 0)
    def _():
        start_all(gather_copy, 0, chunks)

    start_all(scatter_copy, 1, n_rep)

    for t, copy in enumerate(weight_copies):
        copy.wait()
        acc_ref[ds(me, rows), pl.ds(t * tile, tile)] = dot(
            nm_ref[ds(me, rows), :], w_ref[:, pl.ds(t * tile, tile)]
        )
    acc_ref[ds(peer, rows), :] = jnp.zeros((rows, total), jnp.float32)
    for copy in late_copies:
        copy.wait()

    heads_q, heads_kv = qw // HEAD_SIZE, kw // HEAD_SIZE

    def rope_rows(which):
        block = ds(which, rows)
        cosine, sine = cos_ref[block, :], sin_ref[block, :]

        def rope_head(source, target, index):
            vector = acc_ref[block, pl.ds(source * HEAD_SIZE, HEAD_SIZE)]
            target[block, pl.ds(index * HEAD_SIZE, HEAD_SIZE)] = (
                vector * cosine + pltpu.roll(vector, HEAD_SIZE // 2, 1) * sine
            ).astype(jnp.bfloat16)

        for h in range(heads_q):
            rope_head(h, q_ref, h)
        for h in range(heads_kv):
            rope_head(heads_q + h, k_ref, h)
        v_ref[block, :] = acc_ref[block, pl.ds(qw + kw, kw)].astype(jnp.bfloat16)

    rope_rows(me)

    def average_pieces():
        own_piece.wait()
        wait_recv_all(scatter_copy, 1, n_rep)
        summed = pieces_ref[0].astype(jnp.float32)
        for j in range(1, n_rep):
            summed = summed + pieces_ref[j].astype(jnp.float32)
        summed = (summed * (1.0 / n_rep)).astype(jnp.bfloat16)
        own_mean_ref[...] = summed
        mean_ref[piece(rep)] = summed
        start_all(lambda j: spread_copy(j, rep), 1, n_rep)

    @pl.when(side == 1)
    def _():
        pl.semaphore_wait(go_sem, 1)
        start_all(gather_copy, 0, chunks)
        average_pieces()

    def arrived(c, _):
        pltpu.make_async_remote_copy(
            src_ref=nm_ref.at[ds(peer, rows), ds(c, cw)],
            dst_ref=nm_ref.at[ds(peer, rows), ds(c, cw)],
            send_sem=ag_send.at[c],
            recv_sem=ag_recv.at[c],
            device_id={"tp": peer},
            device_id_type=MESH,
        ).wait_recv()

        @pl.when((side == 0) & (c == chunks - 2))
        def _():
            pl.semaphore_signal(
                go_sem, inc=1, device_id={"rep": lax.rem(rep + 1, n_rep)}, device_id_type=MESH
            )

        part = nm_ref[ds(peer, rows), ds(c, cw)]

        def one(t, _):
            acc_ref[ds(peer, rows), ds(t, tile)] += dot(part, w_ref[ds(c, cw), ds(t, tile)])
            return 0

        lax.fori_loop(0, total // tile, one, 0)
        return 0

    lax.fori_loop(0, chunks, arrived, 0)
    rope_rows(peer)

    group = heads_q // heads_kv
    scale = HEAD_SIZE ** (-0.5)
    key_pos = lax.broadcasted_iota(jnp.int32, (rows, rows), 0)
    query_pos = lax.broadcasted_iota(jnp.int32, (rows, rows), 1)
    bias = jnp.where(key_pos <= query_pos, 0.0, -jnp.inf).astype(jnp.float32)
    bias = jnp.concatenate([bias] * group, axis=1)

    def reverse(gradient, block):
        c = cos_ref[block * rows : (block + 1) * rows]
        s = sin_ref[block * rows : (block + 1) * rows]
        return (gradient * c - pltpu.roll(gradient, HEAD_SIZE // 2, 1) * s).astype(jnp.bfloat16)

    def kv_head(g, _):
        @pl.when((side == 0) & (g == 1))
        def _():
            average_pieces()

        grad_k = [None, None]
        grad_v = [None, None]
        kv = ds(g, HEAD_SIZE)
        for b in range(2):
            keys = (b + 1) * rows
            block = pl.ds(b * rows, rows)
            heads = [ds(g * group + r, HEAD_SIZE) for r in range(group)]
            query = jnp.concatenate([q_ref[block, head] for head in heads], axis=0)
            out_grad = jnp.concatenate([go_ref[block, head] for head in heads], axis=0)
            key = k_ref[pl.ds(0, keys), kv]
            value = v_ref[pl.ds(0, keys), kv]
            scores = dot(key, query, NT)
            grad_prob = dot(value, out_grad, NT)
            if b == 0:
                scores = scores + bias
            else:
                scores = jnp.concatenate([scores[:rows], scores[rows:] + bias], axis=0)
            highest = jnp.max(scores, axis=0, keepdims=True)
            powers = jnp.exp2((scores - highest) * (scale * LOG2_E))
            prob = powers * (1.0 / jnp.sum(powers, axis=0, keepdims=True))
            inner = jnp.sum(grad_prob * prob, axis=0, keepdims=True)
            score_low = (prob * (grad_prob - inner) * scale).astype(jnp.bfloat16)
            grad_q = dot(score_low, key, TN)
            for r, head in enumerate(heads):
                d_ref[block, head] = reverse(grad_q[r * rows : (r + 1) * rows], b)
            part_v = dot(prob.astype(jnp.bfloat16), out_grad)
            part_k = dot(score_low, query)
            for j in range(b + 1):
                pv = part_v[j * rows : (j + 1) * rows]
                pk = part_k[j * rows : (j + 1) * rows]
                grad_v[j] = pv if grad_v[j] is None else grad_v[j] + pv
                grad_k[j] = pk if grad_k[j] is None else grad_k[j] + pk
        for j in range(2):
            block = pl.ds(j * rows, rows)
            d_ref[block, ds(heads_q + g, HEAD_SIZE)] = reverse(grad_k[j], j)
            d_ref[block, ds(heads_q + heads_kv + g, HEAD_SIZE)] = grad_v[j].astype(jnp.bfloat16)
        return 0

    lax.fori_loop(0, heads_kv, kv_head, 0)

    def back(t, _):
        both = jnp.concatenate([d_ref[ds(peer, rows), :], d_ref[ds(me, rows), :]], axis=0)
        part = dot(both, w_ref[ds(t, tile), :], NT).astype(jnp.bfloat16)
        cols = ds(t, tile)
        far_ref[pl.ds(0, rows), cols] = part[:rows]
        here_ref[:, cols] = part[rows:]
        wide = part.astype(jnp.float32)
        products = wide[:rows] * nm_ref[ds(peer, rows), cols].astype(jnp.float32)
        products += wide[rows:] * nm_ref[ds(me, rows), cols].astype(jnp.float32)
        gain_part = jnp.sum(products, axis=0, keepdims=True) / gain_ref[:, cols]
        gain_part_ref[:, cols] = gain_part
        lines = []
        for _ in range(3):
            lines.append(gain_part.astype(jnp.bfloat16).astype(jnp.float32))
            gain_part = gain_part - lines[-1]
        lines = jnp.concatenate(lines + [jnp.zeros((pad - 3, tile), jnp.float32)], axis=0)
        far_ref[pl.ds(rows, pad), cols] = lines.astype(jnp.bfloat16)
        return 0

    pad = far_ref.shape[0] - rows
    lax.fori_loop(0, width // tile, back, 0)

    wait_recv_all(lambda j: spread_copy(j, lax.rem(rep + n_rep - j, n_rep)), 1, n_rep)
    wait_send_all(gather_copy, 0, chunks)
    wait_send_all(scatter_copy, 1, n_rep)
    wait_send_all(lambda j: spread_copy(j, rep), 1, n_rep)


def weights_kernel(nm_ref, d_ref, mean_ref, global_ref, momentum_ref, gq_ref, gk_ref, gv_ref, ng_ref, nmom_ref):
    i = pl.program_id(0)
    wide = gq_ref.shape[0]
    qw, kw = gq_ref.shape[1], gk_ref.shape[1]
    grad = dot(nm_ref[:, ds(i, wide)], d_ref[...], TN).astype(jnp.bfloat16)
    gq_ref[...] = grad[:, :qw]
    gk_ref[...] = grad[:, qw : qw + kw]
    gv_ref[...] = grad[:, qw + kw :]
    held = global_ref[...]
    mean_delta = held - mean_ref[:, ds(i, wide)].astype(jnp.float32)
    new_momentum = outer_momentum * momentum_ref[...] + mean_delta
    nmom_ref[...] = new_momentum
    ng_ref[...] = held - outer_rate * (mean_delta + outer_momentum * new_momentum)


def rows_kernel(x_ref, here_ref, gain_ref, landed_ref, gain_part_ref, out_ref, gain_out_ref):
    i = pl.program_id(0)
    count = out_ref.shape[0]
    rows, width = x_ref.shape

    @pl.when(i == 0)
    def _():
        lines = landed_ref[pl.ds(rows, landed_ref.shape[0] - rows), :].astype(jnp.float32)
        gain_out_ref[...] = gain_part_ref[...] + (lines[2:3] + lines[1:2] + lines[:1])

    step = 16

    def some(j, _):
        block = pl.ds(pl.multiple_of(i * count + j * step, step), step)
        x = x_ref[block, :].astype(jnp.float32)
        inverse = lax.rsqrt(jnp.mean(x * x, axis=-1, keepdims=True) + epsilon)
        scaled = (
            here_ref[block, :].astype(jnp.float32) + landed_ref[block, :].astype(jnp.float32)
        ) * gain_ref[...]
        pull = jnp.mean(scaled * x, axis=-1, keepdims=True) * (inverse * inverse)
        out_ref[ds(j, step), :] = (inverse * (scaled - x * pull)).astype(jnp.bfloat16)
        return 0

    lax.fori_loop(0, count // step, some, 0, unroll=2)


def pair_body(
    n_rep,
    tokens,
    norm_gain,
    w_query,
    key_weight,
    value_weight,
    attention_gradient,
    global_fragment,
    momentum,
    local_fragment,
):
    rows, width = tokens.shape[1:]
    sequence = 2 * rows
    weight_q, weight_k, weight_v = w_query[0], key_weight[0], value_weight[0]
    qw, kw = weight_q.shape[1], weight_k.shape[1]
    total = qw + 2 * kw
    frag_rows = local_fragment.shape[1]
    piece_rows = 16
    piece_cols = width * frag_rows // piece_rows // n_rep
    chunks = 6
    tile = 512
    pad = 8
    bf16, f32 = jnp.bfloat16, jnp.float32
    cosine, sine = host_tables(sequence, HEAD_SIZE)
    vmem = pl.BlockSpec(memory_space=pltpu.VMEM)
    hbm = pl.BlockSpec(memory_space=pltpu.HBM)
    x, normed, d, here, far, gain_partial, mean_local = pl.pallas_call(
        functools.partial(front_kernel, n_rep, chunks, tile),
        out_shape=(
            pltpu.VMEM((rows, width), bf16),
            pltpu.VMEM((sequence, width), bf16),
            pltpu.VMEM((sequence, total), bf16),
            pltpu.VMEM((rows, width), bf16),
            pltpu.VMEM((rows + pad, width), bf16),
            pltpu.VMEM((1, width), f32),
            pltpu.VMEM((frag_rows, width), bf16),
        ),
        in_specs=[hbm] * 9,
        out_specs=(vmem,) * 7,
        scratch_shapes=[
            pltpu.VMEM((1, width), f32),
            pltpu.VMEM((sequence, qw), bf16),
            pltpu.VMEM((sequence, HEAD_SIZE), f32),
            pltpu.VMEM((sequence, HEAD_SIZE), f32),
            pltpu.VMEM((width, total), bf16),
            pltpu.VMEM((sequence, total), f32),
            pltpu.VMEM((sequence, qw), bf16),
            pltpu.VMEM((sequence, kw), bf16),
            pltpu.VMEM((sequence, kw), bf16),
            pltpu.VMEM((n_rep, piece_rows, piece_cols), bf16),
            pltpu.VMEM((piece_rows, piece_cols), bf16),
            pltpu.SemaphoreType.DMA((5,)),
            pltpu.SemaphoreType.DMA((total // tile,)),
            pltpu.SemaphoreType.DMA((chunks,)),
            pltpu.SemaphoreType.DMA((chunks,)),
            pltpu.SemaphoreType.DMA((n_rep,)),
            pltpu.SemaphoreType.DMA((n_rep,)),
            pltpu.SemaphoreType.DMA((n_rep,)),
            pltpu.SemaphoreType.DMA((n_rep,)),
            pltpu.SemaphoreType.DMA,
            pltpu.SemaphoreType.REGULAR,
        ],
        compiler_params=pltpu.CompilerParams(
            collective_id=0, has_side_effects=True, vmem_limit_bytes=48 * 1024 * 1024
        ),
    )(
        *[
            pltpu.with_memory_space_constraint(array, pltpu.HBM)
            for array in (
                tokens[0],
                norm_gain,
                weight_q,
                weight_k,
                weight_v,
                attention_gradient[0],
                cosine,
                sine,
                local_fragment[0],
            )
        ]
    )
    swap = [(0, 1), (1, 0)]
    landed = lax.ppermute(far, "tp", swap)
    wide = 256
    columns = lambda size: pl.BlockSpec((size, wide), lambda i: (0, i))
    grad_wq, grad_wk, grad_wv, new_global, new_momentum = pl.pallas_call(
        weights_kernel,
        grid=(width // wide,),
        out_shape=(
            jax.ShapeDtypeStruct((width, qw), bf16),
            jax.ShapeDtypeStruct((width, kw), bf16),
            jax.ShapeDtypeStruct((width, kw), bf16),
            jax.ShapeDtypeStruct((frag_rows, width), f32),
            jax.ShapeDtypeStruct((frag_rows, width), f32),
        ),
        in_specs=[vmem, vmem, vmem, columns(frag_rows), columns(frag_rows)],
        out_specs=(
            pl.BlockSpec((wide, qw), lambda i: (i, 0)),
            pl.BlockSpec((wide, kw), lambda i: (i, 0)),
            pl.BlockSpec((wide, kw), lambda i: (i, 0)),
            columns(frag_rows),
            columns(frag_rows),
        ),
        compiler_params=pltpu.CompilerParams(vmem_limit_bytes=16 * 1024 * 1024),
        cost_estimate=pl.CostEstimate(
            flops=2 * sequence * width * total, bytes_accessed=3 * width * total, transcendentals=0
        ),
    )(normed, d, mean_local, global_fragment, momentum)
    count = 32
    block = pl.BlockSpec((count, width), lambda i: (i, 0))
    gradient_rows, gains_gradient = pl.pallas_call(
        rows_kernel,
        grid=(rows // count,),
        out_shape=(
            jax.ShapeDtypeStruct((rows, width), bf16),
            jax.ShapeDtypeStruct((1, width), f32),
        ),
        in_specs=[vmem] * 5,
        out_specs=(block, pl.BlockSpec((1, width), lambda i: (0, 0))),
        compiler_params=pltpu.CompilerParams(vmem_limit_bytes=8 * 1024 * 1024),
        cost_estimate=pl.CostEstimate(
            flops=12 * rows * width, bytes_accessed=4 * rows * width, transcendentals=0
        ),
    )(x, here, norm_gain, landed, gain_partial)
    return (
        grad_wq[None],
        grad_wk[None],
        grad_wv[None],
        gains_gradient,
        gradient_rows[None],
        new_global,
        new_momentum,
    )


def solution(mesh):
    placed = (
        P("rep", "tp", None),
        P("rep", None),
        P("rep", None, "tp"),
        P("rep", None, "tp"),
        P("rep", None, "tp"),
        P("rep", None, "tp"),
        P("tp", None),
        P("tp", None),
        P("rep", "tp", None),
    )
    paired = mesh.shape["tp"] == 2 and mesh.shape["rep"] % 2 == 0
    chosen = functools.partial(pair_body, mesh.shape["rep"]) if paired else body
    return jax.shard_map(
        chosen,
        mesh=mesh,
        in_specs=placed,
        out_specs=(
            P("rep", None, "tp"),
            P("rep", None, "tp"),
            P("rep", None, "tp"),
            P("rep", None),
            P("rep", "tp", None),
            P("tp", None),
            P("tp", None),
        ),
        check_vma=False,
    )
```

```python
import functools

import jax
import jax.numpy as jnp
import numpy as np
from jax import lax
from jax.experimental import pallas as pl
from jax.experimental.pallas import tpu as pltpu
from jax.sharding import PartitionSpec as P


MESH = pl.DeviceIdType.MESH

HEAD_SIZE = 128


epsilon = 1e-05
rope_base = 500000.0
outer_rate = 0.7
outer_momentum = 0.9
LOG2_E = 1.4426950408889634
LANES = 128
SUBLANES = 8


def rope_tables(sequence_length, width):
    middle = width // 2
    frequency = rope_base ** (-2.0 * jnp.arange(middle, dtype=jnp.float32) / width)
    angles = jnp.arange(sequence_length, dtype=jnp.float32)[:, None] * frequency[None, :]
    angles = jnp.concatenate([angles, angles], axis=1)
    return (jnp.cos(angles)[:, None, :], jnp.sin(angles)[:, None, :])


def rotate(vectors, cosine_table, sine_table):
    middle = vectors.shape[-1] // 2
    turned = jnp.concatenate([-vectors[..., middle:], vectors[..., :middle]], axis=-1)
    return vectors * cosine_table + turned * sine_table


def reverse_rotation(gradient, cosine_table, sine_table):
    middle = gradient.shape[-1] // 2
    shifted = gradient * sine_table
    turned = jnp.concatenate([shifted[..., middle:], -shifted[..., :middle]], axis=-1)
    return gradient * cosine_table + turned


def attention_reverse(query_rows, rotated_keys, values_bfloat, grad_out, block_of_rows):
    sequence_length = query_rows.shape[0]
    score_scale = query_rows.shape[-1] ** (-0.5)

    def one_block(running, block_index):
        acc_key, acc_value = running
        offset = block_index * block_of_rows
        query_block = lax.dynamic_slice_in_dim(query_rows, offset, block_of_rows, 0)
        grad_block = lax.dynamic_slice_in_dim(grad_out, offset, block_of_rows, 0)
        scores = (
            jnp.einsum(
                "qgrd,kgd->grqk", query_block, rotated_keys, preferred_element_type=jnp.float32
            )
            * score_scale
        )
        row_pos = offset + jnp.arange(block_of_rows)
        col_pos = jnp.arange(sequence_length)
        allowed = col_pos[None, :] <= row_pos[:, None]
        scores = jnp.where(allowed, scores, -jnp.inf)
        highest = jnp.max(scores, axis=-1, keepdims=True)
        powers = jnp.exp(scores - highest)
        probability = powers / jnp.sum(powers, axis=-1, keepdims=True)
        prob_low = probability.astype(jnp.bfloat16)
        acc_value = acc_value + jnp.einsum(
            "grqk,qgrd->kgd", prob_low, grad_block, preferred_element_type=jnp.float32
        )
        grad_prob = jnp.einsum(
            "qgrd,kgd->grqk", grad_block, values_bfloat, preferred_element_type=jnp.float32
        )
        grad_score = (
            probability
            * (grad_prob - jnp.sum(grad_prob * probability, axis=-1, keepdims=True))
            * score_scale
        )
        score_low = grad_score.astype(jnp.bfloat16)
        grad_query = jnp.einsum(
            "grqk,kgd->qgrd", score_low, rotated_keys, preferred_element_type=jnp.float32
        )
        acc_key = acc_key + jnp.einsum(
            "grqk,qgrd->kgd", score_low, query_block, preferred_element_type=jnp.float32
        )
        return ((acc_key, acc_value), grad_query)

    initial = jnp.zeros(rotated_keys.shape, jnp.float32)
    (acc_key, acc_value), grad_blocks = lax.scan(
        one_block, (initial, initial), jnp.arange(sequence_length // block_of_rows)
    )
    return (grad_blocks.reshape(query_rows.shape), acc_key, acc_value)


def body(
    tokens,
    norm_gain,
    w_query,
    key_weight,
    value_weight,
    attention_gradient,
    global_fragment,
    momentum,
    local_fragment,
):
    local_rows = tokens[0]
    norm_gains = norm_gain[0]
    weight_q = w_query[0]
    weight_k = key_weight[0]
    weight_v = value_weight[0]
    widened_rows = local_rows.astype(jnp.float32)
    inverse_norm = lax.rsqrt(
        jnp.mean(widened_rows * widened_rows, axis=-1, keepdims=True) + epsilon
    )
    normalized_input = widened_rows * inverse_norm
    normalized_local = (normalized_input * norm_gains[None, :]).astype(jnp.bfloat16)
    normalized = lax.all_gather(normalized_local, "tp", axis=0, tiled=True)
    sequence_length = normalized.shape[0]
    heads_q = weight_q.shape[1] // HEAD_SIZE
    heads_kv = weight_k.shape[1] // HEAD_SIZE
    cosine_table, sine_table = rope_tables(sequence_length, HEAD_SIZE)
    query_rows = jnp.dot(normalized, weight_q, preferred_element_type=jnp.float32).reshape(
        sequence_length, heads_q, HEAD_SIZE
    )
    query_rows = rotate(query_rows, cosine_table, sine_table).astype(jnp.bfloat16)
    rotated_keys = jnp.dot(normalized, weight_k, preferred_element_type=jnp.float32).reshape(
        sequence_length, heads_kv, HEAD_SIZE
    )
    rotated_keys = rotate(rotated_keys, cosine_table, sine_table).astype(jnp.bfloat16)
    values_bfloat = (
        jnp.dot(normalized, weight_v, preferred_element_type=jnp.float32)
        .astype(jnp.bfloat16)
        .reshape(sequence_length, heads_kv, HEAD_SIZE)
    )
    replica_group = heads_q // heads_kv
    block_of_rows = min(512, sequence_length)
    query_input_gradient, key_input_gradient, value_input_gradient = attention_reverse(
        query_rows.reshape(sequence_length, heads_kv, replica_group, HEAD_SIZE),
        rotated_keys,
        values_bfloat,
        attention_gradient[0].reshape(sequence_length, heads_kv, replica_group, HEAD_SIZE),
        block_of_rows,
    )
    dquery = (
        reverse_rotation(
            query_input_gradient.reshape(sequence_length, heads_q, HEAD_SIZE),
            cosine_table,
            sine_table,
        )
        .astype(jnp.bfloat16)
        .reshape(sequence_length, heads_q * HEAD_SIZE)
    )
    key_gradient = (
        reverse_rotation(key_input_gradient, cosine_table, sine_table)
        .astype(jnp.bfloat16)
        .reshape(sequence_length, heads_kv * HEAD_SIZE)
    )
    value_gradient = value_input_gradient.astype(jnp.bfloat16).reshape(
        sequence_length, heads_kv * HEAD_SIZE
    )
    contract = (((0,), (0,)), ((), ()))
    grad_wq = lax.dot_general(
        normalized, dquery, contract, preferred_element_type=jnp.float32
    ).astype(jnp.bfloat16)
    grad_wk = lax.dot_general(
        normalized, key_gradient, contract, preferred_element_type=jnp.float32
    ).astype(jnp.bfloat16)
    grad_wv = lax.dot_general(
        normalized, value_gradient, contract, preferred_element_type=jnp.float32
    ).astype(jnp.bfloat16)
    back = (((1,), (1,)), ((), ()))
    partial_value = lax.dot_general(dquery, weight_q, back, preferred_element_type=jnp.float32)
    partial_value = partial_value + lax.dot_general(
        key_gradient, weight_k, back, preferred_element_type=jnp.float32
    )
    summed_rows = lax.psum_scatter(
        (
            partial_value
            + lax.dot_general(value_gradient, weight_v, back, preferred_element_type=jnp.float32)
        ).astype(jnp.bfloat16),
        "tp",
        scatter_dimension=0,
        tiled=True,
    ).astype(jnp.float32)
    gains_gradient = lax.psum(jnp.sum(summed_rows * normalized_input, axis=0), "tp")
    scaled_rows = summed_rows * norm_gains[None, :]
    gradient_rows = (
        inverse_norm
        * (
            scaled_rows
            - normalized_input * jnp.mean(scaled_rows * normalized_input, axis=-1, keepdims=True)
        )
    ).astype(jnp.bfloat16)
    delta = global_fragment - local_fragment[0].astype(jnp.float32)
    replicas = lax.axis_size("rep")
    mean_delta = lax.psum(delta, "rep") / replicas
    new_momentum = outer_momentum * momentum + mean_delta
    new_global = global_fragment - outer_rate * (mean_delta + outer_momentum * new_momentum)
    return (
        grad_wq[None],
        grad_wk[None],
        grad_wv[None],
        gains_gradient[None],
        gradient_rows[None],
        new_global,
        new_momentum,
    )


NT = (((1,), (1,)), ((), ()))
TN = (((0,), (0,)), ((), ()))


def dot(a, b, dims=(((1,), (0,)), ((), ()))):
    return lax.dot_general(a, b, dims, preferred_element_type=jnp.float32)


def ds(index, size):
    return pl.ds(pl.multiple_of(index * size, size), size)


def host_tables(sequence_length, width):
    middle = width // 2
    frequency = rope_base ** (-2.0 * np.arange(middle) / width)
    angles = np.arange(sequence_length)[:, None] * frequency[None, :]
    cosine, sine = np.cos(angles), np.sin(angles)
    return (
        jnp.asarray(np.concatenate([cosine, cosine], axis=1), jnp.float32),
        jnp.asarray(np.concatenate([-sine, sine], axis=1), jnp.float32),
    )


def shares(d_ref, nm_ref, w_ref, gain_ref, far_ref, here_ref, gain_part_ref, low, tile):
    me = lax.axis_index("tp")
    peer = 1 - me
    rows = here_ref.shape[0]
    offset = gain_part_ref.shape[1] - here_ref.shape[1] if low else 0

    def back(t, _):
        both = jnp.concatenate([d_ref[ds(peer, rows), :], d_ref[ds(me, rows), :]], axis=0)
        cols = pl.ds(pl.multiple_of(low + t * tile, tile), tile)
        own = ds(t, tile)
        part = dot(both, w_ref[cols, :], NT).astype(jnp.bfloat16)
        far_ref[pl.ds(0, rows), own] = part[:rows]
        here_ref[:, own] = part[rows:]
        wide = part.astype(jnp.float32)
        products = wide[:rows] * nm_ref[ds(peer, rows), cols].astype(jnp.float32)
        products += wide[rows:] * nm_ref[ds(me, rows), cols].astype(jnp.float32)
        gain_part = jnp.sum(products, axis=0, keepdims=True) / gain_ref[:, cols]
        gain_part_ref[:, pl.ds(pl.multiple_of(offset + t * tile, tile), tile)] = gain_part
        return 0

    lax.fori_loop(0, here_ref.shape[1] // tile, back, 0)


def front_kernel(
    n_rep,
    chunks,
    tile,
    tokens_hbm,
    gain_hbm,
    wq_hbm,
    wk_hbm,
    wv_hbm,
    go_hbm,
    cos_hbm,
    sin_hbm,
    local_hbm,
    x_ref,
    nm_ref,
    d_ref,
    here_ref,
    far_ref,
    gain_part_ref,
    mean_ref,
    w_ref,
    gain_ref,
    go_ref,
    cos_ref,
    sin_ref,
    acc_ref,
    q_ref,
    k_ref,
    v_ref,
    raw_ref,
    wide_ref,
    inv_ref,
    mine_ref,
    theirs_ref,
    pair_ref,
    pieces_ref,
    own_mean_ref,
    in_sems,
    w_sems,
    ag_send,
    ag_recv,
    fr_send,
    fr_recv,
    fg_send,
    fg_recv,
    pair_sems,
    own_sem,
    go_sem,
):
    me = lax.axis_index("tp")
    peer = 1 - me
    rep = lax.axis_index("rep")
    side = lax.rem(rep, 2)
    partner = rep + 1 - 2 * side
    lane = rep // 2
    n_lanes = n_rep // 2
    rows, width = x_ref.shape
    qw, kw = wq_hbm.shape[1], wk_hbm.shape[1]
    total = qw + 2 * kw
    cw = width // chunks
    piece_rows, piece_cols = own_mean_ref.shape
    col_blocks = width // piece_cols

    def along(j):
        return 2 * lax.rem(lane + j, n_lanes) + side

    barrier = pltpu.get_barrier_semaphore()
    pl.semaphore_signal(barrier, inc=1, device_id={"tp": peer}, device_id_type=MESH)
    pl.semaphore_signal(barrier, inc=1, device_id={"rep": partner}, device_id_type=MESH)

    @pl.when(side == 1)
    def _():
        def greet(j, _):
            pl.semaphore_signal(barrier, inc=1, device_id={"rep": along(j)}, device_id_type=MESH)
            return 0

        lax.fori_loop(1, n_lanes, greet, 0)

    first_copies = [
        pltpu.make_async_copy(tokens_hbm, x_ref, in_sems.at[0]),
        pltpu.make_async_copy(gain_hbm, gain_ref, in_sems.at[1]),
    ]
    late_copies = [
        pltpu.make_async_copy(cos_hbm, cos_ref, in_sems.at[2]),
        pltpu.make_async_copy(sin_hbm, sin_ref, in_sems.at[3]),
        pltpu.make_async_copy(go_hbm, go_ref, in_sems.at[4]),
    ]
    half_copy = pltpu.make_async_copy(local_hbm, mine_ref, own_sem)
    weight_copies = []
    for source, offset in ((wq_hbm, 0), (wk_hbm, qw), (wv_hbm, qw + kw)):
        for t in range(source.shape[1] // tile):
            weight_copies.append(
                pltpu.make_async_copy(
                    source.at[:, pl.ds(t * tile, tile)],
                    w_ref.at[:, pl.ds(offset + t * tile, tile)],
                    w_sems.at[len(weight_copies)],
                )
            )
    for copy in first_copies:
        copy.start()

    @pl.when(side == 1)
    def _():
        half_copy.start()


    def gather_copy(c):
        return pltpu.make_async_remote_copy(
            src_ref=tokens_hbm.at[:, ds(c, cw)],
            dst_ref=raw_ref.at[:, ds(c, cw)],
            send_sem=ag_send.at[c],
            recv_sem=ag_recv.at[c],
            device_id={"tp": peer},
            device_id_type=MESH,
        )

    norm_copy = pltpu.make_async_remote_copy(
        src_ref=inv_ref.at[0],
        dst_ref=inv_ref.at[1],
        send_sem=pair_sems.at[0],
        recv_sem=pair_sems.at[1],
        device_id={"tp": peer},
        device_id_type=MESH,
    )
    pair_copy = pltpu.make_async_remote_copy(
        src_ref=local_hbm,
        dst_ref=theirs_ref,
        send_sem=pair_sems.at[2],
        recv_sem=pair_sems.at[3],
        device_id={"rep": partner},
        device_id_type=MESH,
    )

    mean_copy = pltpu.make_async_remote_copy(
        src_ref=mean_ref,
        dst_ref=mean_ref,
        send_sem=pair_sems.at[4],
        recv_sem=pair_sems.at[5],
        device_id={"rep": partner},
        device_id_type=MESH,
    )

    def piece(owner):
        return (
            ds(owner // col_blocks, piece_rows),
            ds(lax.rem(owner, col_blocks), piece_cols),
        )

    def scatter_copy(j):
        return pltpu.make_async_remote_copy(
            src_ref=pair_ref.at[piece(lax.rem(lane + j, n_lanes))],
            dst_ref=pieces_ref.at[j],
            send_sem=fr_send.at[j],
            recv_sem=fr_recv.at[j],
            device_id={"rep": along(j)},
            device_id_type=MESH,
        )

    def spread_copy(j, owner):
        return pltpu.make_async_remote_copy(
            src_ref=own_mean_ref,
            dst_ref=mean_ref.at[piece(owner)],
            send_sem=fg_send.at[j],
            recv_sem=fg_recv.at[j],
            device_id={"rep": along(j)},
            device_id_type=MESH,
        )

    def start_all(make, low, high):
        def one(j, _):
            make(j).start()
            return 0

        lax.fori_loop(low, high, one, 0)

    def wait_recv_all(make, low, high):
        def one(j, _):
            make(j).wait_recv()
            return 0

        lax.fori_loop(low, high, one, 0)

    def wait_send_all(make, low, high):
        def one(j, _):
            make(j).wait_send()
            return 0

        lax.fori_loop(low, high, one, 0)

    early = chunks // 3
    pl.semaphore_wait(barrier, 2 + side * (n_lanes - 1))

    @pl.when(side == 0)
    def _():
        start_all(gather_copy, 0, early)
        pair_copy.start()

    for copy in first_copies:
        copy.wait()
    for copy in weight_copies + late_copies:
        copy.start()

    step = 16

    def norm_rows(i, _):
        x = x_ref[ds(i, step), :].astype(jnp.float32)
        inverse = lax.rsqrt(jnp.mean(x * x, axis=-1, keepdims=True) + epsilon)
        wide_ref[ds(i, step), :] = jnp.broadcast_to(inverse, (step, LANES))
        nm_ref[pl.ds(pl.multiple_of(me * rows + i * step, step), step), :] = (
            x * inverse * gain_ref[...]
        ).astype(jnp.bfloat16)
        return 0

    lax.fori_loop(0, rows // step, norm_rows, 0)
    inv_ref[0] = wide_ref[...].T[:SUBLANES]
    norm_copy.start()

    @pl.when(side == 0)
    def _():
        start_all(gather_copy, early, chunks)

    @pl.when(side == 1)
    def _():
        half_copy.wait()
        pair_copy.wait_recv()
        pair_ref[...] = (
            mine_ref[...].astype(jnp.float32) + theirs_ref[...].astype(jnp.float32)
        ).astype(jnp.bfloat16)
        start_all(scatter_copy, 1, n_lanes)

    heads_q, heads_kv = qw // HEAD_SIZE, kw // HEAD_SIZE
    for t, copy in enumerate(weight_copies):
        copy.wait()
        acc_ref[ds(me, rows), pl.ds(t * tile, tile)] = dot(
            nm_ref[ds(me, rows), :], w_ref[:, pl.ds(t * tile, tile)]
        )
    acc_ref[ds(peer, rows), :] = jnp.zeros((rows, total), jnp.float32)
    for copy in late_copies:
        copy.wait()

    def rope_rows(which):
        block = ds(which, rows)
        cosine, sine = cos_ref[block, :], sin_ref[block, :]

        def rope_head(source, target, index):
            vector = acc_ref[block, pl.ds(source * HEAD_SIZE, HEAD_SIZE)]
            target[block, pl.ds(index * HEAD_SIZE, HEAD_SIZE)] = (
                vector * cosine + pltpu.roll(vector, HEAD_SIZE // 2, 1) * sine
            ).astype(jnp.bfloat16)

        for h in range(heads_q):
            rope_head(h, q_ref, h)
        for h in range(heads_kv):
            rope_head(heads_q + h, k_ref, h)
        v_ref[block, :] = acc_ref[block, pl.ds(qw + kw, kw)].astype(jnp.bfloat16)

    rope_rows(me)

    def average_pieces():
        wait_recv_all(scatter_copy, 1, n_lanes)
        summed = pair_ref[piece(lane)].astype(jnp.float32)
        for j in range(1, n_lanes):
            summed = summed + pieces_ref[j].astype(jnp.float32)
        summed = (summed * (1.0 / n_rep)).astype(jnp.bfloat16)
        own_mean_ref[...] = summed
        mean_ref[piece(lane)] = summed
        start_all(lambda j: spread_copy(j, lane), 1, n_lanes)

    def pass_mean():
        wait_recv_all(
            lambda j: spread_copy(j, lax.rem(lane + n_lanes - j, n_lanes)), 1, n_lanes
        )
        mean_copy.start()

    @pl.when(side == 1)
    def _():
        average_pieces()
        pl.semaphore_wait(go_sem, 1)
        start_all(gather_copy, 0, chunks)

    norm_copy.wait_recv()
    wide_ref[...] = jnp.broadcast_to(inv_ref[1][:1], (LANES, rows)).T

    def arrived(c, _):
        gather_copy(c).wait_recv()

        @pl.when((side == 0) & (c == chunks - 4))
        def _():
            pl.semaphore_signal(go_sem, inc=1, device_id={"rep": partner}, device_id_type=MESH)

        @pl.when((side == 1) & (c == chunks - 5))
        def _():
            pass_mean()

        inverse = wide_ref[...]
        parts = []
        for part in range(cw // LANES):
            cols = pl.ds(pl.multiple_of(c * cw + part * LANES, LANES), LANES)
            parts.append(
                (raw_ref[:, cols].astype(jnp.float32) * inverse * gain_ref[:, cols]).astype(
                    jnp.bfloat16
                )
            )
        part = jnp.concatenate(parts, axis=1)
        nm_ref[ds(peer, rows), ds(c, cw)] = part
        acc_ref[ds(peer, rows), :] += dot(part, w_ref[ds(c, cw), :])
        return 0

    lax.fori_loop(0, chunks, arrived, 0)
    rope_rows(peer)

    group = heads_q // heads_kv
    scale = HEAD_SIZE ** (-0.5)
    key_pos = lax.broadcasted_iota(jnp.int32, (rows, rows), 0)
    query_pos = lax.broadcasted_iota(jnp.int32, (rows, rows), 1)
    bias = jnp.where(key_pos <= query_pos, 0.0, -jnp.inf).astype(jnp.float32)
    bias = jnp.concatenate([bias] * group, axis=1)

    def reverse(gradient, block):
        c = cos_ref[block * rows : (block + 1) * rows]
        s = sin_ref[block * rows : (block + 1) * rows]
        return (gradient * c - pltpu.roll(gradient, HEAD_SIZE // 2, 1) * s).astype(jnp.bfloat16)

    def kv_head(g, _):
        grad_k = [None, None]
        grad_v = [None, None]
        kv = ds(g, HEAD_SIZE)
        for b in range(2):
            keys = (b + 1) * rows
            block = pl.ds(b * rows, rows)
            heads = [ds(g * group + r, HEAD_SIZE) for r in range(group)]
            query = jnp.concatenate([q_ref[block, head] for head in heads], axis=0)
            out_grad = jnp.concatenate([go_ref[block, head] for head in heads], axis=0)
            key = k_ref[pl.ds(0, keys), kv]
            value = v_ref[pl.ds(0, keys), kv]
            scores = dot(key, query, NT)
            grad_prob = dot(value, out_grad, NT)
            if b == 0:
                scores = scores + bias
            else:
                scores = jnp.concatenate([scores[:rows], scores[rows:] + bias], axis=0)
            highest = jnp.max(scores, axis=0, keepdims=True)
            powers = jnp.exp2((scores - highest) * (scale * LOG2_E))
            prob = powers * (1.0 / jnp.sum(powers, axis=0, keepdims=True))
            inner = jnp.sum(grad_prob * prob, axis=0, keepdims=True)
            score_low = (prob * (grad_prob - inner) * scale).astype(jnp.bfloat16)
            grad_q = dot(score_low, key, TN)
            for r, head in enumerate(heads):
                d_ref[block, head] = reverse(grad_q[r * rows : (r + 1) * rows], b)
            part_v = dot(prob.astype(jnp.bfloat16), out_grad)
            part_k = dot(score_low, query)
            for j in range(b + 1):
                pv = part_v[j * rows : (j + 1) * rows]
                pk = part_k[j * rows : (j + 1) * rows]
                grad_v[j] = pv if grad_v[j] is None else grad_v[j] + pv
                grad_k[j] = pk if grad_k[j] is None else grad_k[j] + pk
        for j in range(2):
            block = pl.ds(j * rows, rows)
            d_ref[block, ds(heads_q + g, HEAD_SIZE)] = reverse(grad_k[j], j)
            d_ref[block, ds(heads_q + heads_kv + g, HEAD_SIZE)] = grad_v[j].astype(jnp.bfloat16)
        return 0

    lax.fori_loop(0, heads_kv, kv_head, 0, unroll=True)

    shares(d_ref, nm_ref, w_ref, gain_ref, far_ref, here_ref, gain_part_ref, 0, tile)

    norm_copy.wait_send()
    wait_send_all(gather_copy, 0, chunks)

    @pl.when(side == 0)
    def _():
        pair_copy.wait_send()
        mean_copy.wait_recv()

    @pl.when(side == 1)
    def _():
        wait_send_all(scatter_copy, 1, n_lanes)
        wait_send_all(lambda j: spread_copy(j, lane), 1, n_lanes)
        mean_copy.wait_send()


def second_kernel(
    tile, d_ref, nm_ref, w_ref, gain_ref, gain_a_ref, far_ref, here_ref, gain_part_ref
):
    rows, cols = here_ref.shape
    done = gain_a_ref.shape[1]
    gain_part_ref[:, pl.ds(0, done)] = gain_a_ref[...]
    shares(d_ref, nm_ref, w_ref, gain_ref, far_ref, here_ref, gain_part_ref, done, tile)
    lines = []
    for low in range(0, done + cols, cols):
        gain_part = gain_part_ref[:, pl.ds(low, cols)]
        for _ in range(3):
            lines.append(gain_part.astype(jnp.bfloat16).astype(jnp.float32))
            gain_part = gain_part - lines[-1]
    pad = far_ref.shape[0] - rows
    lines = jnp.concatenate(lines + [jnp.zeros((pad - len(lines), cols), jnp.float32)], axis=0)
    far_ref[pl.ds(rows, pad), :] = lines.astype(jnp.bfloat16)


def weights_kernel(nm_ref, d_ref, mean_ref, global_ref, momentum_ref, gq_ref, gk_ref, gv_ref, ng_ref, nmom_ref):
    i = pl.program_id(0)
    wide = gq_ref.shape[0]
    qw, kw = gq_ref.shape[1], gk_ref.shape[1]
    grad = dot(nm_ref[:, ds(i, wide)], d_ref[...], TN).astype(jnp.bfloat16)
    gq_ref[...] = grad[:, :qw]
    gk_ref[...] = grad[:, qw : qw + kw]
    gv_ref[...] = grad[:, qw + kw :]
    held = global_ref[...]
    mean_delta = held - mean_ref[:, ds(i, wide)].astype(jnp.float32)
    new_momentum = outer_momentum * momentum_ref[...] + mean_delta
    nmom_ref[...] = new_momentum
    ng_ref[...] = held - outer_rate * (mean_delta + outer_momentum * new_momentum)


def rows_kernel(
    x_ref, here_a_ref, here_b_ref, gain_ref, landed_a_ref, landed_b_ref, part_ref, out_ref, gain_out_ref
):
    i = pl.program_id(0)
    count = out_ref.shape[0]
    rows, _ = x_ref.shape

    @pl.when(i == 0)
    def _():
        lines = landed_b_ref[pl.ds(rows, landed_b_ref.shape[0] - rows), :].astype(jnp.float32)
        sums = [lines[k + 2 : k + 3] + lines[k + 1 : k + 2] + lines[k : k + 1] for k in (0, 3)]
        gain_out_ref[...] = part_ref[...] + jnp.concatenate(sums, axis=1)

    step = 16

    def some(j, _):
        block = pl.ds(pl.multiple_of(i * count + j * step, step), step)
        x = x_ref[block, :].astype(jnp.float32)
        inverse = lax.rsqrt(jnp.mean(x * x, axis=-1, keepdims=True) + epsilon)
        summed = [
            here[block, :].astype(jnp.float32) + landed[block, :].astype(jnp.float32)
            for here, landed in ((here_a_ref, landed_a_ref), (here_b_ref, landed_b_ref))
        ]
        scaled = jnp.concatenate(summed, axis=1) * gain_ref[...]
        pull = jnp.mean(scaled * x, axis=-1, keepdims=True) * (inverse * inverse)
        out_ref[ds(j, step), :] = (inverse * (scaled - x * pull)).astype(jnp.bfloat16)
        return 0

    lax.fori_loop(0, count // step, some, 0, unroll=True)


def pair_parts(
    n_rep,
    tokens,
    norm_gain,
    w_query,
    key_weight,
    value_weight,
    attention_gradient,
    global_fragment,
    momentum,
    local_fragment,
):
    rows, width = tokens.shape[1:]
    sequence = 2 * rows
    weight_q, weight_k, weight_v = w_query[0], key_weight[0], value_weight[0]
    qw, kw = weight_q.shape[1], weight_k.shape[1]
    total = qw + 2 * kw
    frag_rows = local_fragment.shape[1]
    piece_rows = 16
    n_lanes = n_rep // 2
    piece_cols = width * frag_rows // piece_rows // n_lanes
    chunks = 12
    tile = 512
    pad = 8
    first = width // 2
    bf16, f32 = jnp.bfloat16, jnp.float32
    cosine, sine = host_tables(sequence, HEAD_SIZE)
    vmem = pl.BlockSpec(memory_space=pltpu.VMEM)
    hbm = pl.BlockSpec(memory_space=pltpu.HBM)
    x, normed, d, here_a, far_a, gain_a, mean_local, weights = pl.pallas_call(
        functools.partial(front_kernel, n_rep, chunks, tile),
        out_shape=(
            pltpu.VMEM((rows, width), bf16),
            pltpu.VMEM((sequence, width), bf16),
            pltpu.VMEM((sequence, total), bf16),
            pltpu.VMEM((rows, first), bf16),
            pltpu.VMEM((rows, first), bf16),
            pltpu.VMEM((1, first), f32),
            pltpu.VMEM((frag_rows, width), bf16),
            pltpu.VMEM((width, total), bf16),
        ),
        in_specs=[hbm] * 9,
        out_specs=(vmem,) * 8,
        scratch_shapes=[
            pltpu.VMEM((1, width), f32),
            pltpu.VMEM((sequence, qw), bf16),
            pltpu.VMEM((sequence, HEAD_SIZE), f32),
            pltpu.VMEM((sequence, HEAD_SIZE), f32),
            pltpu.VMEM((sequence, total), f32),
            pltpu.VMEM((sequence, qw), bf16),
            pltpu.VMEM((sequence, kw), bf16),
            pltpu.VMEM((sequence, kw), bf16),
            pltpu.VMEM((rows, width), bf16),
            pltpu.VMEM((rows, LANES), f32),
            pltpu.VMEM((2, SUBLANES, rows), f32),
            pltpu.VMEM((frag_rows, width), bf16),
            pltpu.VMEM((frag_rows, width), bf16),
            pltpu.VMEM((frag_rows, width), bf16),
            pltpu.VMEM((n_lanes, piece_rows, piece_cols), bf16),
            pltpu.VMEM((piece_rows, piece_cols), bf16),
            pltpu.SemaphoreType.DMA((5,)),
            pltpu.SemaphoreType.DMA((total // tile,)),
            pltpu.SemaphoreType.DMA((chunks,)),
            pltpu.SemaphoreType.DMA((chunks,)),
            pltpu.SemaphoreType.DMA((n_lanes,)),
            pltpu.SemaphoreType.DMA((n_lanes,)),
            pltpu.SemaphoreType.DMA((n_lanes,)),
            pltpu.SemaphoreType.DMA((n_lanes,)),
            pltpu.SemaphoreType.DMA((6,)),
            pltpu.SemaphoreType.DMA,
            pltpu.SemaphoreType.REGULAR,
        ],
        compiler_params=pltpu.CompilerParams(
            collective_id=0, has_side_effects=True, vmem_limit_bytes=20 * 1024 * 1024
        ),
    )(
        *[
            pltpu.with_memory_space_constraint(array, pltpu.HBM)
            for array in (
                tokens[0],
                norm_gain,
                weight_q,
                weight_k,
                weight_v,
                attention_gradient[0],
                cosine,
                sine,
                local_fragment[0],
            )
        ]
    )
    swap = [(0, 1), (1, 0)]
    landed_a = lax.ppermute(far_a, "tp", swap)
    far_b, here_b, gain_partial = pl.pallas_call(
        functools.partial(second_kernel, tile),
        out_shape=(
            pltpu.VMEM((rows + pad, width - first), bf16),
            pltpu.VMEM((rows, width - first), bf16),
            pltpu.VMEM((1, width), f32),
        ),
        in_specs=[vmem] * 5,
        out_specs=(vmem,) * 3,
        compiler_params=pltpu.CompilerParams(vmem_limit_bytes=8 * 1024 * 1024),
        cost_estimate=pl.CostEstimate(
            flops=sequence * width * total, bytes_accessed=width * total, transcendentals=0
        ),
    )(d, normed, weights, norm_gain, gain_a)
    landed_b = lax.ppermute(far_b, "tp", swap)
    wide = 768
    columns = lambda size: pl.BlockSpec((size, wide), lambda i: (0, i))
    grad_wq, grad_wk, grad_wv, new_global, new_momentum = pl.pallas_call(
        weights_kernel,
        grid=(width // wide,),
        out_shape=(
            jax.ShapeDtypeStruct((width, qw), bf16),
            jax.ShapeDtypeStruct((width, kw), bf16),
            jax.ShapeDtypeStruct((width, kw), bf16),
            jax.ShapeDtypeStruct((frag_rows, width), f32),
            jax.ShapeDtypeStruct((frag_rows, width), f32),
        ),
        in_specs=[vmem, vmem, vmem, columns(frag_rows), columns(frag_rows)],
        out_specs=(
            pl.BlockSpec((wide, qw), lambda i: (i, 0)),
            pl.BlockSpec((wide, kw), lambda i: (i, 0)),
            pl.BlockSpec((wide, kw), lambda i: (i, 0)),
            columns(frag_rows),
            columns(frag_rows),
        ),
        compiler_params=pltpu.CompilerParams(vmem_limit_bytes=28 * 1024 * 1024),
        cost_estimate=pl.CostEstimate(
            flops=2 * sequence * width * total, bytes_accessed=3 * width * total, transcendentals=0
        ),
    )(normed, d, mean_local, global_fragment, momentum)
    count = 64
    block = pl.BlockSpec((count, width), lambda i: (i, 0))
    gradient_rows, gains_gradient = pl.pallas_call(
        rows_kernel,
        grid=(rows // count,),
        out_shape=(
            jax.ShapeDtypeStruct((rows, width), bf16),
            jax.ShapeDtypeStruct((1, width), f32),
        ),
        in_specs=[vmem] * 7,
        out_specs=(block, pl.BlockSpec((1, width), lambda i: (0, 0))),
        compiler_params=pltpu.CompilerParams(vmem_limit_bytes=8 * 1024 * 1024),
        cost_estimate=pl.CostEstimate(
            flops=12 * rows * width, bytes_accessed=4 * rows * width, transcendentals=0
        ),
    )(x, here_a, here_b, norm_gain, landed_a, landed_b, gain_partial)
    return (
        grad_wq[None],
        grad_wk[None],
        grad_wv[None],
        gains_gradient,
        gradient_rows[None],
        new_global,
        new_momentum,
    )


def solution(mesh):
    placed = (
        P("rep", "tp", None),
        P("rep", None),
        P("rep", None, "tp"),
        P("rep", None, "tp"),
        P("rep", None, "tp"),
        P("rep", None, "tp"),
        P("tp", None),
        P("tp", None),
        P("rep", "tp", None),
    )
    paired = mesh.shape["tp"] == 2 and mesh.shape["rep"] % 2 == 0
    chosen = functools.partial(pair_parts, mesh.shape["rep"]) if paired else body
    return jax.shard_map(
        chosen,
        mesh=mesh,
        in_specs=placed,
        out_specs=(
            P("rep", None, "tp"),
            P("rep", None, "tp"),
            P("rep", None, "tp"),
            P("rep", None),
            P("rep", "tp", None),
            P("tp", None),
            P("tp", None),
        ),
        check_vma=False,
    )
```

```python
import functools

import jax
import jax.numpy as jnp
import numpy as np
from jax import lax
from jax.experimental import pallas as pl
from jax.experimental.pallas import tpu as pltpu
from jax.sharding import PartitionSpec as P


MESH = pl.DeviceIdType.MESH

HEAD_SIZE = 128


epsilon = 1e-05
rope_base = 500000.0
outer_rate = 0.7
outer_momentum = 0.9
LOG2_E = 1.4426950408889634
LANES = 128
SUBLANES = 8


def rope_tables(sequence_length, width):
    middle = width // 2
    frequency = rope_base ** (-2.0 * jnp.arange(middle, dtype=jnp.float32) / width)
    angles = jnp.arange(sequence_length, dtype=jnp.float32)[:, None] * frequency[None, :]
    angles = jnp.concatenate([angles, angles], axis=1)
    return (jnp.cos(angles)[:, None, :], jnp.sin(angles)[:, None, :])


def rotate(vectors, cosine_table, sine_table):
    middle = vectors.shape[-1] // 2
    turned = jnp.concatenate([-vectors[..., middle:], vectors[..., :middle]], axis=-1)
    return vectors * cosine_table + turned * sine_table


def reverse_rotation(gradient, cosine_table, sine_table):
    middle = gradient.shape[-1] // 2
    shifted = gradient * sine_table
    turned = jnp.concatenate([shifted[..., middle:], -shifted[..., :middle]], axis=-1)
    return gradient * cosine_table + turned


def attention_reverse(query_rows, rotated_keys, values_bfloat, grad_out, block_of_rows):
    sequence_length = query_rows.shape[0]
    score_scale = query_rows.shape[-1] ** (-0.5)

    def one_block(running, block_index):
        acc_key, acc_value = running
        offset = block_index * block_of_rows
        query_block = lax.dynamic_slice_in_dim(query_rows, offset, block_of_rows, 0)
        grad_block = lax.dynamic_slice_in_dim(grad_out, offset, block_of_rows, 0)
        scores = (
            jnp.einsum(
                "qgrd,kgd->grqk", query_block, rotated_keys, preferred_element_type=jnp.float32
            )
            * score_scale
        )
        row_pos = offset + jnp.arange(block_of_rows)
        col_pos = jnp.arange(sequence_length)
        allowed = col_pos[None, :] <= row_pos[:, None]
        scores = jnp.where(allowed, scores, -jnp.inf)
        highest = jnp.max(scores, axis=-1, keepdims=True)
        powers = jnp.exp(scores - highest)
        probability = powers / jnp.sum(powers, axis=-1, keepdims=True)
        prob_low = probability.astype(jnp.bfloat16)
        acc_value = acc_value + jnp.einsum(
            "grqk,qgrd->kgd", prob_low, grad_block, preferred_element_type=jnp.float32
        )
        grad_prob = jnp.einsum(
            "qgrd,kgd->grqk", grad_block, values_bfloat, preferred_element_type=jnp.float32
        )
        grad_score = (
            probability
            * (grad_prob - jnp.sum(grad_prob * probability, axis=-1, keepdims=True))
            * score_scale
        )
        score_low = grad_score.astype(jnp.bfloat16)
        grad_query = jnp.einsum(
            "grqk,kgd->qgrd", score_low, rotated_keys, preferred_element_type=jnp.float32
        )
        acc_key = acc_key + jnp.einsum(
            "grqk,qgrd->kgd", score_low, query_block, preferred_element_type=jnp.float32
        )
        return ((acc_key, acc_value), grad_query)

    initial = jnp.zeros(rotated_keys.shape, jnp.float32)
    (acc_key, acc_value), grad_blocks = lax.scan(
        one_block, (initial, initial), jnp.arange(sequence_length // block_of_rows)
    )
    return (grad_blocks.reshape(query_rows.shape), acc_key, acc_value)


def body(
    tokens,
    norm_gain,
    w_query,
    key_weight,
    value_weight,
    attention_gradient,
    global_fragment,
    momentum,
    local_fragment,
):
    local_rows = tokens[0]
    norm_gains = norm_gain[0]
    weight_q = w_query[0]
    weight_k = key_weight[0]
    weight_v = value_weight[0]
    widened_rows = local_rows.astype(jnp.float32)
    inverse_norm = lax.rsqrt(
        jnp.mean(widened_rows * widened_rows, axis=-1, keepdims=True) + epsilon
    )
    normalized_input = widened_rows * inverse_norm
    normalized_local = (normalized_input * norm_gains[None, :]).astype(jnp.bfloat16)
    normalized = lax.all_gather(normalized_local, "tp", axis=0, tiled=True)
    sequence_length = normalized.shape[0]
    heads_q = weight_q.shape[1] // HEAD_SIZE
    heads_kv = weight_k.shape[1] // HEAD_SIZE
    cosine_table, sine_table = rope_tables(sequence_length, HEAD_SIZE)
    query_rows = jnp.dot(normalized, weight_q, preferred_element_type=jnp.float32).reshape(
        sequence_length, heads_q, HEAD_SIZE
    )
    query_rows = rotate(query_rows, cosine_table, sine_table).astype(jnp.bfloat16)
    rotated_keys = jnp.dot(normalized, weight_k, preferred_element_type=jnp.float32).reshape(
        sequence_length, heads_kv, HEAD_SIZE
    )
    rotated_keys = rotate(rotated_keys, cosine_table, sine_table).astype(jnp.bfloat16)
    values_bfloat = (
        jnp.dot(normalized, weight_v, preferred_element_type=jnp.float32)
        .astype(jnp.bfloat16)
        .reshape(sequence_length, heads_kv, HEAD_SIZE)
    )
    replica_group = heads_q // heads_kv
    block_of_rows = min(512, sequence_length)
    query_input_gradient, key_input_gradient, value_input_gradient = attention_reverse(
        query_rows.reshape(sequence_length, heads_kv, replica_group, HEAD_SIZE),
        rotated_keys,
        values_bfloat,
        attention_gradient[0].reshape(sequence_length, heads_kv, replica_group, HEAD_SIZE),
        block_of_rows,
    )
    dquery = (
        reverse_rotation(
            query_input_gradient.reshape(sequence_length, heads_q, HEAD_SIZE),
            cosine_table,
            sine_table,
        )
        .astype(jnp.bfloat16)
        .reshape(sequence_length, heads_q * HEAD_SIZE)
    )
    key_gradient = (
        reverse_rotation(key_input_gradient, cosine_table, sine_table)
        .astype(jnp.bfloat16)
        .reshape(sequence_length, heads_kv * HEAD_SIZE)
    )
    value_gradient = value_input_gradient.astype(jnp.bfloat16).reshape(
        sequence_length, heads_kv * HEAD_SIZE
    )
    contract = (((0,), (0,)), ((), ()))
    grad_wq = lax.dot_general(
        normalized, dquery, contract, preferred_element_type=jnp.float32
    ).astype(jnp.bfloat16)
    grad_wk = lax.dot_general(
        normalized, key_gradient, contract, preferred_element_type=jnp.float32
    ).astype(jnp.bfloat16)
    grad_wv = lax.dot_general(
        normalized, value_gradient, contract, preferred_element_type=jnp.float32
    ).astype(jnp.bfloat16)
    back = (((1,), (1,)), ((), ()))
    partial_value = lax.dot_general(dquery, weight_q, back, preferred_element_type=jnp.float32)
    partial_value = partial_value + lax.dot_general(
        key_gradient, weight_k, back, preferred_element_type=jnp.float32
    )
    summed_rows = lax.psum_scatter(
        (
            partial_value
            + lax.dot_general(value_gradient, weight_v, back, preferred_element_type=jnp.float32)
        ).astype(jnp.bfloat16),
        "tp",
        scatter_dimension=0,
        tiled=True,
    ).astype(jnp.float32)
    gains_gradient = lax.psum(jnp.sum(summed_rows * normalized_input, axis=0), "tp")
    scaled_rows = summed_rows * norm_gains[None, :]
    gradient_rows = (
        inverse_norm
        * (
            scaled_rows
            - normalized_input * jnp.mean(scaled_rows * normalized_input, axis=-1, keepdims=True)
        )
    ).astype(jnp.bfloat16)
    delta = global_fragment - local_fragment[0].astype(jnp.float32)
    replicas = lax.axis_size("rep")
    mean_delta = lax.psum(delta, "rep") / replicas
    new_momentum = outer_momentum * momentum + mean_delta
    new_global = global_fragment - outer_rate * (mean_delta + outer_momentum * new_momentum)
    return (
        grad_wq[None],
        grad_wk[None],
        grad_wv[None],
        gains_gradient[None],
        gradient_rows[None],
        new_global,
        new_momentum,
    )


NT = (((1,), (1,)), ((), ()))
TN = (((0,), (0,)), ((), ()))


def dot(a, b, dims=(((1,), (0,)), ((), ()))):
    return lax.dot_general(a, b, dims, preferred_element_type=jnp.float32)


def ds(index, size):
    return pl.ds(pl.multiple_of(index * size, size), size)


def host_tables(sequence_length, width):
    middle = width // 2
    frequency = rope_base ** (-2.0 * np.arange(middle) / width)
    angles = np.arange(sequence_length)[:, None] * frequency[None, :]
    cosine, sine = np.cos(angles), np.sin(angles)
    return (
        jnp.asarray(np.concatenate([cosine, cosine], axis=1), jnp.float32),
        jnp.asarray(np.concatenate([-sine, sine], axis=1), jnp.float32),
    )


def shares(d_ref, nm_ref, w_ref, gain_ref, far_ref, here_ref, gain_part_ref, low, tile):
    me = lax.axis_index("tp")
    peer = 1 - me
    rows = here_ref.shape[0]
    offset = gain_part_ref.shape[1] - here_ref.shape[1] if low else 0

    def back(t, _):
        both = jnp.concatenate([d_ref[ds(peer, rows), :], d_ref[ds(me, rows), :]], axis=0)
        cols = pl.ds(pl.multiple_of(low + t * tile, tile), tile)
        own = ds(t, tile)
        part = dot(both, w_ref[cols, :], NT).astype(jnp.bfloat16)
        far_ref[pl.ds(0, rows), own] = part[:rows]
        here_ref[:, own] = part[rows:]
        wide = part.astype(jnp.float32)
        products = wide[:rows] * nm_ref[ds(peer, rows), cols].astype(jnp.float32)
        products += wide[rows:] * nm_ref[ds(me, rows), cols].astype(jnp.float32)
        gain_part = jnp.sum(products, axis=0, keepdims=True) / gain_ref[:, cols]
        gain_part_ref[:, pl.ds(pl.multiple_of(offset + t * tile, tile), tile)] = gain_part
        return 0

    lax.fori_loop(0, here_ref.shape[1] // tile, back, 0, unroll=True)


def front_kernel(
    n_rep,
    chunks,
    tile,
    tokens_hbm,
    gain_hbm,
    wq_hbm,
    wk_hbm,
    wv_hbm,
    go_hbm,
    cos_hbm,
    sin_hbm,
    local_hbm,
    x_ref,
    nm_ref,
    d_ref,
    here_ref,
    far_ref,
    gain_part_ref,
    mean_ref,
    w_ref,
    gain_ref,
    go_ref,
    cos_ref,
    sin_ref,
    acc_ref,
    q_ref,
    k_ref,
    v_ref,
    raw_ref,
    wide_ref,
    inv_ref,
    mine_ref,
    theirs_ref,
    pair_ref,
    pieces_ref,
    own_mean_ref,
    in_sems,
    w_sems,
    ag_send,
    ag_recv,
    fr_send,
    fr_recv,
    fg_send,
    fg_recv,
    pair_sems,
    own_sem,
    go_sem,
):
    me = lax.axis_index("tp")
    peer = 1 - me
    rep = lax.axis_index("rep")
    side = lax.rem(rep, 2)
    partner = rep + 1 - 2 * side
    lane = rep // 2
    n_lanes = n_rep // 2
    rows, width = x_ref.shape
    qw, kw = wq_hbm.shape[1], wk_hbm.shape[1]
    total = qw + 2 * kw
    cw = width // chunks
    piece_rows, piece_cols = own_mean_ref.shape
    col_blocks = width // piece_cols

    def along(j):
        return 2 * lax.rem(lane + j, n_lanes) + side

    barrier = pltpu.get_barrier_semaphore()
    pl.semaphore_signal(barrier, inc=1, device_id={"tp": peer}, device_id_type=MESH)
    pl.semaphore_signal(barrier, inc=1, device_id={"rep": partner}, device_id_type=MESH)

    @pl.when(side == 1)
    def _():
        def greet(j, _):
            pl.semaphore_signal(barrier, inc=1, device_id={"rep": along(j)}, device_id_type=MESH)
            return 0

        lax.fori_loop(1, n_lanes, greet, 0)

    first_copies = [
        pltpu.make_async_copy(tokens_hbm, x_ref, in_sems.at[0]),
        pltpu.make_async_copy(gain_hbm, gain_ref, in_sems.at[1]),
    ]
    late_copies = [
        pltpu.make_async_copy(cos_hbm, cos_ref, in_sems.at[2]),
        pltpu.make_async_copy(sin_hbm, sin_ref, in_sems.at[3]),
        pltpu.make_async_copy(go_hbm, go_ref, in_sems.at[4]),
    ]
    half_copy = pltpu.make_async_copy(local_hbm, mine_ref, own_sem)
    weight_copies = []
    for source, offset in ((wq_hbm, 0), (wk_hbm, qw), (wv_hbm, qw + kw)):
        for t in range(source.shape[1] // tile):
            weight_copies.append(
                pltpu.make_async_copy(
                    source.at[:, pl.ds(t * tile, tile)],
                    w_ref.at[:, pl.ds(offset + t * tile, tile)],
                    w_sems.at[len(weight_copies)],
                )
            )
    for copy in first_copies:
        copy.start()

    @pl.when(side == 1)
    def _():
        half_copy.start()


    def gather_copy(c, source=x_ref):
        return pltpu.make_async_remote_copy(
            src_ref=source.at[:, ds(c, cw)],
            dst_ref=raw_ref.at[:, ds(c, cw)],
            send_sem=ag_send.at[c],
            recv_sem=ag_recv.at[c],
            device_id={"tp": peer},
            device_id_type=MESH,
        )

    norm_copy = pltpu.make_async_remote_copy(
        src_ref=inv_ref.at[0],
        dst_ref=inv_ref.at[1],
        send_sem=pair_sems.at[0],
        recv_sem=pair_sems.at[1],
        device_id={"tp": peer},
        device_id_type=MESH,
    )
    pair_copy = pltpu.make_async_remote_copy(
        src_ref=local_hbm,
        dst_ref=theirs_ref,
        send_sem=pair_sems.at[2],
        recv_sem=pair_sems.at[3],
        device_id={"rep": partner},
        device_id_type=MESH,
    )

    mean_copy = pltpu.make_async_remote_copy(
        src_ref=mean_ref,
        dst_ref=mean_ref,
        send_sem=pair_sems.at[4],
        recv_sem=pair_sems.at[5],
        device_id={"rep": partner},
        device_id_type=MESH,
    )

    def piece(owner):
        return (
            ds(owner // col_blocks, piece_rows),
            ds(lax.rem(owner, col_blocks), piece_cols),
        )

    def scatter_copy(j):
        return pltpu.make_async_remote_copy(
            src_ref=pair_ref.at[piece(lax.rem(lane + j, n_lanes))],
            dst_ref=pieces_ref.at[j],
            send_sem=fr_send.at[j],
            recv_sem=fr_recv.at[j],
            device_id={"rep": along(j)},
            device_id_type=MESH,
        )

    def spread_copy(j, owner):
        return pltpu.make_async_remote_copy(
            src_ref=own_mean_ref,
            dst_ref=mean_ref.at[piece(owner)],
            send_sem=fg_send.at[j],
            recv_sem=fg_recv.at[j],
            device_id={"rep": along(j)},
            device_id_type=MESH,
        )

    def start_all(make, low, high):
        def one(j, _):
            make(j).start()
            return 0

        lax.fori_loop(low, high, one, 0)

    def wait_recv_all(make, low, high):
        def one(j, _):
            make(j).wait_recv()
            return 0

        lax.fori_loop(low, high, one, 0)

    def wait_send_all(make, low, high):
        def one(j, _):
            make(j).wait_send()
            return 0

        lax.fori_loop(low, high, one, 0)

    early = chunks // 3

    @pl.when(side == 0)
    def _():
        pl.semaphore_wait(barrier, 2)
        start_all(lambda c: gather_copy(c, tokens_hbm), 0, early)
        pair_copy.start()

    for copy in first_copies:
        copy.wait()

    for copy in weight_copies + late_copies:
        copy.start()

    step = 16

    def norm_rows(i, _):
        x = x_ref[ds(i, step), :].astype(jnp.float32)
        inverse = lax.rsqrt(jnp.mean(x * x, axis=-1, keepdims=True) + epsilon)
        wide_ref[ds(i, step), :] = jnp.broadcast_to(inverse, (step, LANES))
        nm_ref[pl.ds(pl.multiple_of(me * rows + i * step, step), step), :] = (
            x * inverse * gain_ref[...]
        ).astype(jnp.bfloat16)
        return 0

    lax.fori_loop(0, rows // step, norm_rows, 0, unroll=2)
    inv_ref[0] = wide_ref[...].T[:SUBLANES]

    @pl.when(side == 1)
    def _():
        pl.semaphore_wait(barrier, n_lanes + 1)

    norm_copy.start()

    @pl.when(side == 0)
    def _():
        start_all(gather_copy, early, chunks)

    @pl.when(side == 1)
    def _():
        half_copy.wait()
        pair_copy.wait_recv()
        pair_ref[...] = (
            mine_ref[...].astype(jnp.float32) + theirs_ref[...].astype(jnp.float32)
        ).astype(jnp.bfloat16)
        start_all(scatter_copy, 1, n_lanes)

    heads_q, heads_kv = qw // HEAD_SIZE, kw // HEAD_SIZE
    for t, copy in enumerate(weight_copies):
        copy.wait()
        acc_ref[ds(me, rows), pl.ds(t * tile, tile)] = dot(
            nm_ref[ds(me, rows), :], w_ref[:, pl.ds(t * tile, tile)]
        )
    acc_ref[ds(peer, rows), :] = jnp.zeros((rows, total), jnp.float32)
    for copy in late_copies:
        copy.wait()

    def rope_rows(which):
        block = ds(which, rows)
        cosine, sine = cos_ref[block, :], sin_ref[block, :]

        def rope_head(source, target, index):
            vector = acc_ref[block, pl.ds(source * HEAD_SIZE, HEAD_SIZE)]
            target[block, pl.ds(index * HEAD_SIZE, HEAD_SIZE)] = (
                vector * cosine + pltpu.roll(vector, HEAD_SIZE // 2, 1) * sine
            ).astype(jnp.bfloat16)

        for h in range(heads_q):
            rope_head(h, q_ref, h)
        for h in range(heads_kv):
            rope_head(heads_q + h, k_ref, h)
        v_ref[block, :] = acc_ref[block, pl.ds(qw + kw, kw)].astype(jnp.bfloat16)

    rope_rows(me)

    def average_pieces():
        wait_recv_all(scatter_copy, 1, n_lanes)
        summed = pair_ref[piece(lane)].astype(jnp.float32)
        for j in range(1, n_lanes):
            summed = summed + pieces_ref[j].astype(jnp.float32)
        summed = (summed * (1.0 / n_rep)).astype(jnp.bfloat16)
        own_mean_ref[...] = summed
        mean_ref[piece(lane)] = summed
        start_all(lambda j: spread_copy(j, lane), 1, n_lanes)

    def pass_mean():
        wait_recv_all(
            lambda j: spread_copy(j, lax.rem(lane + n_lanes - j, n_lanes)), 1, n_lanes
        )
        mean_copy.start()

    @pl.when(side == 1)
    def _():
        average_pieces()
        pl.semaphore_wait(go_sem, 1)
        start_all(gather_copy, 0, chunks)

    norm_copy.wait_recv()
    wide_ref[...] = jnp.broadcast_to(inv_ref[1][:1], (LANES, rows)).T

    def arrived(c, _):
        gather_copy(c).wait_recv()

        @pl.when((side == 0) & (c == chunks - 5))
        def _():
            pl.semaphore_signal(go_sem, inc=1, device_id={"rep": partner}, device_id_type=MESH)

        @pl.when((side == 1) & (c == chunks - 8))
        def _():
            pass_mean()

        inverse = wide_ref[...]
        parts = []
        for part in range(cw // LANES):
            cols = pl.ds(pl.multiple_of(c * cw + part * LANES, LANES), LANES)
            parts.append(
                (raw_ref[:, cols].astype(jnp.float32) * inverse * gain_ref[:, cols]).astype(
                    jnp.bfloat16
                )
            )
        part = jnp.concatenate(parts, axis=1)
        nm_ref[ds(peer, rows), ds(c, cw)] = part
        acc_ref[ds(peer, rows), :] += dot(part, w_ref[ds(c, cw), :])
        return 0

    lax.fori_loop(0, chunks, arrived, 0)
    rope_rows(peer)

    group = heads_q // heads_kv
    scale = HEAD_SIZE ** (-0.5)
    key_pos = lax.broadcasted_iota(jnp.int32, (rows, rows), 0)
    query_pos = lax.broadcasted_iota(jnp.int32, (rows, rows), 1)
    bias = jnp.where(key_pos <= query_pos, 0.0, -jnp.inf).astype(jnp.float32)
    bias = jnp.concatenate([bias] * group, axis=1)

    def reverse(gradient, block):
        c = cos_ref[block * rows : (block + 1) * rows]
        s = sin_ref[block * rows : (block + 1) * rows]
        return (gradient * c - pltpu.roll(gradient, HEAD_SIZE // 2, 1) * s).astype(jnp.bfloat16)

    def kv_heads(low):
        members = range(low, low + 4)
        grads = {}
        for b in range(2):
            keys = (b + 1) * rows
            block = pl.ds(b * rows, rows)
            loaded, dots, soft = {}, {}, {}
            for g in members:
                heads = [pl.ds((g * group + r) * HEAD_SIZE, HEAD_SIZE) for r in range(group)]
                kv = pl.ds(g * HEAD_SIZE, HEAD_SIZE)
                query = jnp.concatenate([q_ref[block, head] for head in heads], axis=0)
                out_grad = jnp.concatenate([go_ref[block, head] for head in heads], axis=0)
                key = k_ref[pl.ds(0, keys), kv]
                value = v_ref[pl.ds(0, keys), kv]
                loaded[g] = heads, query, out_grad, key
                dots[g] = dot(key, query, NT), dot(value, out_grad, NT)
            for g in members:
                scores, grad_prob = dots[g]
                if b == 0:
                    scores = scores + bias
                else:
                    scores = jnp.concatenate([scores[:rows], scores[rows:] + bias], axis=0)
                highest = jnp.max(scores, axis=0, keepdims=True)
                powers = jnp.exp2((scores - highest) * (scale * LOG2_E))
                prob = powers * (1.0 / jnp.sum(powers, axis=0, keepdims=True))
                inner = jnp.sum(grad_prob * prob, axis=0, keepdims=True)
                score_low = (prob * (grad_prob - inner) * scale).astype(jnp.bfloat16)
                soft[g] = prob.astype(jnp.bfloat16), score_low
            for g in members:
                heads, query, out_grad, key = loaded[g]
                prob_low, score_low = soft[g]
                part_v = dot(prob_low, out_grad)
                part_k = dot(score_low, query)
                grad_q = dot(score_low, key, TN)
                for r, head in enumerate(heads):
                    d_ref[block, head] = reverse(grad_q[r * rows : (r + 1) * rows], b)
                for j in range(b + 1):
                    pv = part_v[j * rows : (j + 1) * rows]
                    pk = part_k[j * rows : (j + 1) * rows]
                    if (g, j) in grads:
                        pv, pk = pv + grads[g, j][0], pk + grads[g, j][1]
                    grads[g, j] = pv, pk
        for g in members:
            for j in range(2):
                block = pl.ds(j * rows, rows)
                low_k = (heads_q + g) * HEAD_SIZE
                d_ref[block, pl.ds(low_k, HEAD_SIZE)] = reverse(grads[g, j][1], j)
                low_v = (heads_q + heads_kv + g) * HEAD_SIZE
                d_ref[block, pl.ds(low_v, HEAD_SIZE)] = grads[g, j][0].astype(jnp.bfloat16)

    for low in range(0, heads_kv, 4):
        kv_heads(low)

    shares(d_ref, nm_ref, w_ref, gain_ref, far_ref, here_ref, gain_part_ref, 0, tile)

    norm_copy.wait_send()
    wait_send_all(gather_copy, 0, chunks)

    @pl.when(side == 0)
    def _():
        pair_copy.wait_send()
        mean_copy.wait_recv()

    @pl.when(side == 1)
    def _():
        wait_send_all(scatter_copy, 1, n_lanes)
        wait_send_all(lambda j: spread_copy(j, lane), 1, n_lanes)
        mean_copy.wait_send()


def second_kernel(
    tile, d_ref, nm_ref, w_ref, gain_ref, gain_a_ref, far_ref, here_ref, gain_part_ref
):
    rows, cols = here_ref.shape
    done = gain_a_ref.shape[1]
    gain_part_ref[:, pl.ds(0, done)] = gain_a_ref[...]
    shares(d_ref, nm_ref, w_ref, gain_ref, far_ref, here_ref, gain_part_ref, done, tile)
    lines = []
    for low in range(0, done + cols, cols):
        gain_part = gain_part_ref[:, pl.ds(low, cols)]
        for _ in range(3):
            lines.append(gain_part.astype(jnp.bfloat16).astype(jnp.float32))
            gain_part = gain_part - lines[-1]
    pad = far_ref.shape[0] - rows
    lines = jnp.concatenate(lines + [jnp.zeros((pad - len(lines), cols), jnp.float32)], axis=0)
    far_ref[pl.ds(rows, pad), :] = lines.astype(jnp.bfloat16)


def weights_kernel(nm_ref, d_ref, mean_ref, global_ref, momentum_ref, gq_ref, gk_ref, gv_ref, ng_ref, nmom_ref):
    i = pl.program_id(0)
    wide = gq_ref.shape[0]
    qw, kw = gq_ref.shape[1], gk_ref.shape[1]
    grad = dot(nm_ref[:, ds(i, wide)], d_ref[...], TN).astype(jnp.bfloat16)
    gq_ref[...] = grad[:, :qw]
    gk_ref[...] = grad[:, qw : qw + kw]
    gv_ref[...] = grad[:, qw + kw :]
    held = global_ref[...]
    mean_delta = held - mean_ref[:, ds(i, wide)].astype(jnp.float32)
    new_momentum = outer_momentum * momentum_ref[...] + mean_delta
    nmom_ref[...] = new_momentum
    ng_ref[...] = held - outer_rate * (mean_delta + outer_momentum * new_momentum)


def rows_kernel(
    x_ref, here_a_ref, here_b_ref, gain_ref, landed_a_ref, landed_b_ref, part_ref, out_ref, gain_out_ref
):
    i = pl.program_id(0)
    count = out_ref.shape[0]
    rows, _ = x_ref.shape

    @pl.when(i == 0)
    def _():
        lines = landed_b_ref[pl.ds(rows, landed_b_ref.shape[0] - rows), :].astype(jnp.float32)
        sums = [lines[k + 2 : k + 3] + lines[k + 1 : k + 2] + lines[k : k + 1] for k in (0, 3)]
        gain_out_ref[...] = part_ref[...] + jnp.concatenate(sums, axis=1)

    step = 16

    def some(j, _):
        block = pl.ds(pl.multiple_of(i * count + j * step, step), step)
        x = x_ref[block, :].astype(jnp.float32)
        inverse = lax.rsqrt(jnp.mean(x * x, axis=-1, keepdims=True) + epsilon)
        summed = [
            here[block, :].astype(jnp.float32) + landed[block, :].astype(jnp.float32)
            for here, landed in ((here_a_ref, landed_a_ref), (here_b_ref, landed_b_ref))
        ]
        scaled = jnp.concatenate(summed, axis=1) * gain_ref[...]
        pull = jnp.mean(scaled * x, axis=-1, keepdims=True) * (inverse * inverse)
        out_ref[ds(j, step), :] = (inverse * (scaled - x * pull)).astype(jnp.bfloat16)
        return 0

    lax.fori_loop(0, count // step, some, 0, unroll=True)


def pair_parts(
    n_rep,
    tokens,
    norm_gain,
    w_query,
    key_weight,
    value_weight,
    attention_gradient,
    global_fragment,
    momentum,
    local_fragment,
):
    rows, width = tokens.shape[1:]
    sequence = 2 * rows
    weight_q, weight_k, weight_v = w_query[0], key_weight[0], value_weight[0]
    qw, kw = weight_q.shape[1], weight_k.shape[1]
    total = qw + 2 * kw
    frag_rows = local_fragment.shape[1]
    piece_rows = 16
    n_lanes = n_rep // 2
    piece_cols = width * frag_rows // piece_rows // n_lanes
    chunks = 12
    tile = 512
    pad = 8
    first = width // 2
    bf16, f32 = jnp.bfloat16, jnp.float32
    cosine, sine = host_tables(sequence, HEAD_SIZE)
    vmem = pl.BlockSpec(memory_space=pltpu.VMEM)
    hbm = pl.BlockSpec(memory_space=pltpu.HBM)
    x, normed, d, here_a, far_a, gain_a, mean_local, weights = pl.pallas_call(
        functools.partial(front_kernel, n_rep, chunks, tile),
        out_shape=(
            pltpu.VMEM((rows, width), bf16),
            pltpu.VMEM((sequence, width), bf16),
            pltpu.VMEM((sequence, total), bf16),
            pltpu.VMEM((rows, first), bf16),
            pltpu.VMEM((rows, first), bf16),
            pltpu.VMEM((1, first), f32),
            pltpu.VMEM((frag_rows, width), bf16),
            pltpu.VMEM((width, total), bf16),
        ),
        in_specs=[hbm] * 9,
        out_specs=(vmem,) * 8,
        scratch_shapes=[
            pltpu.VMEM((1, width), f32),
            pltpu.VMEM((sequence, qw), bf16),
            pltpu.VMEM((sequence, HEAD_SIZE), f32),
            pltpu.VMEM((sequence, HEAD_SIZE), f32),
            pltpu.VMEM((sequence, total), f32),
            pltpu.VMEM((sequence, qw), bf16),
            pltpu.VMEM((sequence, kw), bf16),
            pltpu.VMEM((sequence, kw), bf16),
            pltpu.VMEM((rows, width), bf16),
            pltpu.VMEM((rows, LANES), f32),
            pltpu.VMEM((2, SUBLANES, rows), f32),
            pltpu.VMEM((frag_rows, width), bf16),
            pltpu.VMEM((frag_rows, width), bf16),
            pltpu.VMEM((frag_rows, width), bf16),
            pltpu.VMEM((n_lanes, piece_rows, piece_cols), bf16),
            pltpu.VMEM((piece_rows, piece_cols), bf16),
            pltpu.SemaphoreType.DMA((5,)),
            pltpu.SemaphoreType.DMA((total // tile,)),
            pltpu.SemaphoreType.DMA((chunks,)),
            pltpu.SemaphoreType.DMA((chunks,)),
            pltpu.SemaphoreType.DMA((n_lanes,)),
            pltpu.SemaphoreType.DMA((n_lanes,)),
            pltpu.SemaphoreType.DMA((n_lanes,)),
            pltpu.SemaphoreType.DMA((n_lanes,)),
            pltpu.SemaphoreType.DMA((6,)),
            pltpu.SemaphoreType.DMA,
            pltpu.SemaphoreType.REGULAR,
        ],
        compiler_params=pltpu.CompilerParams(
            collective_id=0, has_side_effects=True, vmem_limit_bytes=20 * 1024 * 1024
        ),
    )(
        *[
            pltpu.with_memory_space_constraint(array, pltpu.HBM)
            for array in (
                tokens[0],
                norm_gain,
                weight_q,
                weight_k,
                weight_v,
                attention_gradient[0],
                cosine,
                sine,
                local_fragment[0],
            )
        ]
    )
    swap = [(0, 1), (1, 0)]
    landed_a = lax.ppermute(far_a, "tp", swap)
    far_b, here_b, gain_partial = pl.pallas_call(
        functools.partial(second_kernel, tile),
        out_shape=(
            pltpu.VMEM((rows + pad, width - first), bf16),
            pltpu.VMEM((rows, width - first), bf16),
            pltpu.VMEM((1, width), f32),
        ),
        in_specs=[vmem] * 5,
        out_specs=(vmem,) * 3,
        compiler_params=pltpu.CompilerParams(vmem_limit_bytes=8 * 1024 * 1024),
        cost_estimate=pl.CostEstimate(
            flops=sequence * width * total, bytes_accessed=width * total, transcendentals=0
        ),
    )(d, normed, weights, norm_gain, gain_a)
    landed_b = lax.ppermute(far_b, "tp", swap)
    wide = 768
    columns = lambda size: pl.BlockSpec((size, wide), lambda i: (0, i))
    grad_wq, grad_wk, grad_wv, new_global, new_momentum = pl.pallas_call(
        weights_kernel,
        grid=(width // wide,),
        out_shape=(
            jax.ShapeDtypeStruct((width, qw), bf16),
            jax.ShapeDtypeStruct((width, kw), bf16),
            jax.ShapeDtypeStruct((width, kw), bf16),
            jax.ShapeDtypeStruct((frag_rows, width), f32),
            jax.ShapeDtypeStruct((frag_rows, width), f32),
        ),
        in_specs=[vmem, vmem, vmem, columns(frag_rows), columns(frag_rows)],
        out_specs=(
            pl.BlockSpec((wide, qw), lambda i: (i, 0)),
            pl.BlockSpec((wide, kw), lambda i: (i, 0)),
            pl.BlockSpec((wide, kw), lambda i: (i, 0)),
            columns(frag_rows),
            columns(frag_rows),
        ),
        compiler_params=pltpu.CompilerParams(vmem_limit_bytes=28 * 1024 * 1024),
        cost_estimate=pl.CostEstimate(
            flops=2 * sequence * width * total, bytes_accessed=3 * width * total, transcendentals=0
        ),
    )(normed, d, mean_local, global_fragment, momentum)
    count = rows // 2
    block = pl.BlockSpec((count, width), lambda i: (i, 0))
    gradient_rows, gains_gradient = pl.pallas_call(
        rows_kernel,
        grid=(rows // count,),
        out_shape=(
            jax.ShapeDtypeStruct((rows, width), bf16),
            jax.ShapeDtypeStruct((1, width), f32),
        ),
        in_specs=[vmem] * 7,
        out_specs=(block, pl.BlockSpec((1, width), lambda i: (0, 0))),
        compiler_params=pltpu.CompilerParams(vmem_limit_bytes=8 * 1024 * 1024),
        cost_estimate=pl.CostEstimate(
            flops=12 * rows * width, bytes_accessed=4 * rows * width, transcendentals=0
        ),
    )(x, here_a, here_b, norm_gain, landed_a, landed_b, gain_partial)
    return (
        grad_wq[None],
        grad_wk[None],
        grad_wv[None],
        gains_gradient,
        gradient_rows[None],
        new_global,
        new_momentum,
    )


def solution(mesh):
    placed = (
        P("rep", "tp", None),
        P("rep", None),
        P("rep", None, "tp"),
        P("rep", None, "tp"),
        P("rep", None, "tp"),
        P("rep", None, "tp"),
        P("tp", None),
        P("tp", None),
        P("rep", "tp", None),
    )
    paired = mesh.shape["tp"] == 2 and mesh.shape["rep"] % 2 == 0
    chosen = functools.partial(pair_parts, mesh.shape["rep"]) if paired else body
    return jax.shard_map(
        chosen,
        mesh=mesh,
        in_specs=placed,
        out_specs=(
            P("rep", None, "tp"),
            P("rep", None, "tp"),
            P("rep", None, "tp"),
            P("rep", None),
            P("rep", "tp", None),
            P("tp", None),
            P("tp", None),
        ),
        check_vma=False,
    )
```

```python
import functools

import jax
import jax.numpy as jnp
import numpy as np
from jax import lax
from jax.experimental import pallas as pl
from jax.experimental.pallas import tpu as pltpu
from jax.sharding import PartitionSpec as P


MESH = pl.DeviceIdType.MESH

HEAD_SIZE = 128


epsilon = 1e-05
rope_base = 500000.0
outer_rate = 0.7
outer_momentum = 0.9
LOG2_E = 1.4426950408889634
LANES = 128
SUBLANES = 8


def rope_tables(sequence_length, width):
    middle = width // 2
    frequency = rope_base ** (-2.0 * jnp.arange(middle, dtype=jnp.float32) / width)
    angles = jnp.arange(sequence_length, dtype=jnp.float32)[:, None] * frequency[None, :]
    angles = jnp.concatenate([angles, angles], axis=1)
    return (jnp.cos(angles)[:, None, :], jnp.sin(angles)[:, None, :])


def rotate(vectors, cosine_table, sine_table):
    middle = vectors.shape[-1] // 2
    turned = jnp.concatenate([-vectors[..., middle:], vectors[..., :middle]], axis=-1)
    return vectors * cosine_table + turned * sine_table


def reverse_rotation(gradient, cosine_table, sine_table):
    middle = gradient.shape[-1] // 2
    shifted = gradient * sine_table
    turned = jnp.concatenate([shifted[..., middle:], -shifted[..., :middle]], axis=-1)
    return gradient * cosine_table + turned


def attention_reverse(query_rows, rotated_keys, values_bfloat, grad_out, block_of_rows):
    sequence_length = query_rows.shape[0]
    score_scale = query_rows.shape[-1] ** (-0.5)

    def one_block(running, block_index):
        acc_key, acc_value = running
        offset = block_index * block_of_rows
        query_block = lax.dynamic_slice_in_dim(query_rows, offset, block_of_rows, 0)
        grad_block = lax.dynamic_slice_in_dim(grad_out, offset, block_of_rows, 0)
        scores = (
            jnp.einsum(
                "qgrd,kgd->grqk", query_block, rotated_keys, preferred_element_type=jnp.float32
            )
            * score_scale
        )
        row_pos = offset + jnp.arange(block_of_rows)
        col_pos = jnp.arange(sequence_length)
        allowed = col_pos[None, :] <= row_pos[:, None]
        scores = jnp.where(allowed, scores, -jnp.inf)
        highest = jnp.max(scores, axis=-1, keepdims=True)
        powers = jnp.exp(scores - highest)
        probability = powers / jnp.sum(powers, axis=-1, keepdims=True)
        prob_low = probability.astype(jnp.bfloat16)
        acc_value = acc_value + jnp.einsum(
            "grqk,qgrd->kgd", prob_low, grad_block, preferred_element_type=jnp.float32
        )
        grad_prob = jnp.einsum(
            "qgrd,kgd->grqk", grad_block, values_bfloat, preferred_element_type=jnp.float32
        )
        grad_score = (
            probability
            * (grad_prob - jnp.sum(grad_prob * probability, axis=-1, keepdims=True))
            * score_scale
        )
        score_low = grad_score.astype(jnp.bfloat16)
        grad_query = jnp.einsum(
            "grqk,kgd->qgrd", score_low, rotated_keys, preferred_element_type=jnp.float32
        )
        acc_key = acc_key + jnp.einsum(
            "grqk,qgrd->kgd", score_low, query_block, preferred_element_type=jnp.float32
        )
        return ((acc_key, acc_value), grad_query)

    initial = jnp.zeros(rotated_keys.shape, jnp.float32)
    (acc_key, acc_value), grad_blocks = lax.scan(
        one_block, (initial, initial), jnp.arange(sequence_length // block_of_rows)
    )
    return (grad_blocks.reshape(query_rows.shape), acc_key, acc_value)


def body(
    tokens,
    norm_gain,
    w_query,
    key_weight,
    value_weight,
    attention_gradient,
    global_fragment,
    momentum,
    local_fragment,
):
    local_rows = tokens[0]
    norm_gains = norm_gain[0]
    weight_q = w_query[0]
    weight_k = key_weight[0]
    weight_v = value_weight[0]
    widened_rows = local_rows.astype(jnp.float32)
    inverse_norm = lax.rsqrt(
        jnp.mean(widened_rows * widened_rows, axis=-1, keepdims=True) + epsilon
    )
    normalized_input = widened_rows * inverse_norm
    normalized_local = (normalized_input * norm_gains[None, :]).astype(jnp.bfloat16)
    normalized = lax.all_gather(normalized_local, "tp", axis=0, tiled=True)
    sequence_length = normalized.shape[0]
    heads_q = weight_q.shape[1] // HEAD_SIZE
    heads_kv = weight_k.shape[1] // HEAD_SIZE
    cosine_table, sine_table = rope_tables(sequence_length, HEAD_SIZE)
    query_rows = jnp.dot(normalized, weight_q, preferred_element_type=jnp.float32).reshape(
        sequence_length, heads_q, HEAD_SIZE
    )
    query_rows = rotate(query_rows, cosine_table, sine_table).astype(jnp.bfloat16)
    rotated_keys = jnp.dot(normalized, weight_k, preferred_element_type=jnp.float32).reshape(
        sequence_length, heads_kv, HEAD_SIZE
    )
    rotated_keys = rotate(rotated_keys, cosine_table, sine_table).astype(jnp.bfloat16)
    values_bfloat = (
        jnp.dot(normalized, weight_v, preferred_element_type=jnp.float32)
        .astype(jnp.bfloat16)
        .reshape(sequence_length, heads_kv, HEAD_SIZE)
    )
    replica_group = heads_q // heads_kv
    block_of_rows = min(512, sequence_length)
    query_input_gradient, key_input_gradient, value_input_gradient = attention_reverse(
        query_rows.reshape(sequence_length, heads_kv, replica_group, HEAD_SIZE),
        rotated_keys,
        values_bfloat,
        attention_gradient[0].reshape(sequence_length, heads_kv, replica_group, HEAD_SIZE),
        block_of_rows,
    )
    dquery = (
        reverse_rotation(
            query_input_gradient.reshape(sequence_length, heads_q, HEAD_SIZE),
            cosine_table,
            sine_table,
        )
        .astype(jnp.bfloat16)
        .reshape(sequence_length, heads_q * HEAD_SIZE)
    )
    key_gradient = (
        reverse_rotation(key_input_gradient, cosine_table, sine_table)
        .astype(jnp.bfloat16)
        .reshape(sequence_length, heads_kv * HEAD_SIZE)
    )
    value_gradient = value_input_gradient.astype(jnp.bfloat16).reshape(
        sequence_length, heads_kv * HEAD_SIZE
    )
    contract = (((0,), (0,)), ((), ()))
    grad_wq = lax.dot_general(
        normalized, dquery, contract, preferred_element_type=jnp.float32
    ).astype(jnp.bfloat16)
    grad_wk = lax.dot_general(
        normalized, key_gradient, contract, preferred_element_type=jnp.float32
    ).astype(jnp.bfloat16)
    grad_wv = lax.dot_general(
        normalized, value_gradient, contract, preferred_element_type=jnp.float32
    ).astype(jnp.bfloat16)
    back = (((1,), (1,)), ((), ()))
    partial_value = lax.dot_general(dquery, weight_q, back, preferred_element_type=jnp.float32)
    partial_value = partial_value + lax.dot_general(
        key_gradient, weight_k, back, preferred_element_type=jnp.float32
    )
    summed_rows = lax.psum_scatter(
        (
            partial_value
            + lax.dot_general(value_gradient, weight_v, back, preferred_element_type=jnp.float32)
        ).astype(jnp.bfloat16),
        "tp",
        scatter_dimension=0,
        tiled=True,
    ).astype(jnp.float32)
    gains_gradient = lax.psum(jnp.sum(summed_rows * normalized_input, axis=0), "tp")
    scaled_rows = summed_rows * norm_gains[None, :]
    gradient_rows = (
        inverse_norm
        * (
            scaled_rows
            - normalized_input * jnp.mean(scaled_rows * normalized_input, axis=-1, keepdims=True)
        )
    ).astype(jnp.bfloat16)
    delta = global_fragment - local_fragment[0].astype(jnp.float32)
    replicas = lax.axis_size("rep")
    mean_delta = lax.psum(delta, "rep") / replicas
    new_momentum = outer_momentum * momentum + mean_delta
    new_global = global_fragment - outer_rate * (mean_delta + outer_momentum * new_momentum)
    return (
        grad_wq[None],
        grad_wk[None],
        grad_wv[None],
        gains_gradient[None],
        gradient_rows[None],
        new_global,
        new_momentum,
    )


NT = (((1,), (1,)), ((), ()))
TN = (((0,), (0,)), ((), ()))


def dot(a, b, dims=(((1,), (0,)), ((), ()))):
    return lax.dot_general(a, b, dims, preferred_element_type=jnp.float32)


def ds(index, size):
    return pl.ds(pl.multiple_of(index * size, size), size)


def host_tables(sequence_length, width):
    middle = width // 2
    frequency = rope_base ** (-2.0 * np.arange(middle) / width)
    angles = np.arange(sequence_length)[:, None] * frequency[None, :]
    cosine, sine = np.cos(angles), np.sin(angles)
    return (
        jnp.asarray(np.concatenate([cosine, cosine], axis=1), jnp.float32),
        jnp.asarray(np.concatenate([-sine, sine], axis=1), jnp.float32),
    )


def shares(d_ref, nm_ref, w_ref, gain_ref, far_ref, here_ref, gain_part_ref, low, tile):
    me = lax.axis_index("tp")
    peer = 1 - me
    rows = here_ref.shape[0]
    offset = gain_part_ref.shape[1] - here_ref.shape[1] if low else 0

    def back(t, _):
        both = jnp.concatenate([d_ref[ds(peer, rows), :], d_ref[ds(me, rows), :]], axis=0)
        cols = pl.ds(pl.multiple_of(low + t * tile, tile), tile)
        own = ds(t, tile)
        part = dot(both, w_ref[cols, :], NT).astype(jnp.bfloat16)
        far_ref[pl.ds(0, rows), own] = part[:rows]
        here_ref[:, own] = part[rows:]
        wide = part.astype(jnp.float32)
        products = wide[:rows] * nm_ref[ds(peer, rows), cols].astype(jnp.float32)
        products += wide[rows:] * nm_ref[ds(me, rows), cols].astype(jnp.float32)
        gain_part = jnp.sum(products, axis=0, keepdims=True) / gain_ref[:, cols]
        gain_part_ref[:, pl.ds(pl.multiple_of(offset + t * tile, tile), tile)] = gain_part
        return 0

    lax.fori_loop(0, here_ref.shape[1] // tile, back, 0, unroll=True)


def front_kernel(
    n_rep,
    chunks,
    tile,
    tokens_hbm,
    gain_hbm,
    wq_hbm,
    wk_hbm,
    wv_hbm,
    go_hbm,
    cos_hbm,
    sin_hbm,
    local_hbm,
    x_ref,
    nm_ref,
    d_ref,
    here_ref,
    far_ref,
    gain_part_ref,
    mean_ref,
    w_ref,
    gain_ref,
    go_ref,
    cos_ref,
    sin_ref,
    acc_ref,
    q_ref,
    k_ref,
    v_ref,
    raw_ref,
    wide_ref,
    inv_ref,
    mine_ref,
    theirs_ref,
    pair_ref,
    pieces_ref,
    own_mean_ref,
    in_sems,
    w_sems,
    ag_send,
    ag_recv,
    fr_send,
    fr_recv,
    fg_send,
    fg_recv,
    pair_sems,
    own_sem,
    go_sem,
):
    me = lax.axis_index("tp")
    peer = 1 - me
    rep = lax.axis_index("rep")
    side = lax.rem(rep, 2)
    partner = rep + 1 - 2 * side
    lane = rep // 2
    n_lanes = n_rep // 2
    rows, width = x_ref.shape
    qw, kw = wq_hbm.shape[1], wk_hbm.shape[1]
    total = qw + 2 * kw
    cw = width // chunks
    piece_rows, piece_cols = own_mean_ref.shape
    col_blocks = width // piece_cols

    def along(j):
        return 2 * lax.rem(lane + j, n_lanes) + side

    barrier = pltpu.get_barrier_semaphore()
    pl.semaphore_signal(barrier, inc=1, device_id={"tp": peer}, device_id_type=MESH)
    pl.semaphore_signal(barrier, inc=1, device_id={"rep": partner}, device_id_type=MESH)

    @pl.when(side == 1)
    def _():
        def greet(j, _):
            pl.semaphore_signal(barrier, inc=1, device_id={"rep": along(j)}, device_id_type=MESH)
            return 0

        lax.fori_loop(1, n_lanes, greet, 0)

    first_copies = [
        pltpu.make_async_copy(tokens_hbm, x_ref, in_sems.at[0]),
        pltpu.make_async_copy(gain_hbm, gain_ref, in_sems.at[1]),
    ]
    late_copies = [
        pltpu.make_async_copy(cos_hbm, cos_ref, in_sems.at[2]),
        pltpu.make_async_copy(sin_hbm, sin_ref, in_sems.at[3]),
        pltpu.make_async_copy(go_hbm, go_ref, in_sems.at[4]),
    ]
    half_copy = pltpu.make_async_copy(local_hbm, mine_ref, own_sem)
    weight_copies = []
    for source, offset in ((wq_hbm, 0), (wk_hbm, qw), (wv_hbm, qw + kw)):
        for t in range(source.shape[1] // tile):
            weight_copies.append(
                pltpu.make_async_copy(
                    source.at[:, pl.ds(t * tile, tile)],
                    w_ref.at[:, pl.ds(offset + t * tile, tile)],
                    w_sems.at[len(weight_copies)],
                )
            )
    for copy in first_copies:
        copy.start()

    @pl.when(side == 1)
    def _():
        half_copy.start()


    def gather_copy(c, source=x_ref):
        return pltpu.make_async_remote_copy(
            src_ref=source.at[:, ds(c, cw)],
            dst_ref=raw_ref.at[:, ds(c, cw)],
            send_sem=ag_send,
            recv_sem=ag_recv.at[c],
            device_id={"tp": peer},
            device_id_type=MESH,
        )

    norm_copy = pltpu.make_async_remote_copy(
        src_ref=inv_ref.at[0],
        dst_ref=inv_ref.at[1],
        send_sem=pair_sems.at[0],
        recv_sem=pair_sems.at[1],
        device_id={"tp": peer},
        device_id_type=MESH,
    )
    pair_copy = pltpu.make_async_remote_copy(
        src_ref=local_hbm,
        dst_ref=theirs_ref,
        send_sem=pair_sems.at[2],
        recv_sem=pair_sems.at[3],
        device_id={"rep": partner},
        device_id_type=MESH,
    )

    mean_copy = pltpu.make_async_remote_copy(
        src_ref=mean_ref,
        dst_ref=mean_ref,
        send_sem=pair_sems.at[4],
        recv_sem=pair_sems.at[5],
        device_id={"rep": partner},
        device_id_type=MESH,
    )

    def piece(owner):
        return (
            ds(owner // col_blocks, piece_rows),
            ds(lax.rem(owner, col_blocks), piece_cols),
        )

    def scatter_copy(j):
        return pltpu.make_async_remote_copy(
            src_ref=pair_ref.at[piece(lax.rem(lane + j, n_lanes))],
            dst_ref=pieces_ref.at[j],
            send_sem=fr_send,
            recv_sem=fr_recv,
            device_id={"rep": along(j)},
            device_id_type=MESH,
        )

    def spread_copy(j, owner):
        return pltpu.make_async_remote_copy(
            src_ref=own_mean_ref,
            dst_ref=mean_ref.at[piece(owner)],
            send_sem=fg_send,
            recv_sem=fg_recv,
            device_id={"rep": along(j)},
            device_id_type=MESH,
        )

    def all_of(part, send_sem, recv_sem):
        return pltpu.make_async_remote_copy(
            src_ref=part,
            dst_ref=part,
            send_sem=send_sem,
            recv_sem=recv_sem,
            device_id={"rep": partner},
            device_id_type=MESH,
        )

    others = pieces_ref.at[pl.ds(1, n_lanes - 1)]
    all_scattered = all_of(others, fr_send, fr_recv)
    all_spread = all_of(others, fg_send, fg_recv)
    all_gathered = all_of(x_ref, ag_send, own_sem)

    def start_all(make, low, high):
        def one(j, _):
            make(j).start()
            return 0

        lax.fori_loop(low, high, one, 0)

    early = chunks // 3

    @pl.when(side == 0)
    def _():
        pl.semaphore_wait(barrier, 2)
        start_all(lambda c: gather_copy(c, tokens_hbm), 0, early)
        pair_copy.start()

    for copy in first_copies:
        copy.wait()

    for copy in weight_copies + late_copies:
        copy.start()

    step = 16

    def norm_rows(i, _):
        x = x_ref[ds(i, step), :].astype(jnp.float32)
        inverse = lax.rsqrt(jnp.mean(x * x, axis=-1, keepdims=True) + epsilon)
        wide_ref[ds(i, step), :] = jnp.broadcast_to(inverse, (step, LANES))
        nm_ref[pl.ds(pl.multiple_of(me * rows + i * step, step), step), :] = (
            x * inverse * gain_ref[...]
        ).astype(jnp.bfloat16)
        return 0

    lax.fori_loop(0, rows // step, norm_rows, 0, unroll=2)
    inv_ref[0] = wide_ref[...].T[:SUBLANES]

    @pl.when(side == 1)
    def _():
        pl.semaphore_wait(barrier, n_lanes + 1)

    norm_copy.start()

    @pl.when(side == 0)
    def _():
        start_all(gather_copy, early, chunks)

    @pl.when(side == 1)
    def _():
        half_copy.wait()
        pair_copy.wait_recv()
        pair_ref[...] = (
            mine_ref[...].astype(jnp.float32) + theirs_ref[...].astype(jnp.float32)
        ).astype(jnp.bfloat16)
        start_all(scatter_copy, 1, n_lanes)

    heads_q, heads_kv = qw // HEAD_SIZE, kw // HEAD_SIZE
    for t, copy in enumerate(weight_copies):
        copy.wait()
        acc_ref[ds(me, rows), pl.ds(t * tile, tile)] = dot(
            nm_ref[ds(me, rows), :], w_ref[:, pl.ds(t * tile, tile)]
        )
    acc_ref[ds(peer, rows), :] = jnp.zeros((rows, total), jnp.float32)
    for copy in late_copies:
        copy.wait()

    def rope_rows(which):
        block = ds(which, rows)
        cosine, sine = cos_ref[block, :], sin_ref[block, :]

        def rope_head(source, target, index):
            vector = acc_ref[block, pl.ds(source * HEAD_SIZE, HEAD_SIZE)]
            target[block, pl.ds(index * HEAD_SIZE, HEAD_SIZE)] = (
                vector * cosine + pltpu.roll(vector, HEAD_SIZE // 2, 1) * sine
            ).astype(jnp.bfloat16)

        for h in range(heads_q):
            rope_head(h, q_ref, h)
        for h in range(heads_kv):
            rope_head(heads_q + h, k_ref, h)
        v_ref[block, :] = acc_ref[block, pl.ds(qw + kw, kw)].astype(jnp.bfloat16)

    rope_rows(me)

    def average_pieces():
        all_scattered.wait_recv()
        summed = pair_ref[piece(lane)].astype(jnp.float32)
        for j in range(1, n_lanes):
            summed = summed + pieces_ref[j].astype(jnp.float32)
        summed = (summed * (1.0 / n_rep)).astype(jnp.bfloat16)
        own_mean_ref[...] = summed
        mean_ref[piece(lane)] = summed
        start_all(lambda j: spread_copy(j, lane), 1, n_lanes)

    def pass_mean():
        all_spread.wait_recv()
        mean_copy.start()

    @pl.when(side == 1)
    def _():
        average_pieces()
        pl.semaphore_wait(go_sem, 1)
        start_all(gather_copy, 0, chunks)

    norm_copy.wait_recv()
    wide_ref[...] = jnp.broadcast_to(inv_ref[1][:1], (LANES, rows)).T

    def arrived(c, _):
        gather_copy(c).wait_recv()

        @pl.when((side == 0) & (c == chunks - 5))
        def _():
            pl.semaphore_signal(go_sem, inc=1, device_id={"rep": partner}, device_id_type=MESH)

        @pl.when((side == 1) & (c == chunks - 8))
        def _():
            pass_mean()

        inverse = wide_ref[...]
        parts = []
        for part in range(cw // LANES):
            cols = pl.ds(pl.multiple_of(c * cw + part * LANES, LANES), LANES)
            parts.append(
                (raw_ref[:, cols].astype(jnp.float32) * inverse * gain_ref[:, cols]).astype(
                    jnp.bfloat16
                )
            )
        part = jnp.concatenate(parts, axis=1)
        nm_ref[ds(peer, rows), ds(c, cw)] = part
        acc_ref[ds(peer, rows), :] += dot(part, w_ref[ds(c, cw), :])
        return 0

    lax.fori_loop(0, chunks, arrived, 0)
    rope_rows(peer)

    group = heads_q // heads_kv
    scale = HEAD_SIZE ** (-0.5)
    key_pos = lax.broadcasted_iota(jnp.int32, (rows, rows), 0)
    query_pos = lax.broadcasted_iota(jnp.int32, (rows, rows), 1)
    bias = jnp.where(key_pos <= query_pos, 0.0, -jnp.inf).astype(jnp.float32)
    bias = jnp.concatenate([bias] * group, axis=1)

    def reverse(gradient, block):
        c = cos_ref[block * rows : (block + 1) * rows]
        s = sin_ref[block * rows : (block + 1) * rows]
        return (gradient * c - pltpu.roll(gradient, HEAD_SIZE // 2, 1) * s).astype(jnp.bfloat16)

    def kv_heads(low):
        members = range(low, low + 4)
        grads = {}
        for b in range(2):
            keys = (b + 1) * rows
            block = pl.ds(b * rows, rows)
            loaded, dots, soft = {}, {}, {}
            for g in members:
                heads = [pl.ds((g * group + r) * HEAD_SIZE, HEAD_SIZE) for r in range(group)]
                kv = pl.ds(g * HEAD_SIZE, HEAD_SIZE)
                query = jnp.concatenate([q_ref[block, head] for head in heads], axis=0)
                out_grad = jnp.concatenate([go_ref[block, head] for head in heads], axis=0)
                key = k_ref[pl.ds(0, keys), kv]
                value = v_ref[pl.ds(0, keys), kv]
                loaded[g] = heads, query, out_grad, key
                dots[g] = dot(key, query, NT), dot(value, out_grad, NT)
            for g in members:
                scores, grad_prob = dots[g]
                if b == 0:
                    scores = scores + bias
                else:
                    scores = jnp.concatenate([scores[:rows], scores[rows:] + bias], axis=0)
                highest = jnp.max(scores, axis=0, keepdims=True)
                powers = jnp.exp2((scores - highest) * (scale * LOG2_E))
                prob = powers * (1.0 / jnp.sum(powers, axis=0, keepdims=True))
                inner = jnp.sum(grad_prob * prob, axis=0, keepdims=True)
                score_low = (prob * (grad_prob - inner) * scale).astype(jnp.bfloat16)
                soft[g] = prob.astype(jnp.bfloat16), score_low
            for g in members:
                heads, query, out_grad, key = loaded[g]
                prob_low, score_low = soft[g]
                part_v = dot(prob_low, out_grad)
                part_k = dot(score_low, query)
                grad_q = dot(score_low, key, TN)
                for r, head in enumerate(heads):
                    d_ref[block, head] = reverse(grad_q[r * rows : (r + 1) * rows], b)
                for j in range(b + 1):
                    pv = part_v[j * rows : (j + 1) * rows]
                    pk = part_k[j * rows : (j + 1) * rows]
                    if (g, j) in grads:
                        pv, pk = pv + grads[g, j][0], pk + grads[g, j][1]
                    grads[g, j] = pv, pk
        for g in members:
            for j in range(2):
                block = pl.ds(j * rows, rows)
                low_k = (heads_q + g) * HEAD_SIZE
                d_ref[block, pl.ds(low_k, HEAD_SIZE)] = reverse(grads[g, j][1], j)
                low_v = (heads_q + heads_kv + g) * HEAD_SIZE
                d_ref[block, pl.ds(low_v, HEAD_SIZE)] = grads[g, j][0].astype(jnp.bfloat16)

    for low in range(0, heads_kv, 4):
        kv_heads(low)

    shares(d_ref, nm_ref, w_ref, gain_ref, far_ref, here_ref, gain_part_ref, 0, tile)

    norm_copy.wait_send()
    all_gathered.wait_send()

    @pl.when(side == 0)
    def _():
        pair_copy.wait_send()
        mean_copy.wait_recv()

    @pl.when(side == 1)
    def _():
        all_scattered.wait_send()
        all_spread.wait_send()
        mean_copy.wait_send()


def second_kernel(
    tile, d_ref, nm_ref, w_ref, gain_ref, gain_a_ref, far_ref, here_ref, gain_part_ref
):
    rows, cols = here_ref.shape
    done = gain_a_ref.shape[1]
    gain_part_ref[:, pl.ds(0, done)] = gain_a_ref[...]
    shares(d_ref, nm_ref, w_ref, gain_ref, far_ref, here_ref, gain_part_ref, done, tile)
    lines = []
    for low in range(0, done + cols, cols):
        gain_part = gain_part_ref[:, pl.ds(low, cols)]
        for _ in range(3):
            lines.append(gain_part.astype(jnp.bfloat16).astype(jnp.float32))
            gain_part = gain_part - lines[-1]
    pad = far_ref.shape[0] - rows
    lines = jnp.concatenate(lines + [jnp.zeros((pad - len(lines), cols), jnp.float32)], axis=0)
    far_ref[pl.ds(rows, pad), :] = lines.astype(jnp.bfloat16)


def weights_kernel(nm_ref, d_ref, mean_ref, global_ref, momentum_ref, gq_ref, gk_ref, gv_ref, ng_ref, nmom_ref):
    i = pl.program_id(0)
    wide = gq_ref.shape[0]
    qw, kw = gq_ref.shape[1], gk_ref.shape[1]
    grad = dot(nm_ref[:, ds(i, wide)], d_ref[...], TN).astype(jnp.bfloat16)
    gq_ref[...] = grad[:, :qw]
    gk_ref[...] = grad[:, qw : qw + kw]
    gv_ref[...] = grad[:, qw + kw :]
    held = global_ref[...]
    mean_delta = held - mean_ref[:, ds(i, wide)].astype(jnp.float32)
    new_momentum = outer_momentum * momentum_ref[...] + mean_delta
    nmom_ref[...] = new_momentum
    ng_ref[...] = held - outer_rate * (mean_delta + outer_momentum * new_momentum)


def rows_kernel(
    x_ref, here_a_ref, here_b_ref, gain_ref, landed_a_ref, landed_b_ref, part_ref, out_ref, gain_out_ref
):
    i = pl.program_id(0)
    count = out_ref.shape[0]
    rows, _ = x_ref.shape

    @pl.when(i == 0)
    def _():
        lines = landed_b_ref[pl.ds(rows, landed_b_ref.shape[0] - rows), :].astype(jnp.float32)
        sums = [lines[k + 2 : k + 3] + lines[k + 1 : k + 2] + lines[k : k + 1] for k in (0, 3)]
        gain_out_ref[...] = part_ref[...] + jnp.concatenate(sums, axis=1)

    step = 16

    def some(j, _):
        block = pl.ds(pl.multiple_of(i * count + j * step, step), step)
        x = x_ref[block, :].astype(jnp.float32)
        inverse = lax.rsqrt(jnp.mean(x * x, axis=-1, keepdims=True) + epsilon)
        summed = [
            here[block, :].astype(jnp.float32) + landed[block, :].astype(jnp.float32)
            for here, landed in ((here_a_ref, landed_a_ref), (here_b_ref, landed_b_ref))
        ]
        scaled = jnp.concatenate(summed, axis=1) * gain_ref[...]
        pull = jnp.mean(scaled * x, axis=-1, keepdims=True) * (inverse * inverse)
        out_ref[ds(j, step), :] = (inverse * (scaled - x * pull)).astype(jnp.bfloat16)
        return 0

    lax.fori_loop(0, count // step, some, 0, unroll=True)


def pair_parts(
    n_rep,
    tokens,
    norm_gain,
    w_query,
    key_weight,
    value_weight,
    attention_gradient,
    global_fragment,
    momentum,
    local_fragment,
):
    rows, width = tokens.shape[1:]
    sequence = 2 * rows
    weight_q, weight_k, weight_v = w_query[0], key_weight[0], value_weight[0]
    qw, kw = weight_q.shape[1], weight_k.shape[1]
    total = qw + 2 * kw
    frag_rows = local_fragment.shape[1]
    piece_rows = 16
    n_lanes = n_rep // 2
    piece_cols = width * frag_rows // piece_rows // n_lanes
    chunks = 12
    tile = 512
    pad = 8
    first = width // 2
    bf16, f32 = jnp.bfloat16, jnp.float32
    cosine, sine = host_tables(sequence, HEAD_SIZE)
    vmem = pl.BlockSpec(memory_space=pltpu.VMEM)
    hbm = pl.BlockSpec(memory_space=pltpu.HBM)
    x, normed, d, here_a, far_a, gain_a, mean_local, weights = pl.pallas_call(
        functools.partial(front_kernel, n_rep, chunks, tile),
        out_shape=(
            pltpu.VMEM((rows, width), bf16),
            pltpu.VMEM((sequence, width), bf16),
            pltpu.VMEM((sequence, total), bf16),
            pltpu.VMEM((rows, first), bf16),
            pltpu.VMEM((rows, first), bf16),
            pltpu.VMEM((1, first), f32),
            pltpu.VMEM((frag_rows, width), bf16),
            pltpu.VMEM((width, total), bf16),
        ),
        in_specs=[hbm] * 9,
        out_specs=(vmem,) * 8,
        scratch_shapes=[
            pltpu.VMEM((1, width), f32),
            pltpu.VMEM((sequence, qw), bf16),
            pltpu.VMEM((sequence, HEAD_SIZE), f32),
            pltpu.VMEM((sequence, HEAD_SIZE), f32),
            pltpu.VMEM((sequence, total), f32),
            pltpu.VMEM((sequence, qw), bf16),
            pltpu.VMEM((sequence, kw), bf16),
            pltpu.VMEM((sequence, kw), bf16),
            pltpu.VMEM((rows, width), bf16),
            pltpu.VMEM((rows, LANES), f32),
            pltpu.VMEM((2, SUBLANES, rows), f32),
            pltpu.VMEM((frag_rows, width), bf16),
            pltpu.VMEM((frag_rows, width), bf16),
            pltpu.VMEM((frag_rows, width), bf16),
            pltpu.VMEM((n_lanes, piece_rows, piece_cols), bf16),
            pltpu.VMEM((piece_rows, piece_cols), bf16),
            pltpu.SemaphoreType.DMA((5,)),
            pltpu.SemaphoreType.DMA((total // tile,)),
            pltpu.SemaphoreType.DMA,
            pltpu.SemaphoreType.DMA((chunks,)),
            pltpu.SemaphoreType.DMA,
            pltpu.SemaphoreType.DMA,
            pltpu.SemaphoreType.DMA,
            pltpu.SemaphoreType.DMA,
            pltpu.SemaphoreType.DMA((6,)),
            pltpu.SemaphoreType.DMA,
            pltpu.SemaphoreType.REGULAR,
        ],
        compiler_params=pltpu.CompilerParams(
            collective_id=0, has_side_effects=True, vmem_limit_bytes=20 * 1024 * 1024
        ),
    )(
        *[
            pltpu.with_memory_space_constraint(array, pltpu.HBM)
            for array in (
                tokens[0],
                norm_gain,
                weight_q,
                weight_k,
                weight_v,
                attention_gradient[0],
                cosine,
                sine,
                local_fragment[0],
            )
        ]
    )
    swap = [(0, 1), (1, 0)]
    landed_a = lax.ppermute(far_a, "tp", swap)
    far_b, here_b, gain_partial = pl.pallas_call(
        functools.partial(second_kernel, tile),
        out_shape=(
            pltpu.VMEM((rows + pad, width - first), bf16),
            pltpu.VMEM((rows, width - first), bf16),
            pltpu.VMEM((1, width), f32),
        ),
        in_specs=[vmem] * 5,
        out_specs=(vmem,) * 3,
        compiler_params=pltpu.CompilerParams(vmem_limit_bytes=8 * 1024 * 1024),
        cost_estimate=pl.CostEstimate(
            flops=sequence * width * total, bytes_accessed=width * total, transcendentals=0
        ),
    )(d, normed, weights, norm_gain, gain_a)
    landed_b = lax.ppermute(far_b, "tp", swap)
    wide = 768
    columns = lambda size: pl.BlockSpec((size, wide), lambda i: (0, i))
    grad_wq, grad_wk, grad_wv, new_global, new_momentum = pl.pallas_call(
        weights_kernel,
        grid=(width // wide,),
        out_shape=(
            jax.ShapeDtypeStruct((width, qw), bf16),
            jax.ShapeDtypeStruct((width, kw), bf16),
            jax.ShapeDtypeStruct((width, kw), bf16),
            jax.ShapeDtypeStruct((frag_rows, width), f32),
            jax.ShapeDtypeStruct((frag_rows, width), f32),
        ),
        in_specs=[vmem, vmem, vmem, columns(frag_rows), columns(frag_rows)],
        out_specs=(
            pl.BlockSpec((wide, qw), lambda i: (i, 0)),
            pl.BlockSpec((wide, kw), lambda i: (i, 0)),
            pl.BlockSpec((wide, kw), lambda i: (i, 0)),
            columns(frag_rows),
            columns(frag_rows),
        ),
        compiler_params=pltpu.CompilerParams(vmem_limit_bytes=28 * 1024 * 1024),
        cost_estimate=pl.CostEstimate(
            flops=2 * sequence * width * total, bytes_accessed=3 * width * total, transcendentals=0
        ),
    )(normed, d, mean_local, global_fragment, momentum)
    count = rows // 2
    block = pl.BlockSpec((count, width), lambda i: (i, 0))
    gradient_rows, gains_gradient = pl.pallas_call(
        rows_kernel,
        grid=(rows // count,),
        out_shape=(
            jax.ShapeDtypeStruct((rows, width), bf16),
            jax.ShapeDtypeStruct((1, width), f32),
        ),
        in_specs=[vmem] * 7,
        out_specs=(block, pl.BlockSpec((1, width), lambda i: (0, 0))),
        compiler_params=pltpu.CompilerParams(vmem_limit_bytes=8 * 1024 * 1024),
        cost_estimate=pl.CostEstimate(
            flops=12 * rows * width, bytes_accessed=4 * rows * width, transcendentals=0
        ),
    )(x, here_a, here_b, norm_gain, landed_a, landed_b, gain_partial)
    return (
        grad_wq[None],
        grad_wk[None],
        grad_wv[None],
        gains_gradient,
        gradient_rows[None],
        new_global,
        new_momentum,
    )


def solution(mesh):
    placed = (
        P("rep", "tp", None),
        P("rep", None),
        P("rep", None, "tp"),
        P("rep", None, "tp"),
        P("rep", None, "tp"),
        P("rep", None, "tp"),
        P("tp", None),
        P("tp", None),
        P("rep", "tp", None),
    )
    paired = mesh.shape["tp"] == 2 and mesh.shape["rep"] % 2 == 0
    chosen = functools.partial(pair_parts, mesh.shape["rep"]) if paired else body
    return jax.shard_map(
        chosen,
        mesh=mesh,
        in_specs=placed,
        out_specs=(
            P("rep", None, "tp"),
            P("rep", None, "tp"),
            P("rep", None, "tp"),
            P("rep", None),
            P("rep", "tp", None),
            P("tp", None),
            P("tp", None),
        ),
        check_vma=False,
    )
```

```python
import functools

import jax
import jax.numpy as jnp
import numpy as np
from jax import lax
from jax.experimental import pallas as pl
from jax.experimental.pallas import tpu as pltpu
from jax.sharding import PartitionSpec as P


MESH = pl.DeviceIdType.MESH

HEAD_SIZE = 128


epsilon = 1e-05
rope_base = 500000.0
outer_rate = 0.7
outer_momentum = 0.9
LOG2_E = 1.4426950408889634
LANES = 128
SUBLANES = 8


def rope_tables(sequence_length, width):
    middle = width // 2
    frequency = rope_base ** (-2.0 * jnp.arange(middle, dtype=jnp.float32) / width)
    angles = jnp.arange(sequence_length, dtype=jnp.float32)[:, None] * frequency[None, :]
    angles = jnp.concatenate([angles, angles], axis=1)
    return (jnp.cos(angles)[:, None, :], jnp.sin(angles)[:, None, :])


def rotate(vectors, cosine_table, sine_table):
    middle = vectors.shape[-1] // 2
    turned = jnp.concatenate([-vectors[..., middle:], vectors[..., :middle]], axis=-1)
    return vectors * cosine_table + turned * sine_table


def reverse_rotation(gradient, cosine_table, sine_table):
    middle = gradient.shape[-1] // 2
    shifted = gradient * sine_table
    turned = jnp.concatenate([shifted[..., middle:], -shifted[..., :middle]], axis=-1)
    return gradient * cosine_table + turned


def attention_reverse(query_rows, rotated_keys, values_bfloat, grad_out, block_of_rows):
    sequence_length = query_rows.shape[0]
    score_scale = query_rows.shape[-1] ** (-0.5)

    def one_block(running, block_index):
        acc_key, acc_value = running
        offset = block_index * block_of_rows
        query_block = lax.dynamic_slice_in_dim(query_rows, offset, block_of_rows, 0)
        grad_block = lax.dynamic_slice_in_dim(grad_out, offset, block_of_rows, 0)
        scores = (
            jnp.einsum(
                "qgrd,kgd->grqk", query_block, rotated_keys, preferred_element_type=jnp.float32
            )
            * score_scale
        )
        row_pos = offset + jnp.arange(block_of_rows)
        col_pos = jnp.arange(sequence_length)
        allowed = col_pos[None, :] <= row_pos[:, None]
        scores = jnp.where(allowed, scores, -jnp.inf)
        highest = jnp.max(scores, axis=-1, keepdims=True)
        powers = jnp.exp(scores - highest)
        probability = powers / jnp.sum(powers, axis=-1, keepdims=True)
        prob_low = probability.astype(jnp.bfloat16)
        acc_value = acc_value + jnp.einsum(
            "grqk,qgrd->kgd", prob_low, grad_block, preferred_element_type=jnp.float32
        )
        grad_prob = jnp.einsum(
            "qgrd,kgd->grqk", grad_block, values_bfloat, preferred_element_type=jnp.float32
        )
        grad_score = (
            probability
            * (grad_prob - jnp.sum(grad_prob * probability, axis=-1, keepdims=True))
            * score_scale
        )
        score_low = grad_score.astype(jnp.bfloat16)
        grad_query = jnp.einsum(
            "grqk,kgd->qgrd", score_low, rotated_keys, preferred_element_type=jnp.float32
        )
        acc_key = acc_key + jnp.einsum(
            "grqk,qgrd->kgd", score_low, query_block, preferred_element_type=jnp.float32
        )
        return ((acc_key, acc_value), grad_query)

    initial = jnp.zeros(rotated_keys.shape, jnp.float32)
    (acc_key, acc_value), grad_blocks = lax.scan(
        one_block, (initial, initial), jnp.arange(sequence_length // block_of_rows)
    )
    return (grad_blocks.reshape(query_rows.shape), acc_key, acc_value)


def body(
    tokens,
    norm_gain,
    w_query,
    key_weight,
    value_weight,
    attention_gradient,
    global_fragment,
    momentum,
    local_fragment,
):
    local_rows = tokens[0]
    norm_gains = norm_gain[0]
    weight_q = w_query[0]
    weight_k = key_weight[0]
    weight_v = value_weight[0]
    widened_rows = local_rows.astype(jnp.float32)
    inverse_norm = lax.rsqrt(
        jnp.mean(widened_rows * widened_rows, axis=-1, keepdims=True) + epsilon
    )
    normalized_input = widened_rows * inverse_norm
    normalized_local = (normalized_input * norm_gains[None, :]).astype(jnp.bfloat16)
    normalized = lax.all_gather(normalized_local, "tp", axis=0, tiled=True)
    sequence_length = normalized.shape[0]
    heads_q = weight_q.shape[1] // HEAD_SIZE
    heads_kv = weight_k.shape[1] // HEAD_SIZE
    cosine_table, sine_table = rope_tables(sequence_length, HEAD_SIZE)
    query_rows = jnp.dot(normalized, weight_q, preferred_element_type=jnp.float32).reshape(
        sequence_length, heads_q, HEAD_SIZE
    )
    query_rows = rotate(query_rows, cosine_table, sine_table).astype(jnp.bfloat16)
    rotated_keys = jnp.dot(normalized, weight_k, preferred_element_type=jnp.float32).reshape(
        sequence_length, heads_kv, HEAD_SIZE
    )
    rotated_keys = rotate(rotated_keys, cosine_table, sine_table).astype(jnp.bfloat16)
    values_bfloat = (
        jnp.dot(normalized, weight_v, preferred_element_type=jnp.float32)
        .astype(jnp.bfloat16)
        .reshape(sequence_length, heads_kv, HEAD_SIZE)
    )
    replica_group = heads_q // heads_kv
    block_of_rows = min(512, sequence_length)
    query_input_gradient, key_input_gradient, value_input_gradient = attention_reverse(
        query_rows.reshape(sequence_length, heads_kv, replica_group, HEAD_SIZE),
        rotated_keys,
        values_bfloat,
        attention_gradient[0].reshape(sequence_length, heads_kv, replica_group, HEAD_SIZE),
        block_of_rows,
    )
    dquery = (
        reverse_rotation(
            query_input_gradient.reshape(sequence_length, heads_q, HEAD_SIZE),
            cosine_table,
            sine_table,
        )
        .astype(jnp.bfloat16)
        .reshape(sequence_length, heads_q * HEAD_SIZE)
    )
    key_gradient = (
        reverse_rotation(key_input_gradient, cosine_table, sine_table)
        .astype(jnp.bfloat16)
        .reshape(sequence_length, heads_kv * HEAD_SIZE)
    )
    value_gradient = value_input_gradient.astype(jnp.bfloat16).reshape(
        sequence_length, heads_kv * HEAD_SIZE
    )
    contract = (((0,), (0,)), ((), ()))
    grad_wq = lax.dot_general(
        normalized, dquery, contract, preferred_element_type=jnp.float32
    ).astype(jnp.bfloat16)
    grad_wk = lax.dot_general(
        normalized, key_gradient, contract, preferred_element_type=jnp.float32
    ).astype(jnp.bfloat16)
    grad_wv = lax.dot_general(
        normalized, value_gradient, contract, preferred_element_type=jnp.float32
    ).astype(jnp.bfloat16)
    back = (((1,), (1,)), ((), ()))
    partial_value = lax.dot_general(dquery, weight_q, back, preferred_element_type=jnp.float32)
    partial_value = partial_value + lax.dot_general(
        key_gradient, weight_k, back, preferred_element_type=jnp.float32
    )
    summed_rows = lax.psum_scatter(
        (
            partial_value
            + lax.dot_general(value_gradient, weight_v, back, preferred_element_type=jnp.float32)
        ).astype(jnp.bfloat16),
        "tp",
        scatter_dimension=0,
        tiled=True,
    ).astype(jnp.float32)
    gains_gradient = lax.psum(jnp.sum(summed_rows * normalized_input, axis=0), "tp")
    scaled_rows = summed_rows * norm_gains[None, :]
    gradient_rows = (
        inverse_norm
        * (
            scaled_rows
            - normalized_input * jnp.mean(scaled_rows * normalized_input, axis=-1, keepdims=True)
        )
    ).astype(jnp.bfloat16)
    delta = global_fragment - local_fragment[0].astype(jnp.float32)
    replicas = lax.axis_size("rep")
    mean_delta = lax.psum(delta, "rep") / replicas
    new_momentum = outer_momentum * momentum + mean_delta
    new_global = global_fragment - outer_rate * (mean_delta + outer_momentum * new_momentum)
    return (
        grad_wq[None],
        grad_wk[None],
        grad_wv[None],
        gains_gradient[None],
        gradient_rows[None],
        new_global,
        new_momentum,
    )


NT = (((1,), (1,)), ((), ()))
TN = (((0,), (0,)), ((), ()))


def dot(a, b, dims=(((1,), (0,)), ((), ()))):
    return lax.dot_general(a, b, dims, preferred_element_type=jnp.float32)


def ds(index, size):
    return pl.ds(pl.multiple_of(index * size, size), size)


def host_tables(sequence_length, width):
    middle = width // 2
    frequency = rope_base ** (-2.0 * np.arange(middle) / width)
    angles = np.arange(sequence_length)[:, None] * frequency[None, :]
    cosine, sine = np.cos(angles), np.sin(angles)
    return (
        jnp.asarray(np.concatenate([cosine, cosine], axis=1), jnp.float32),
        jnp.asarray(np.concatenate([-sine, sine], axis=1), jnp.float32),
    )


def shares(d_ref, nm_ref, w_ref, gain_ref, far_ref, here_ref, gain_part_ref, low, tile):
    me = lax.axis_index("tp")
    peer = 1 - me
    rows = here_ref.shape[0]
    offset = gain_part_ref.shape[1] - here_ref.shape[1] if low else 0

    def back(t, _):
        both = jnp.concatenate([d_ref[ds(peer, rows), :], d_ref[ds(me, rows), :]], axis=0)
        cols = pl.ds(pl.multiple_of(low + t * tile, tile), tile)
        own = ds(t, tile)
        part = dot(both, w_ref[cols, :], NT).astype(jnp.bfloat16)
        far_ref[pl.ds(0, rows), own] = part[:rows]
        here_ref[:, own] = part[rows:]
        wide = part.astype(jnp.float32)
        products = wide[:rows] * nm_ref[ds(peer, rows), cols].astype(jnp.float32)
        products += wide[rows:] * nm_ref[ds(me, rows), cols].astype(jnp.float32)
        gain_part = jnp.sum(products, axis=0, keepdims=True) / gain_ref[:, cols]
        gain_part_ref[:, pl.ds(pl.multiple_of(offset + t * tile, tile), tile)] = gain_part
        return 0

    lax.fori_loop(0, here_ref.shape[1] // tile, back, 0, unroll=True)


def front_kernel(
    n_rep,
    chunks,
    tile,
    tokens_hbm,
    gain_hbm,
    wq_hbm,
    wk_hbm,
    wv_hbm,
    go_hbm,
    cos_hbm,
    sin_hbm,
    local_hbm,
    x_ref,
    nm_ref,
    d_ref,
    here_ref,
    far_ref,
    gain_part_ref,
    mean_ref,
    w_ref,
    gain_ref,
    go_ref,
    cos_ref,
    sin_ref,
    acc_ref,
    q_ref,
    k_ref,
    v_ref,
    raw_ref,
    wide_ref,
    inv_ref,
    mine_ref,
    theirs_ref,
    pair_ref,
    pieces_ref,
    own_mean_ref,
    in_sems,
    w_sems,
    ag_send,
    ag_recv,
    fr_send,
    fr_recv,
    fg_send,
    fg_recv,
    pair_sems,
    own_sem,
    go_sem,
):
    me = lax.axis_index("tp")
    peer = 1 - me
    rep = lax.axis_index("rep")
    side = lax.rem(rep, 2)
    partner = rep + 1 - 2 * side
    lane = rep // 2
    n_lanes = n_rep // 2
    rows, width = x_ref.shape
    qw, kw = wq_hbm.shape[1], wk_hbm.shape[1]
    total = qw + 2 * kw
    cw = width // chunks
    piece_rows, piece_cols = own_mean_ref.shape
    col_blocks = width // piece_cols

    def along(j):
        return 2 * lax.rem(lane + j, n_lanes) + side

    barrier = pltpu.get_barrier_semaphore()
    pl.semaphore_signal(barrier, inc=1, device_id={"tp": peer}, device_id_type=MESH)
    pl.semaphore_signal(barrier, inc=1, device_id={"rep": partner}, device_id_type=MESH)

    @pl.when(side == 1)
    def _():
        def greet(j, _):
            pl.semaphore_signal(barrier, inc=1, device_id={"rep": along(j)}, device_id_type=MESH)
            return 0

        lax.fori_loop(1, n_lanes, greet, 0)

    first_copies = [
        pltpu.make_async_copy(tokens_hbm, x_ref, in_sems.at[0]),
        pltpu.make_async_copy(gain_hbm, gain_ref, in_sems.at[1]),
    ]
    late_copies = [
        pltpu.make_async_copy(cos_hbm, cos_ref, in_sems.at[2]),
        pltpu.make_async_copy(sin_hbm, sin_ref, in_sems.at[3]),
        pltpu.make_async_copy(go_hbm, go_ref, in_sems.at[4]),
    ]
    half_copy = pltpu.make_async_copy(local_hbm, mine_ref, own_sem)
    weight_copies = []
    for source, offset in ((wq_hbm, 0), (wk_hbm, qw), (wv_hbm, qw + kw)):
        for t in range(source.shape[1] // tile):
            weight_copies.append(
                pltpu.make_async_copy(
                    source.at[:, pl.ds(t * tile, tile)],
                    w_ref.at[:, pl.ds(offset + t * tile, tile)],
                    w_sems.at[len(weight_copies)],
                )
            )
    for copy in first_copies:
        copy.start()

    @pl.when(side == 1)
    def _():
        half_copy.start()


    def gather_copy(c, source=x_ref):
        return pltpu.make_async_remote_copy(
            src_ref=source.at[:, ds(c, cw)],
            dst_ref=raw_ref.at[:, ds(c, cw)],
            send_sem=ag_send,
            recv_sem=ag_recv.at[c],
            device_id={"tp": peer},
            device_id_type=MESH,
        )

    norm_copy = pltpu.make_async_remote_copy(
        src_ref=inv_ref.at[0],
        dst_ref=inv_ref.at[1],
        send_sem=pair_sems.at[0],
        recv_sem=pair_sems.at[1],
        device_id={"tp": peer},
        device_id_type=MESH,
    )
    pair_copy = pltpu.make_async_remote_copy(
        src_ref=local_hbm,
        dst_ref=theirs_ref,
        send_sem=pair_sems.at[2],
        recv_sem=pair_sems.at[3],
        device_id={"rep": partner},
        device_id_type=MESH,
    )

    mean_copy = pltpu.make_async_remote_copy(
        src_ref=mean_ref,
        dst_ref=mean_ref,
        send_sem=pair_sems.at[4],
        recv_sem=pair_sems.at[5],
        device_id={"rep": partner},
        device_id_type=MESH,
    )

    def piece(owner):
        return (
            ds(owner // col_blocks, piece_rows),
            ds(lax.rem(owner, col_blocks), piece_cols),
        )

    def scatter_copy(j):
        return pltpu.make_async_remote_copy(
            src_ref=pair_ref.at[piece(lax.rem(lane + j, n_lanes))],
            dst_ref=pieces_ref.at[j],
            send_sem=fr_send,
            recv_sem=fr_recv,
            device_id={"rep": along(j)},
            device_id_type=MESH,
        )

    def spread_copy(j, owner):
        return pltpu.make_async_remote_copy(
            src_ref=own_mean_ref,
            dst_ref=mean_ref.at[piece(owner)],
            send_sem=fg_send,
            recv_sem=fg_recv,
            device_id={"rep": along(j)},
            device_id_type=MESH,
        )

    def all_of(part, send_sem, recv_sem):
        return pltpu.make_async_remote_copy(
            src_ref=part,
            dst_ref=part,
            send_sem=send_sem,
            recv_sem=recv_sem,
            device_id={"rep": partner},
            device_id_type=MESH,
        )

    others = pieces_ref.at[pl.ds(1, n_lanes - 1)]
    all_scattered = all_of(others, fr_send, fr_recv)
    all_spread = all_of(others, fg_send, fg_recv)
    all_gathered = all_of(x_ref, ag_send, own_sem)

    def start_all(make, low, high):
        def one(j, _):
            make(j).start()
            return 0

        lax.fori_loop(low, high, one, 0)

    early = chunks // 3

    @pl.when(side == 0)
    def _():
        pl.semaphore_wait(barrier, 2)

        @pl.when(me == 1)
        def _():
            start_all(lambda c: gather_copy(c, tokens_hbm), 0, early)

        pair_copy.start()

    for copy in first_copies:
        copy.wait()


    @pl.when((side == 0) & (me == 0))
    def _():
        start_all(gather_copy, 0, early)

    for copy in weight_copies + late_copies:
        copy.start()

    step = 16

    def norm_rows(i, _):
        x = x_ref[ds(i, step), :].astype(jnp.float32)
        inverse = lax.rsqrt(jnp.mean(x * x, axis=-1, keepdims=True) + epsilon)
        wide_ref[ds(i, step), :] = jnp.broadcast_to(inverse, (step, LANES))
        nm_ref[pl.ds(pl.multiple_of(me * rows + i * step, step), step), :] = (
            x * inverse * gain_ref[...]
        ).astype(jnp.bfloat16)
        return 0

    lax.fori_loop(0, rows // step, norm_rows, 0, unroll=2)
    inv_ref[0] = wide_ref[...].T[:SUBLANES]

    @pl.when(side == 1)
    def _():
        pl.semaphore_wait(barrier, n_lanes + 1)

    norm_copy.start()

    @pl.when(side == 0)
    def _():
        start_all(gather_copy, early, chunks)

    @pl.when(side == 1)
    def _():
        half_copy.wait()
        pair_copy.wait_recv()
        pair_ref[...] = (
            mine_ref[...].astype(jnp.float32) + theirs_ref[...].astype(jnp.float32)
        ).astype(jnp.bfloat16)
        start_all(scatter_copy, 1, n_lanes)

    heads_q, heads_kv = qw // HEAD_SIZE, kw // HEAD_SIZE
    for t, copy in enumerate(weight_copies):
        copy.wait()
        acc_ref[ds(me, rows), pl.ds(t * tile, tile)] = dot(
            nm_ref[ds(me, rows), :], w_ref[:, pl.ds(t * tile, tile)]
        )
    acc_ref[ds(peer, rows), :] = jnp.zeros((rows, total), jnp.float32)
    for copy in late_copies:
        copy.wait()

    def rope_rows(which):
        block = ds(which, rows)
        cosine, sine = cos_ref[block, :], sin_ref[block, :]

        def rope_head(source, target, index):
            vector = acc_ref[block, pl.ds(source * HEAD_SIZE, HEAD_SIZE)]
            target[block, pl.ds(index * HEAD_SIZE, HEAD_SIZE)] = (
                vector * cosine + pltpu.roll(vector, HEAD_SIZE // 2, 1) * sine
            ).astype(jnp.bfloat16)

        for h in range(heads_q):
            rope_head(h, q_ref, h)
        for h in range(heads_kv):
            rope_head(heads_q + h, k_ref, h)
        v_ref[block, :] = acc_ref[block, pl.ds(qw + kw, kw)].astype(jnp.bfloat16)

    rope_rows(me)

    def average_pieces():
        all_scattered.wait_recv()
        summed = pair_ref[piece(lane)].astype(jnp.float32)
        for j in range(1, n_lanes):
            summed = summed + pieces_ref[j].astype(jnp.float32)
        summed = (summed * (1.0 / n_rep)).astype(jnp.bfloat16)
        own_mean_ref[...] = summed
        mean_ref[piece(lane)] = summed
        start_all(lambda j: spread_copy(j, lane), 1, n_lanes)

    def pass_mean():
        all_spread.wait_recv()
        mean_copy.start()

    @pl.when(side == 1)
    def _():
        average_pieces()
        pl.semaphore_wait(go_sem, 1)
        start_all(gather_copy, 0, chunks)

    norm_copy.wait_recv()
    wide_ref[...] = jnp.broadcast_to(inv_ref[1][:1], (LANES, rows)).T

    def arrived(c, _):
        gather_copy(c).wait_recv()

        @pl.when((side == 0) & (c == chunks - 5))
        def _():
            pl.semaphore_signal(go_sem, inc=1, device_id={"rep": partner}, device_id_type=MESH)

        @pl.when((side == 1) & (c == chunks - 8))
        def _():
            pass_mean()

        inverse = wide_ref[...]
        parts = []
        for part in range(cw // LANES):
            cols = pl.ds(pl.multiple_of(c * cw + part * LANES, LANES), LANES)
            parts.append(
                (raw_ref[:, cols].astype(jnp.float32) * inverse * gain_ref[:, cols]).astype(
                    jnp.bfloat16
                )
            )
        part = jnp.concatenate(parts, axis=1)
        nm_ref[ds(peer, rows), ds(c, cw)] = part
        acc_ref[ds(peer, rows), :] += dot(part, w_ref[ds(c, cw), :])
        return 0

    lax.fori_loop(0, chunks, arrived, 0)
    rope_rows(peer)

    group = heads_q // heads_kv
    scale = HEAD_SIZE ** (-0.5)
    key_pos = lax.broadcasted_iota(jnp.int32, (rows, rows), 0)
    query_pos = lax.broadcasted_iota(jnp.int32, (rows, rows), 1)
    bias = jnp.where(key_pos <= query_pos, 0.0, -jnp.inf).astype(jnp.float32)
    bias = jnp.concatenate([bias] * group, axis=1)

    def reverse(gradient, block):
        c = cos_ref[block * rows : (block + 1) * rows]
        s = sin_ref[block * rows : (block + 1) * rows]
        return (gradient * c - pltpu.roll(gradient, HEAD_SIZE // 2, 1) * s).astype(jnp.bfloat16)

    def kv_heads(low):
        members = range(low, low + 4)
        grads = {}
        for b in range(2):
            keys = (b + 1) * rows
            block = pl.ds(b * rows, rows)
            loaded, dots, soft = {}, {}, {}
            for g in members:
                heads = [pl.ds((g * group + r) * HEAD_SIZE, HEAD_SIZE) for r in range(group)]
                kv = pl.ds(g * HEAD_SIZE, HEAD_SIZE)
                query = jnp.concatenate([q_ref[block, head] for head in heads], axis=0)
                out_grad = jnp.concatenate([go_ref[block, head] for head in heads], axis=0)
                key = k_ref[pl.ds(0, keys), kv]
                value = v_ref[pl.ds(0, keys), kv]
                loaded[g] = heads, query, out_grad, key
                dots[g] = dot(key, query, NT), dot(value, out_grad, NT)
            for g in members:
                scores, grad_prob = dots[g]
                if b == 0:
                    scores = scores + bias
                else:
                    scores = jnp.concatenate([scores[:rows], scores[rows:] + bias], axis=0)
                highest = jnp.max(scores, axis=0, keepdims=True)
                powers = jnp.exp2((scores - highest) * (scale * LOG2_E))
                prob = powers * (1.0 / jnp.sum(powers, axis=0, keepdims=True))
                inner = jnp.sum(grad_prob * prob, axis=0, keepdims=True)
                score_low = (prob * (grad_prob - inner) * scale).astype(jnp.bfloat16)
                soft[g] = prob.astype(jnp.bfloat16), score_low
            for g in members:
                heads, query, out_grad, key = loaded[g]
                prob_low, score_low = soft[g]
                part_v = dot(prob_low, out_grad)
                part_k = dot(score_low, query)
                grad_q = dot(score_low, key, TN)
                for r, head in enumerate(heads):
                    d_ref[block, head] = reverse(grad_q[r * rows : (r + 1) * rows], b)
                for j in range(b + 1):
                    pv = part_v[j * rows : (j + 1) * rows]
                    pk = part_k[j * rows : (j + 1) * rows]
                    if (g, j) in grads:
                        pv, pk = pv + grads[g, j][0], pk + grads[g, j][1]
                    grads[g, j] = pv, pk
        for g in members:
            for j in range(2):
                block = pl.ds(j * rows, rows)
                low_k = (heads_q + g) * HEAD_SIZE
                d_ref[block, pl.ds(low_k, HEAD_SIZE)] = reverse(grads[g, j][1], j)
                low_v = (heads_q + heads_kv + g) * HEAD_SIZE
                d_ref[block, pl.ds(low_v, HEAD_SIZE)] = grads[g, j][0].astype(jnp.bfloat16)

    for low in range(0, heads_kv, 4):
        kv_heads(low)

    shares(d_ref, nm_ref, w_ref, gain_ref, far_ref, here_ref, gain_part_ref, 0, tile)

    norm_copy.wait_send()
    all_gathered.wait_send()

    @pl.when(side == 0)
    def _():
        pair_copy.wait_send()
        mean_copy.wait_recv()

    @pl.when(side == 1)
    def _():
        all_scattered.wait_send()
        all_spread.wait_send()
        mean_copy.wait_send()


def second_kernel(
    tile, d_ref, nm_ref, w_ref, gain_ref, gain_a_ref, far_ref, here_ref, gain_part_ref
):
    rows, cols = here_ref.shape
    done = gain_a_ref.shape[1]
    gain_part_ref[:, pl.ds(0, done)] = gain_a_ref[...]
    shares(d_ref, nm_ref, w_ref, gain_ref, far_ref, here_ref, gain_part_ref, done, tile)
    lines = []
    for low in range(0, done + cols, cols):
        gain_part = gain_part_ref[:, pl.ds(low, cols)]
        for _ in range(3):
            lines.append(gain_part.astype(jnp.bfloat16).astype(jnp.float32))
            gain_part = gain_part - lines[-1]
    pad = far_ref.shape[0] - rows
    lines = jnp.concatenate(lines + [jnp.zeros((pad - len(lines), cols), jnp.float32)], axis=0)
    far_ref[pl.ds(rows, pad), :] = lines.astype(jnp.bfloat16)


def weights_kernel(nm_ref, d_ref, mean_ref, global_ref, momentum_ref, gq_ref, gk_ref, gv_ref, ng_ref, nmom_ref):
    i = pl.program_id(0)
    wide = gq_ref.shape[0]
    qw, kw = gq_ref.shape[1], gk_ref.shape[1]
    grad = dot(nm_ref[:, ds(i, wide)], d_ref[...], TN).astype(jnp.bfloat16)
    gq_ref[...] = grad[:, :qw]
    gk_ref[...] = grad[:, qw : qw + kw]
    gv_ref[...] = grad[:, qw + kw :]
    held = global_ref[...]
    mean_delta = held - mean_ref[:, ds(i, wide)].astype(jnp.float32)
    new_momentum = outer_momentum * momentum_ref[...] + mean_delta
    nmom_ref[...] = new_momentum
    ng_ref[...] = held - outer_rate * (mean_delta + outer_momentum * new_momentum)


def rows_kernel(
    x_ref, here_a_ref, here_b_ref, gain_ref, landed_a_ref, landed_b_ref, part_ref, out_ref, gain_out_ref
):
    i = pl.program_id(0)
    count = out_ref.shape[0]
    rows, _ = x_ref.shape

    @pl.when(i == 0)
    def _():
        lines = landed_b_ref[pl.ds(rows, landed_b_ref.shape[0] - rows), :].astype(jnp.float32)
        sums = [lines[k + 2 : k + 3] + lines[k + 1 : k + 2] + lines[k : k + 1] for k in (0, 3)]
        gain_out_ref[...] = part_ref[...] + jnp.concatenate(sums, axis=1)

    step = 8

    def some(j, _):
        block = pl.ds(pl.multiple_of(i * count + j * step, step), step)
        x = x_ref[block, :].astype(jnp.float32)
        inverse = lax.rsqrt(jnp.mean(x * x, axis=-1, keepdims=True) + epsilon)
        summed = [
            here[block, :].astype(jnp.float32) + landed[block, :].astype(jnp.float32)
            for here, landed in ((here_a_ref, landed_a_ref), (here_b_ref, landed_b_ref))
        ]
        scaled = jnp.concatenate(summed, axis=1) * gain_ref[...]
        pull = jnp.mean(scaled * x, axis=-1, keepdims=True) * (inverse * inverse)
        out_ref[ds(j, step), :] = (inverse * (scaled - x * pull)).astype(jnp.bfloat16)
        return 0

    lax.fori_loop(0, count // step, some, 0, unroll=True)


def pair_parts(
    n_rep,
    tokens,
    norm_gain,
    w_query,
    key_weight,
    value_weight,
    attention_gradient,
    global_fragment,
    momentum,
    local_fragment,
):
    rows, width = tokens.shape[1:]
    sequence = 2 * rows
    weight_q, weight_k, weight_v = w_query[0], key_weight[0], value_weight[0]
    qw, kw = weight_q.shape[1], weight_k.shape[1]
    total = qw + 2 * kw
    frag_rows = local_fragment.shape[1]
    piece_rows = 16
    n_lanes = n_rep // 2
    piece_cols = width * frag_rows // piece_rows // n_lanes
    chunks = 12
    tile = 512
    pad = 8
    first = width // 2
    bf16, f32 = jnp.bfloat16, jnp.float32
    cosine, sine = host_tables(sequence, HEAD_SIZE)
    vmem = pl.BlockSpec(memory_space=pltpu.VMEM)
    hbm = pl.BlockSpec(memory_space=pltpu.HBM)
    x, normed, d, here_a, far_a, gain_a, mean_local, weights = pl.pallas_call(
        functools.partial(front_kernel, n_rep, chunks, tile),
        out_shape=(
            pltpu.VMEM((rows, width), bf16),
            pltpu.VMEM((sequence, width), bf16),
            pltpu.VMEM((sequence, total), bf16),
            pltpu.VMEM((rows, first), bf16),
            pltpu.VMEM((rows, first), bf16),
            pltpu.VMEM((1, first), f32),
            pltpu.VMEM((frag_rows, width), bf16),
            pltpu.VMEM((width, total), bf16),
        ),
        in_specs=[hbm] * 9,
        out_specs=(vmem,) * 8,
        scratch_shapes=[
            pltpu.VMEM((1, width), f32),
            pltpu.VMEM((sequence, qw), bf16),
            pltpu.VMEM((sequence, HEAD_SIZE), f32),
            pltpu.VMEM((sequence, HEAD_SIZE), f32),
            pltpu.VMEM((sequence, total), f32),
            pltpu.VMEM((sequence, qw), bf16),
            pltpu.VMEM((sequence, kw), bf16),
            pltpu.VMEM((sequence, kw), bf16),
            pltpu.VMEM((rows, width), bf16),
            pltpu.VMEM((rows, LANES), f32),
            pltpu.VMEM((2, SUBLANES, rows), f32),
            pltpu.VMEM((frag_rows, width), bf16),
            pltpu.VMEM((frag_rows, width), bf16),
            pltpu.VMEM((frag_rows, width), bf16),
            pltpu.VMEM((n_lanes, piece_rows, piece_cols), bf16),
            pltpu.VMEM((piece_rows, piece_cols), bf16),
            pltpu.SemaphoreType.DMA((5,)),
            pltpu.SemaphoreType.DMA((total // tile,)),
            pltpu.SemaphoreType.DMA,
            pltpu.SemaphoreType.DMA((chunks,)),
            pltpu.SemaphoreType.DMA,
            pltpu.SemaphoreType.DMA,
            pltpu.SemaphoreType.DMA,
            pltpu.SemaphoreType.DMA,
            pltpu.SemaphoreType.DMA((6,)),
            pltpu.SemaphoreType.DMA,
            pltpu.SemaphoreType.REGULAR,
        ],
        compiler_params=pltpu.CompilerParams(
            collective_id=0, has_side_effects=True, vmem_limit_bytes=20 * 1024 * 1024
        ),
    )(
        *[
            pltpu.with_memory_space_constraint(array, pltpu.HBM)
            for array in (
                tokens[0],
                norm_gain,
                weight_q,
                weight_k,
                weight_v,
                attention_gradient[0],
                cosine,
                sine,
                local_fragment[0],
            )
        ]
    )
    swap = [(0, 1), (1, 0)]
    landed_a = lax.ppermute(far_a, "tp", swap)
    far_b, here_b, gain_partial = pl.pallas_call(
        functools.partial(second_kernel, tile),
        out_shape=(
            pltpu.VMEM((rows + pad, width - first), bf16),
            pltpu.VMEM((rows, width - first), bf16),
            pltpu.VMEM((1, width), f32),
        ),
        in_specs=[vmem] * 5,
        out_specs=(vmem,) * 3,
        compiler_params=pltpu.CompilerParams(vmem_limit_bytes=8 * 1024 * 1024),
        cost_estimate=pl.CostEstimate(
            flops=sequence * width * total, bytes_accessed=width * total, transcendentals=0
        ),
    )(d, normed, weights, norm_gain, gain_a)
    landed_b = lax.ppermute(far_b, "tp", swap)
    wide = 768
    columns = lambda size: pl.BlockSpec((size, wide), lambda i: (0, i))
    grad_wq, grad_wk, grad_wv, new_global, new_momentum = pl.pallas_call(
        weights_kernel,
        grid=(width // wide,),
        out_shape=(
            jax.ShapeDtypeStruct((width, qw), bf16),
            jax.ShapeDtypeStruct((width, kw), bf16),
            jax.ShapeDtypeStruct((width, kw), bf16),
            jax.ShapeDtypeStruct((frag_rows, width), f32),
            jax.ShapeDtypeStruct((frag_rows, width), f32),
        ),
        in_specs=[vmem, vmem, vmem, columns(frag_rows), columns(frag_rows)],
        out_specs=(
            pl.BlockSpec((wide, qw), lambda i: (i, 0)),
            pl.BlockSpec((wide, kw), lambda i: (i, 0)),
            pl.BlockSpec((wide, kw), lambda i: (i, 0)),
            columns(frag_rows),
            columns(frag_rows),
        ),
        compiler_params=pltpu.CompilerParams(vmem_limit_bytes=28 * 1024 * 1024),
        cost_estimate=pl.CostEstimate(
            flops=2 * sequence * width * total, bytes_accessed=3 * width * total, transcendentals=0
        ),
    )(normed, d, mean_local, global_fragment, momentum)
    count = rows // 2
    block = pl.BlockSpec((count, width), lambda i: (i, 0))
    gradient_rows, gains_gradient = pl.pallas_call(
        rows_kernel,
        grid=(rows // count,),
        out_shape=(
            jax.ShapeDtypeStruct((rows, width), bf16),
            jax.ShapeDtypeStruct((1, width), f32),
        ),
        in_specs=[vmem] * 7,
        out_specs=(block, pl.BlockSpec((1, width), lambda i: (0, 0))),
        compiler_params=pltpu.CompilerParams(vmem_limit_bytes=8 * 1024 * 1024),
        cost_estimate=pl.CostEstimate(
            flops=12 * rows * width, bytes_accessed=4 * rows * width, transcendentals=0
        ),
    )(x, here_a, here_b, norm_gain, landed_a, landed_b, gain_partial)
    return (
        grad_wq[None],
        grad_wk[None],
        grad_wv[None],
        gains_gradient,
        gradient_rows[None],
        new_global,
        new_momentum,
    )


def solution(mesh):
    placed = (
        P("rep", "tp", None),
        P("rep", None),
        P("rep", None, "tp"),
        P("rep", None, "tp"),
        P("rep", None, "tp"),
        P("rep", None, "tp"),
        P("tp", None),
        P("tp", None),
        P("rep", "tp", None),
    )
    paired = mesh.shape["tp"] == 2 and mesh.shape["rep"] % 2 == 0
    chosen = functools.partial(pair_parts, mesh.shape["rep"]) if paired else body
    return jax.shard_map(
        chosen,
        mesh=mesh,
        in_specs=placed,
        out_specs=(
            P("rep", None, "tp"),
            P("rep", None, "tp"),
            P("rep", None, "tp"),
            P("rep", None),
            P("rep", "tp", None),
            P("tp", None),
            P("tp", None),
        ),
        check_vma=False,
    )
```
